32 devices in a mesh: rep: 4 (over y, core), shard: 8 (over z, x).
Axes of the slice: x: 2, y: 2, z: 4, core: 2. Of those that a mesh axis runs over, the one named last changes fastest.
Arguments:
- block_input: bfloat16 [4096, 2048], P(('rep', 'shard')), may hold values from -6 to 6
- cotangent: bfloat16 [4096, 2048], P(('rep', 'shard')), may hold values from -6 to 6
- attn_gain: bfloat16 [2048], P('shard'), may hold values from 0.5 to 1.5
- query_weight: bfloat16 [2048, 2048], P('shard'), may hold values from -0.125 to 0.125
- key_weight: bfloat16 [2048, 256], P('shard'), may hold values from -0.125 to 0.125
- value_weight: bfloat16 [2048, 256], P('shard'), may hold values from -0.125 to 0.125
- out_weight: bfloat16 [2048, 2048], P('shard'), may hold values from -1 to 1
- mlp_gain: bfloat16 [2048], P('shard'), may hold values from 0.5 to 1.5
- gate_weight: bfloat16 [2048, 5632], P('shard'), may hold values from -0.125 to 0.125
- up_weight: bfloat16 [2048, 5632], P('shard'), may hold values from -0.125 to 0.125
- down_weight: bfloat16 [5632, 2048], P('shard'), may hold values from -0.078125 to 0.078125
Outputs:
- block_output: bfloat16 [4096, 2048], P(('rep', 'shard'))
- input_grad: float32 [4096, 2048], P(('rep', 'shard'))
- query_grad: float32 [2048, 2048], P('shard')
- key_grad: float32 [2048, 256], P('shard')
- value_grad: float32 [2048, 256], P('shard')
- out_grad: float32 [2048, 2048], P('shard')
- gate_grad: float32 [2048, 5632], P('shard')
- up_grad: float32 [2048, 5632], P('shard')
- down_grad: float32 [5632, 2048], P('shard')
- attn_gain_grad: float32 [2048], P('shard')
- mlp_gain_grad: float32 [2048], P('shard')
The draws below stay inside these ranges and needn't reach their ends.
All inputs are finite; a program needn't handle non-finite values.
Results may differ from the reference program's by a relative error of at most 0.02.
Values may be sent and summed in bfloat16 or wider, within the bound.
A program may use at most 448 MiB of HBM per device.

```python
import math
import jax
import jax.numpy as jnp
from jax import lax

D = 2048
H = 32
KV = 4
HD = 64
FF = 5632
SEQ = 128
TOKENS = 4096


def spiked(values, own_key, source, target, shards_of, factor):
    owner, partner = [(jnp.arange(values.shape[dim]) // (values.shape[dim] // shards_of)).reshape([-1 if axis == dim else 1 for axis in range(values.ndim)]) for dim in (source, target)]
    chosen = jax.random.permutation(own_key, shards_of)[partner]
    strong = (owner == chosen) | (owner == (partner + shards_of // 2) % shards_of)
    return jnp.where(strong, factor * values, values)


def block_scale(own_key, dims, pieces, least, high):
    loudness, own = 1.0, jax.random.fold_in(own_key, 6)
    for axis_at, shards_of in pieces:
        draws = jnp.exp(jax.random.uniform(jax.random.fold_in(own, axis_at), (shards_of,), jnp.float32, least / len(pieces), high / len(pieces)))
        loudness = loudness * jnp.repeat(draws, dims[axis_at] // shards_of).reshape([-1 if axis == axis_at else 1 for axis in range(len(dims))])
    return loudness


def noise(key, shape, scale, bound, split=(), kind=jnp.bfloat16):
    loudness = block_scale(key, shape, split, -0.22, 0.18) if split else 1.0
    drawn = jax.random.normal(key, shape, jnp.float32) * scale * loudness
    return jnp.minimum(jnp.maximum(drawn, -bound), bound).astype(kind)


def heavy_noise(own_key, shape, deviation, most, shards, heavy, kind=jnp.bfloat16):
    values = deviation * jax.random.normal(own_key, shape, jnp.float32)
    if shards:
        values = values * block_scale(own_key, shape, shards, -0.22, 0.18)
    return jnp.clip(spiked(values, jax.random.fold_in(own_key, 3), *heavy), -most, most).astype(kind)


def setup_inputs(seed: int = 0) -> dict:
    key_list = jax.random.split(jax.random.key(seed), 12)
    block_input = noise(key_list[0], (TOKENS, D), 1.0, 6.0, ((0, 32),))
    cotangent = heavy_noise(key_list[1], (TOKENS, D), 1.0, 6.0, ((0, 32),), (0, 1, 32, 2.75))
    attn_gain = jnp.clip(1.0 + 0.1 * jax.random.normal(key_list[2], (D,), jnp.float32), 0.5, 1.5).astype(jnp.bfloat16)
    query_weight = noise(key_list[3], (D, H * HD), D ** -0.5, 0.125, ((0, 8),))
    key_weight = noise(key_list[4], (D, KV * HD), D ** -0.5, 0.125, ((0, 8),))
    value_weight = noise(key_list[5], (D, KV * HD), D ** -0.5, 0.125, ((0, 8),))
    out_weight = noise(key_list[6], (H * HD, D), (H * HD // 64) ** -0.5, 1.0, ((0, 8),))
    mlp_gain = jnp.clip(1.0 + 0.1 * jax.random.normal(key_list[7], (D,), jnp.float32), 0.5, 1.5).astype(jnp.bfloat16)
    gate_weight = noise(key_list[8], (D, FF), D ** -0.5, 0.125, ((0, 8),))
    up_weight = noise(key_list[9], (D, FF), D ** -0.5, 0.125, ((0, 8),))
    down_weight = noise(key_list[10], (FF, D), FF ** -0.5, 0.078125, ((0, 8),))
    return {"block_input": block_input, "cotangent": cotangent, "attn_gain": attn_gain, "query_weight": query_weight, "key_weight": key_weight, "value_weight": value_weight, "out_weight": out_weight, "mlp_gain": mlp_gain, "gate_weight": gate_weight, "up_weight": up_weight, "down_weight": down_weight}


epsilon = 1e-05

def rotary_tables(length, head_size):
    positions = jnp.arange(length, dtype=jnp.float32)[:, None]
    spacing = jnp.arange(head_size // 2, dtype=jnp.float32) * (-2.0 * math.log(10000.0) / head_size)
    angles = positions * jnp.exp(spacing)[None, :]
    cos_table = jnp.cos(angles)
    sin_table = jnp.sin(angles)
    return (jnp.concatenate([cos_table, cos_table], axis=-1), jnp.concatenate([sin_table, sin_table], axis=-1))

def rotate_half(values):
    middle = values.shape[-1] // 2
    return jnp.concatenate([-values[..., middle:], values[..., :middle]], axis=-1)

def rotate_back(values):
    middle = values.shape[-1] // 2
    return jnp.concatenate([values[..., middle:], -values[..., :middle]], axis=-1)

def apply_rotary(values, cos_table, sin_table):
    return values * cos_table[:, None, :] + rotate_half(values) * sin_table[:, None, :]

def rotary_back(grads, cos_table, sin_table):
    return grads * cos_table[:, None, :] + rotate_back(grads * sin_table[:, None, :])

def norm_back(grad_normed, inputs, scale):
    return scale * grad_normed - inputs * (scale * scale * scale) * lax.optimization_barrier(jnp.mean(grad_normed * inputs, axis=-1, keepdims=True))

def matmul(left, right):
    return jnp.dot(left, right, preferred_element_type=jnp.float32)

def one_sequence(inputs, cotangent, attn_gain, query_weight, key_weight, value_weight, out_weight, mlp_gain, gate_weight, up_weight, down_weight):
    length = inputs.shape[0]
    groups = H // KV
    scale_factor = HD ** (-0.5)
    x_float = inputs.astype(jnp.float32)
    rms_one = lax.rsqrt(lax.optimization_barrier(jnp.mean(x_float * x_float, axis=-1, keepdims=True)) + epsilon)
    normed_one = x_float * rms_one
    hidden_one = (normed_one * attn_gain.astype(jnp.float32)).astype(jnp.bfloat16)
    cos_table, sin_table = rotary_tables(length, HD)
    query_rot = apply_rotary(matmul(hidden_one, query_weight).reshape(length, H, HD), cos_table, sin_table)
    query_rot = query_rot.astype(jnp.bfloat16).reshape(length, KV, groups, HD)
    key_rot = apply_rotary(matmul(hidden_one, key_weight).reshape(length, KV, HD), cos_table, sin_table).astype(jnp.bfloat16)
    value_rows = matmul(hidden_one, value_weight).reshape(length, KV, HD).astype(jnp.bfloat16)
    causal = jnp.arange(length)[:, None] >= jnp.arange(length)[None, :]
    scores = jnp.einsum('ikgd,jkd->kgij', query_rot.astype(jnp.float32), key_rot.astype(jnp.float32)) * scale_factor
    log_total = jnp.log(lax.optimization_barrier(jnp.sum(jnp.where(causal, jnp.exp(scores), 0.0), axis=-1)))
    weights = jnp.where(causal, jnp.exp(scores - log_total[..., None]), 0.0)
    weights_bf = weights.astype(jnp.bfloat16)
    attended = jnp.einsum('kgij,jkd->ikgd', weights_bf.astype(jnp.float32), value_rows.astype(jnp.float32))
    attended = attended.reshape(length, H * HD).astype(jnp.bfloat16)
    mixed_sum = x_float + matmul(attended, out_weight)
    rms_two = lax.rsqrt(lax.optimization_barrier(jnp.mean(mixed_sum * mixed_sum, axis=-1, keepdims=True)) + epsilon)
    normed_two = mixed_sum * rms_two
    hidden_two = (normed_two * mlp_gain.astype(jnp.float32)).astype(jnp.bfloat16)
    gate_raw = matmul(hidden_two, gate_weight)
    up_raw = matmul(hidden_two, up_weight)
    sigmoid = jax.nn.sigmoid(gate_raw)
    activated = gate_raw * sigmoid
    product = (activated * up_raw).astype(jnp.bfloat16)
    result = (mixed_sum + matmul(product, down_weight)).astype(jnp.bfloat16)
    down_grad = matmul(product.T, cotangent)
    grad_product = matmul(cotangent, down_weight.T)
    grad_gate = (grad_product * up_raw * sigmoid * (1.0 + gate_raw * (1.0 - sigmoid))).astype(jnp.bfloat16)
    grad_up = (grad_product * activated).astype(jnp.bfloat16)
    gate_grad = matmul(hidden_two.T, grad_gate)
    up_grad = matmul(hidden_two.T, grad_up)
    grad_hidden_two = matmul(grad_gate, gate_weight.T) + matmul(grad_up, up_weight.T)
    mlp_gain_grad = lax.optimization_barrier(jnp.sum(grad_hidden_two * normed_two, axis=0))
    grad_mixed = cotangent.astype(jnp.float32) + norm_back(grad_hidden_two * mlp_gain.astype(jnp.float32), mixed_sum, rms_two)
    grad_mixed_bf = grad_mixed.astype(jnp.bfloat16)
    out_grad = matmul(attended.T, grad_mixed_bf)
    grad_attended = matmul(grad_mixed_bf, out_weight.T).astype(jnp.bfloat16).reshape(length, KV, groups, HD)
    grad_weights = jnp.einsum('ikgd,jkd->kgij', grad_attended.astype(jnp.float32), value_rows.astype(jnp.float32))
    row_total = lax.optimization_barrier(jnp.sum(weights * grad_weights, axis=-1, keepdims=True))
    grad_scores = (weights * (grad_weights - row_total) * scale_factor).astype(jnp.bfloat16)
    grad_query_rot = jnp.einsum('kgij,jkd->ikgd', grad_scores.astype(jnp.float32), key_rot.astype(jnp.float32)).reshape(length, H, HD)
    grad_key_rot = jnp.einsum('kgij,ikgd->jkd', grad_scores.astype(jnp.float32), query_rot.astype(jnp.float32))
    grad_value = jnp.einsum('kgij,ikgd->jkd', weights_bf.astype(jnp.float32), grad_attended.astype(jnp.float32))
    grad_query = rotary_back(grad_query_rot, cos_table, sin_table).astype(jnp.bfloat16).reshape(length, H * HD)
    grad_key = rotary_back(grad_key_rot, cos_table, sin_table).astype(jnp.bfloat16).reshape(length, KV * HD)
    grad_value_bf = grad_value.astype(jnp.bfloat16).reshape(length, KV * HD)
    query_grad = matmul(hidden_one.T, grad_query)
    key_grad = matmul(hidden_one.T, grad_key)
    value_grad = matmul(hidden_one.T, grad_value_bf)
    grad_hidden_one = matmul(grad_query, query_weight.T) + matmul(grad_key, key_weight.T) + matmul(grad_value_bf, value_weight.T)
    attn_gain_grad = lax.optimization_barrier(jnp.sum(grad_hidden_one * normed_one, axis=0))
    input_grad = grad_mixed + norm_back(grad_hidden_one * attn_gain.astype(jnp.float32), x_float, rms_one)
    grads = (query_grad, key_grad, value_grad, out_grad, gate_grad, up_grad, down_grad, attn_gain_grad, mlp_gain_grad)
    return (result, input_grad, grads)

def reference(block_input, cotangent, attn_gain, query_weight, key_weight, value_weight, out_weight, mlp_gain, gate_weight, up_weight, down_weight):
    count = TOKENS // SEQ
    inputs = block_input.reshape(count, SEQ, D)
    cotangents = cotangent.reshape(count, SEQ, D)
    zeros = (jnp.zeros((D, H * HD), jnp.float32), jnp.zeros((D, KV * HD), jnp.float32), jnp.zeros((D, KV * HD), jnp.float32), jnp.zeros((H * HD, D), jnp.float32), jnp.zeros((D, FF), jnp.float32), jnp.zeros((D, FF), jnp.float32), jnp.zeros((FF, D), jnp.float32), jnp.zeros((D,), jnp.float32), jnp.zeros((D,), jnp.float32))

    def step(totals, pair):
        result, input_grad, grads = one_sequence(pair[0], pair[1], attn_gain, query_weight, key_weight, value_weight, out_weight, mlp_gain, gate_weight, up_weight, down_weight)
        return (tuple((total + grad for total, grad in zip(totals, grads))), (result, input_grad))
    totals, (results, input_grads) = lax.scan(step, zeros, (inputs, cotangents))
    return (results.reshape(TOKENS, D), input_grads.reshape(TOKENS, D), totals[0], totals[1], totals[2], totals[3], totals[4], totals[5], totals[6], totals[7], totals[8])
```

```python
import math

import jax
import jax.numpy as jnp
from jax import lax
from jax.sharding import Mesh, PartitionSpec as P

KV = 4
HD = 64
X = 2
epsilon = 1e-05

TP = ("rep", "x")


def rotary_tables(length, head_size):
    positions = jnp.arange(length, dtype=jnp.float32)[:, None]
    spacing = jnp.arange(head_size // 2, dtype=jnp.float32) * (-2.0 * math.log(10000.0) / head_size)
    angles = positions * jnp.exp(spacing)[None, :]
    cos_table = jnp.cos(angles)
    sin_table = jnp.sin(angles)
    return (
        jnp.concatenate([cos_table, cos_table], axis=-1),
        jnp.concatenate([sin_table, sin_table], axis=-1),
    )


def rotate_half(values):
    middle = values.shape[-1] // 2
    return jnp.concatenate([-values[..., middle:], values[..., :middle]], axis=-1)


def rotate_back(values):
    middle = values.shape[-1] // 2
    return jnp.concatenate([values[..., middle:], -values[..., :middle]], axis=-1)


def norm_back(grad_normed, inputs, scale):
    return scale * grad_normed - inputs * (scale * scale * scale) * jnp.mean(
        grad_normed * inputs, axis=-1, keepdims=True
    )


def matmul(left, right):
    return jnp.dot(left, right, preferred_element_type=jnp.float32)


def contract_last(left, right):
    return lax.dot_general(
        left, right, (((1,), (1,)), ((), ())), preferred_element_type=jnp.float32
    )


def contract_first(left, right):
    return lax.dot_general(
        left, right, (((0,), (0,)), ((), ())), preferred_element_type=jnp.float32
    )


def gather_tokens(rows):
    return lax.all_gather(rows, TP, axis=0, tiled=True)


def scatter_tokens(partial):
    return lax.psum_scatter(
        partial.astype(jnp.bfloat16), TP, scatter_dimension=0, tiled=True
    ).astype(jnp.float32)


def swap_x(pieces):
    x = lax.axis_index("x")
    away = jnp.where(x == 0, pieces[1], pieces[0])
    own = jnp.where(x == 0, pieces[0], pieces[1])
    came = lax.ppermute(away, "x", [(0, 1), (1, 0)])
    return jnp.stack([jnp.where(x == 0, own, came), jnp.where(x == 0, came, own)])


def per_device(
    block_input,
    cotangent,
    attn_gain,
    query_weight,
    key_weight,
    value_weight,
    out_weight,
    mlp_gain,
    gate_weight,
    up_weight,
    down_weight,
):
    length, width = block_input.shape
    reps, zs = lax.axis_size("rep"), lax.axis_size("z")
    group = reps * X
    r = lax.axis_index("rep")
    z = lax.axis_index("z")
    x = lax.axis_index("x")
    rows = query_weight.shape[0]
    heads_wide = query_weight.shape[1] // group
    per_kv = zs // KV
    hidden_piece = down_weight.shape[0] // reps
    hidden_wide = zs * hidden_piece
    heads = heads_wide // HD
    scale_factor = HD ** (-0.5)

    def own_rep(values, axis):
        return lax.dynamic_index_in_dim(values, r, axis, keepdims=False)

    def query_columns(weight):
        pieces = own_rep(weight.reshape(rows, KV, per_kv, X, -1), 1)
        return jnp.moveaxis(pieces, 2, 0).reshape(X, rows, heads_wide)

    def hidden_columns(weight):
        pieces = own_rep(weight.reshape(rows, zs, X, reps, hidden_piece), 3)
        return jnp.moveaxis(pieces, 2, 0).reshape(X, rows, hidden_wide)

    def key_columns(weight):
        piece = own_rep(weight.reshape(rows, KV, HD), 1)
        return jnp.broadcast_to(piece[None], (X, rows, HD))

    attn_pack = jnp.concatenate(
        [query_columns(query_weight), key_columns(key_weight), key_columns(value_weight)], axis=2
    )
    mlp_pack = jnp.concatenate([hidden_columns(gate_weight), hidden_columns(up_weight)], axis=2)

    gains = lax.all_gather(jnp.stack([attn_gain, mlp_gain]), ("z", "x"), axis=1, tiled=True)
    gains = gains.astype(jnp.float32)
    gain_one, gain_two = gains[0], gains[1]
    attn_w = lax.all_gather(swap_x(attn_pack), "z", axis=0).reshape(width, -1)
    out_all = lax.all_gather(out_weight, "z", axis=0)
    out_w = own_rep(out_all.reshape(KV, per_kv * rows, width), 0)
    mlp_w = lax.all_gather(swap_x(mlp_pack), "z", axis=0).reshape(width, -1)
    down_w = lax.all_gather(
        own_rep(down_weight.reshape(reps, hidden_piece, width), 0), "z", axis=0
    ).reshape(hidden_wide, width)

    x_float = block_input.astype(jnp.float32)
    rms_one = lax.rsqrt(jnp.mean(x_float * x_float, axis=-1, keepdims=True) + epsilon)
    normed_one = x_float * rms_one
    hidden_one = gather_tokens((normed_one * gain_one[None, :]).astype(jnp.bfloat16))
    cot_all = gather_tokens(cotangent)
    raw = matmul(hidden_one, attn_w).reshape(group, length, -1)
    cos_table, sin_table = rotary_tables(length, HD)

    def rotary(values):
        return (
            values * cos_table[:, None, :] + rotate_half(values) * sin_table[:, None, :]
        ).astype(jnp.bfloat16)

    def rotary_back(grads):
        return (
            grads * cos_table[:, None, :] + rotate_back(grads * sin_table[:, None, :])
        ).astype(jnp.bfloat16)

    query_rot = rotary(raw[..., :heads_wide].reshape(group, length, heads, HD))
    key_rot = rotary(raw[..., None, heads_wide : heads_wide + HD])[:, :, 0]
    value_rows = raw[..., heads_wide + HD :].astype(jnp.bfloat16)
    causal = jnp.arange(length)[:, None] >= jnp.arange(length)[None, :]

    def product_of(spec, left, right):
        return jnp.einsum(spec, left, right, preferred_element_type=jnp.float32)

    scores = product_of("bigd,bjd->bgij", query_rot, key_rot) * scale_factor
    log_total = jnp.log(jnp.sum(jnp.where(causal, jnp.exp(scores), 0.0), axis=-1))
    weights = jnp.where(causal, jnp.exp(scores - log_total[..., None]), 0.0)
    weights_bf = weights.astype(jnp.bfloat16)
    attended = product_of("bgij,bjd->bigd", weights_bf, value_rows)
    attended = attended.astype(jnp.bfloat16).reshape(group * length, heads_wide)
    mixed_sum = x_float + scatter_tokens(matmul(attended, out_w))

    rms_two = lax.rsqrt(jnp.mean(mixed_sum * mixed_sum, axis=-1, keepdims=True) + epsilon)
    normed_two = mixed_sum * rms_two
    hidden_two = gather_tokens((normed_two * gain_two[None, :]).astype(jnp.bfloat16))
    gate_up = matmul(hidden_two, mlp_w)
    gate_raw, up_raw = gate_up[:, :hidden_wide], gate_up[:, hidden_wide:]
    sigmoid = jax.nn.sigmoid(gate_raw)
    activated = gate_raw * sigmoid
    product = (activated * up_raw).astype(jnp.bfloat16)
    grad_product = contract_last(cot_all, down_w)
    grad_gate = grad_product * up_raw * sigmoid * (1.0 + gate_raw * (1.0 - sigmoid))
    grad_up = grad_product * activated
    grad_both = jnp.concatenate([grad_gate, grad_up], axis=1).astype(jnp.bfloat16)
    grad_hidden_two = scatter_tokens(contract_last(grad_both, mlp_w))
    block_output = (mixed_sum + scatter_tokens(matmul(product, down_w))).astype(jnp.bfloat16)
    down_local = contract_first(product, cot_all).astype(jnp.bfloat16)
    mlp_local = contract_first(hidden_two, grad_both).astype(jnp.bfloat16)

    grad_mixed = cotangent.astype(jnp.float32) + norm_back(
        grad_hidden_two * gain_two[None, :], mixed_sum, rms_two
    )

    grad_mixed_bf = gather_tokens(grad_mixed.astype(jnp.bfloat16))
    grad_attended = contract_last(grad_mixed_bf, out_w).astype(jnp.bfloat16)
    out_local = contract_first(attended, grad_mixed_bf).astype(jnp.bfloat16)
    grad_attended = grad_attended.reshape(group, length, heads, HD)
    grad_weights = product_of("bigd,bjd->bgij", grad_attended, value_rows)
    row_total = jnp.sum(weights * grad_weights, axis=-1, keepdims=True)
    grad_scores = (weights * (grad_weights - row_total) * scale_factor).astype(jnp.bfloat16)
    grad_query = rotary_back(product_of("bgij,bjd->bigd", grad_scores, key_rot))
    grad_key = rotary_back(product_of("bgij,bigd->bjd", grad_scores, query_rot)[:, :, None])
    grad_value = product_of("bgij,bigd->bjd", weights_bf, grad_attended).astype(jnp.bfloat16)
    grad_attn = jnp.concatenate(
        [
            grad_query.reshape(group * length, heads_wide),
            grad_key.reshape(group * length, HD),
            grad_value.reshape(group * length, HD),
        ],
        axis=1,
    )
    grad_hidden_one = scatter_tokens(contract_last(grad_attn, attn_w))
    attn_local = contract_first(hidden_one, grad_attn).astype(jnp.bfloat16)
    input_grad = grad_mixed + norm_back(
        grad_hidden_one * gain_one[None, :], x_float, rms_one
    )

    def scatter_z(partial):
        return lax.psum_scatter(partial, "z", scatter_dimension=0, tiled=True)

    def to_owner(partial):
        pieces = swap_x(scatter_z(partial).reshape(X, rows, -1))
        return lax.all_gather(pieces, "rep", axis=0).astype(jnp.float32)

    down_grad = lax.all_gather(scatter_z(down_local), "rep", axis=0, tiled=True).astype(jnp.float32)
    mlp_grad = to_owner(mlp_local).reshape(reps, X, rows, 2, zs, hidden_piece)
    mlp_grad = mlp_grad.transpose(3, 2, 4, 1, 0, 5).reshape(2, rows, -1)
    out_padded = jnp.where(
        (jnp.arange(KV) == r)[:, None, None],
        out_local.reshape(1, per_kv * rows, width),
        jnp.zeros((), jnp.bfloat16),
    )
    out_grad = lax.psum(scatter_z(out_padded.reshape(zs * rows, width)), "rep").astype(jnp.float32)
    attn_grad = to_owner(attn_local)
    query_grad = attn_grad[..., :heads_wide].reshape(KV, X, rows, per_kv, -1)
    query_grad = query_grad.transpose(2, 0, 3, 1, 4).reshape(rows, -1)
    key_value = jnp.sum(attn_grad[..., heads_wide:], axis=1)
    key_grad = key_value[..., :HD].transpose(1, 0, 2).reshape(rows, -1)
    value_grad = key_value[..., HD:].transpose(1, 0, 2).reshape(rows, -1)
    gain_grads = lax.psum(
        jnp.stack(
            [
                jnp.sum(grad_hidden_one * normed_one, axis=0),
                jnp.sum(grad_hidden_two * normed_two, axis=0),
            ]
        ),
        ("rep", "z", "x"),
    )
    gain_grads = lax.dynamic_slice_in_dim(gain_grads, (z * X + x) * rows, rows, axis=1)
    return (
        block_output,
        input_grad,
        query_grad,
        key_grad,
        value_grad,
        out_grad,
        mlp_grad[0],
        mlp_grad[1],
        down_grad,
        gain_grads[0],
        gain_grads[1],
    )


def solution(mesh):
    reps, shards = mesh.shape["rep"], mesh.shape["shard"]
    cube = Mesh(mesh.devices.reshape(reps, shards // X, X), ("rep", "z", "x"))
    tokens = P(("rep", "z", "x"), None)
    matrix = P(("z", "x"), None)
    vector = P(("z", "x"))
    in_specs = (tokens, tokens, vector) + (matrix,) * 4 + (vector,) + (matrix,) * 3
    out_specs = (tokens, tokens) + (matrix,) * 7 + (vector,) * 2
    return jax.shard_map(
        per_device, mesh=cube, in_specs=in_specs, out_specs=out_specs, check_vma=False
    )
```

```python
import math

import jax
import jax.numpy as jnp
from jax import lax
from jax.sharding import Mesh, PartitionSpec as P

KV = 4
HD = 64
PAIR = 2
epsilon = 1e-05

TP = ("rep", "zl")
HOLDERS = ("zh", "x")


def rotary_tables(length, head_size):
    positions = jnp.arange(length, dtype=jnp.float32)[:, None]
    spacing = jnp.arange(head_size // 2, dtype=jnp.float32) * (-2.0 * math.log(10000.0) / head_size)
    angles = positions * jnp.exp(spacing)[None, :]
    cos_table = jnp.cos(angles)
    sin_table = jnp.sin(angles)
    return (
        jnp.concatenate([cos_table, cos_table], axis=-1),
        jnp.concatenate([sin_table, sin_table], axis=-1),
    )


def rotate_half(values):
    middle = values.shape[-1] // 2
    return jnp.concatenate([-values[..., middle:], values[..., :middle]], axis=-1)


def rotate_back(values):
    middle = values.shape[-1] // 2
    return jnp.concatenate([values[..., middle:], -values[..., :middle]], axis=-1)


def norm_back(grad_normed, inputs, scale):
    return scale * grad_normed - inputs * (scale * scale * scale) * jnp.mean(
        grad_normed * inputs, axis=-1, keepdims=True
    )


def matmul(left, right):
    return jnp.dot(left, right, preferred_element_type=jnp.float32)


def contract_last(left, right):
    return lax.dot_general(
        left, right, (((1,), (1,)), ((), ())), preferred_element_type=jnp.float32
    )


def contract_first(left, right):
    return lax.dot_general(
        left, right, (((0,), (0,)), ((), ())), preferred_element_type=jnp.float32
    )


def gather_tokens(rows):
    return lax.all_gather(rows, TP, axis=0, tiled=True)


def scatter_tokens(partial):
    return lax.psum_scatter(
        partial.astype(jnp.bfloat16), TP, scatter_dimension=0, tiled=True
    ).astype(jnp.float32)


SWAP = [(0, 1), (1, 0)]


def swap(pieces, axis):
    first = lax.axis_index(axis) == 0
    came = lax.ppermute(jnp.where(first, pieces[1], pieces[0]), axis, SWAP)
    own = jnp.where(first, pieces[0], pieces[1])
    return jnp.stack([jnp.where(first, own, came), jnp.where(first, came, own)])


def exchange(piece, axis):
    first = lax.axis_index(axis) == 0
    came = lax.ppermute(piece, axis, SWAP)
    return jnp.stack([jnp.where(first, piece, came), jnp.where(first, came, piece)])


def gather_holders(piece):
    if lax.axis_size("zh") == PAIR and lax.axis_size("x") == PAIR:
        both = exchange(exchange(piece, "zh"), "x")
        return jnp.moveaxis(both, 0, 1).reshape((PAIR * PAIR,) + piece.shape)
    return lax.all_gather(piece, HOLDERS, axis=0)


def add(left, right):
    return (left.astype(jnp.float32) + right.astype(jnp.float32)).astype(jnp.bfloat16)


def halve(pieces, axis):
    first = lax.axis_index(axis) == 0
    came = lax.ppermute(jnp.where(first, pieces[1], pieces[0]), axis, SWAP)
    return add(jnp.where(first, pieces[0], pieces[1]), came)


def scatter_holders(partial):
    if lax.axis_size("zh") == PAIR and lax.axis_size("x") == PAIR:
        pieces = jnp.moveaxis(partial.reshape((PAIR, PAIR) + partial.shape[1:]), 1, 0)
        return halve(halve(pieces, "x"), "zh")
    return lax.psum_scatter(partial, HOLDERS, scatter_dimension=0, tiled=False)


def per_device(
    block_input,
    cotangent,
    attn_gain,
    query_weight,
    key_weight,
    value_weight,
    out_weight,
    mlp_gain,
    gate_weight,
    up_weight,
    down_weight,
):
    length, width = block_input.shape
    reps, xs = lax.axis_size("rep"), lax.axis_size("x")
    high = lax.axis_size("zh")
    holders = high * xs
    group = reps * PAIR
    r, zl, x = lax.axis_index("rep"), lax.axis_index("zl"), lax.axis_index("x")
    shard = (lax.axis_index("zh") * PAIR + zl) * xs + x
    rows = query_weight.shape[0]
    heads_wide = query_weight.shape[1] // group
    per_rep = holders // reps
    hidden_piece = down_weight.shape[0] // reps
    hidden_wide = holders * hidden_piece
    heads = heads_wide // HD
    scale_factor = HD ** (-0.5)

    def own_rep(values, axis):
        return lax.dynamic_index_in_dim(values, r, axis, keepdims=False)

    def by_holder(values, axis):
        shape = values.shape
        cut = values.reshape(shape[:axis] + (high, PAIR, xs, -1) + shape[axis + 1 :])
        cut = jnp.moveaxis(cut, axis + 1, 0)
        return cut.reshape((PAIR,) + shape[:axis] + (holders, -1) + shape[axis + 1 :])

    def query_columns(weight):
        pieces = by_holder(weight, 1).reshape(PAIR, rows, reps, heads_wide)
        return own_rep(pieces, 2)

    def hidden_columns(weight):
        pieces = by_holder(weight, 1).reshape(PAIR, rows, holders, reps, hidden_piece)
        return own_rep(pieces, 3).reshape(PAIR, rows, hidden_wide)

    key_heads = [
        (((r * per_rep // xs) * PAIR + low) * xs * heads_wide // (per_rep * HD)) * KV
        // (query_weight.shape[1] // HD)
        for low in range(PAIR)
    ]

    def key_columns(weight):
        pieces = weight.reshape(rows, KV, HD)
        return jnp.stack(
            [lax.dynamic_index_in_dim(pieces, k, 1, keepdims=False) for k in key_heads]
        )

    attn_pack = jnp.concatenate(
        [query_columns(query_weight), key_columns(key_weight), key_columns(value_weight)], axis=2
    )
    mlp_pack = jnp.concatenate([hidden_columns(gate_weight), hidden_columns(up_weight)], axis=2)

    gains = lax.all_gather(
        jnp.stack([attn_gain, mlp_gain]), ("zh", "zl", "x"), axis=1, tiled=True
    )
    gains = gains.astype(jnp.float32)
    gain_one, gain_two = gains[0], gains[1]

    def all_rows(pack):
        whole = gather_holders(swap(pack, "zl"))
        whole = whole.reshape((high, xs, PAIR) + whole.shape[2:])
        return jnp.swapaxes(whole, 1, 2).reshape(width, -1)

    attn_w = all_rows(attn_pack)
    out_w = own_rep(gather_holders(out_weight).reshape(reps, per_rep * rows, width), 0)
    down_w = gather_holders(own_rep(down_weight.reshape(reps, hidden_piece, width), 0))
    down_w = down_w.reshape(hidden_wide, width)
    mlp_w = all_rows(mlp_pack)

    x_float = block_input.astype(jnp.float32)
    rms_one = lax.rsqrt(jnp.mean(x_float * x_float, axis=-1, keepdims=True) + epsilon)
    normed_one = x_float * rms_one
    hidden_one = gather_tokens((normed_one * gain_one[None, :]).astype(jnp.bfloat16))
    cot_all = gather_tokens(cotangent)
    raw = matmul(hidden_one, attn_w).reshape(group, length, -1)
    cos_table, sin_table = rotary_tables(length, HD)

    def rotary(values):
        return (
            values * cos_table[:, None, :] + rotate_half(values) * sin_table[:, None, :]
        ).astype(jnp.bfloat16)

    def rotary_back(grads):
        return (
            grads * cos_table[:, None, :] + rotate_back(grads * sin_table[:, None, :])
        ).astype(jnp.bfloat16)

    query_rot = rotary(raw[..., :heads_wide].reshape(group, length, heads, HD))
    key_rot = rotary(raw[..., None, heads_wide : heads_wide + HD])[:, :, 0]
    value_rows = raw[..., heads_wide + HD :].astype(jnp.bfloat16)
    causal = jnp.arange(length)[:, None] >= jnp.arange(length)[None, :]

    def product_of(spec, left, right):
        return jnp.einsum(spec, left, right, preferred_element_type=jnp.float32)

    scores = product_of("bigd,bjd->bgij", query_rot, key_rot) * scale_factor
    log_total = jnp.log(jnp.sum(jnp.where(causal, jnp.exp(scores), 0.0), axis=-1))
    weights = jnp.where(causal, jnp.exp(scores - log_total[..., None]), 0.0)
    weights_bf = weights.astype(jnp.bfloat16)
    attended = product_of("bgij,bjd->bigd", weights_bf, value_rows)
    attended = attended.astype(jnp.bfloat16).reshape(group * length, heads_wide)
    mixed_sum = x_float + scatter_tokens(matmul(attended, out_w))

    rms_two = lax.rsqrt(jnp.mean(mixed_sum * mixed_sum, axis=-1, keepdims=True) + epsilon)
    normed_two = mixed_sum * rms_two
    hidden_two = gather_tokens((normed_two * gain_two[None, :]).astype(jnp.bfloat16))
    gate_up = matmul(hidden_two, mlp_w)
    gate_raw, up_raw = gate_up[:, :hidden_wide], gate_up[:, hidden_wide:]
    sigmoid = jax.nn.sigmoid(gate_raw)
    activated = gate_raw * sigmoid
    product = (activated * up_raw).astype(jnp.bfloat16)
    grad_product = contract_last(cot_all, down_w)
    grad_gate = grad_product * up_raw * sigmoid * (1.0 + gate_raw * (1.0 - sigmoid))
    grad_up = grad_product * activated
    grad_both = jnp.concatenate([grad_gate, grad_up], axis=1).astype(jnp.bfloat16)
    grad_hidden_two = scatter_tokens(contract_last(grad_both, mlp_w))
    block_output = (mixed_sum + scatter_tokens(matmul(product, down_w))).astype(jnp.bfloat16)
    down_local = contract_first(product, cot_all).astype(jnp.bfloat16)
    mlp_local = contract_first(hidden_two, grad_both).astype(jnp.bfloat16)

    grad_mixed = cotangent.astype(jnp.float32) + norm_back(
        grad_hidden_two * gain_two[None, :], mixed_sum, rms_two
    )

    grad_mixed_bf = gather_tokens(grad_mixed.astype(jnp.bfloat16))
    grad_attended = contract_last(grad_mixed_bf, out_w).astype(jnp.bfloat16)
    out_local = contract_first(attended, grad_mixed_bf).astype(jnp.bfloat16)
    grad_attended = grad_attended.reshape(group, length, heads, HD)
    grad_weights = product_of("bigd,bjd->bgij", grad_attended, value_rows)
    row_total = jnp.sum(weights * grad_weights, axis=-1, keepdims=True)
    grad_scores = (weights * (grad_weights - row_total) * scale_factor).astype(jnp.bfloat16)
    grad_query = rotary_back(product_of("bgij,bjd->bigd", grad_scores, key_rot))
    grad_key = rotary_back(product_of("bgij,bigd->bjd", grad_scores, query_rot)[:, :, None])
    grad_value = product_of("bgij,bigd->bjd", weights_bf, grad_attended).astype(jnp.bfloat16)
    grad_attn = jnp.concatenate(
        [
            grad_query.reshape(group * length, heads_wide),
            grad_key.reshape(group * length, HD),
            grad_value.reshape(group * length, HD),
        ],
        axis=1,
    )
    grad_hidden_one = scatter_tokens(contract_last(grad_attn, attn_w))
    attn_local = contract_first(hidden_one, grad_attn).astype(jnp.bfloat16)
    input_grad = grad_mixed + norm_back(
        grad_hidden_one * gain_one[None, :], x_float, rms_one
    )

    def to_owner(partial):
        pieces = partial.reshape(high, PAIR, xs, rows, -1)
        pieces = jnp.swapaxes(pieces, 1, 2).reshape(holders, PAIR, rows, -1)
        pieces = swap(scatter_holders(pieces), "zl")
        return lax.all_gather(pieces, "rep", axis=0).astype(jnp.float32)

    def from_holder(values):
        cut = values.reshape(PAIR, rows, high, xs, -1)
        return cut.transpose(1, 2, 0, 3, 4).reshape(rows, -1)

    down_grad = scatter_holders(down_local.reshape(holders, hidden_piece, width))
    down_grad = lax.all_gather(down_grad, "rep", axis=0, tiled=True).astype(jnp.float32)
    mlp_grad = to_owner(mlp_local).reshape(reps, PAIR, rows, 2, holders, hidden_piece)
    mlp_grad = mlp_grad.transpose(3, 1, 2, 4, 0, 5)
    gate_grad, up_grad = from_holder(mlp_grad[0]), from_holder(mlp_grad[1])
    out_padded = jnp.where(
        (jnp.arange(reps) == r)[:, None, None],
        out_local.reshape(1, per_rep * rows, width),
        jnp.zeros((), jnp.bfloat16),
    )
    out_padded = scatter_holders(out_padded.reshape(holders, rows, width))
    out_grad = lax.psum(out_padded, "rep").astype(jnp.float32)
    attn_grad = to_owner(attn_local)
    query_grad = attn_grad[..., :heads_wide].transpose(1, 2, 0, 3)
    query_grad = from_holder(query_grad.reshape(PAIR, rows, holders, -1))
    key_value = attn_grad[..., heads_wide:]

    def key_back(values):
        total = jnp.zeros((KV, rows, HD), jnp.float32)
        for rep in range(reps):
            for low in range(PAIR):
                head = (rep * per_rep // xs) * PAIR + low
                head = head * xs * heads_wide // (per_rep * HD)
                head = head * KV // (query_weight.shape[1] // HD)
                total = total.at[head].add(values[rep, low])
        return total.transpose(1, 0, 2).reshape(rows, -1)

    key_grad, value_grad = key_back(key_value[..., :HD]), key_back(key_value[..., HD:])
    gain_grads = lax.psum(
        jnp.stack(
            [
                jnp.sum(grad_hidden_one * normed_one, axis=0),
                jnp.sum(grad_hidden_two * normed_two, axis=0),
            ]
        ),
        ("rep", "zh", "zl", "x"),
    )
    gain_grads = lax.dynamic_slice_in_dim(gain_grads, shard * rows, rows, axis=1)
    return (
        block_output,
        input_grad,
        query_grad,
        key_grad,
        value_grad,
        out_grad,
        gate_grad,
        up_grad,
        down_grad,
        gain_grads[0],
        gain_grads[1],
    )


def solution(mesh):
    reps, shards = mesh.shape["rep"], mesh.shape["shard"]
    xs = 1
    while 2 * (2 * xs) ** 2 <= shards:
        xs *= 2
    names = ("rep", "zh", "zl", "x")
    cube = Mesh(mesh.devices.reshape(reps, shards // (PAIR * xs), PAIR, xs), names)
    tokens, matrix, vector = P(names, None), P(names[1:], None), P(names[1:])
    in_specs = (tokens, tokens, vector) + (matrix,) * 4 + (vector,) + (matrix,) * 3
    out_specs = (tokens, tokens) + (matrix,) * 7 + (vector,) * 2
    return jax.shard_map(
        per_device, mesh=cube, in_specs=in_specs, out_specs=out_specs, check_vma=False
    )
```

```python
import math

import jax
import jax.numpy as jnp
from jax import lax
from jax.experimental import pallas as pl
from jax.experimental.pallas import tpu as pltpu
from jax.sharding import Mesh, PartitionSpec as P

KV = 4
HD = 64
PAIR = 2
SQUARE_DEVICES = 8
MESH = pl.DeviceIdType.MESH
epsilon = 1e-05

TP = ("rep", "zl")
HOLDERS = ("zh", "x")


def rotary_tables(length, head_size):
    positions = jnp.arange(length, dtype=jnp.float32)[:, None]
    spacing = jnp.arange(head_size // 2, dtype=jnp.float32) * (-2.0 * math.log(10000.0) / head_size)
    angles = positions * jnp.exp(spacing)[None, :]
    cos_table = jnp.cos(angles)
    sin_table = jnp.sin(angles)
    return (
        jnp.concatenate([cos_table, cos_table], axis=-1),
        jnp.concatenate([sin_table, sin_table], axis=-1),
    )


def rotate_half(values):
    middle = values.shape[-1] // 2
    return jnp.concatenate([-values[..., middle:], values[..., :middle]], axis=-1)


def rotate_back(values):
    middle = values.shape[-1] // 2
    return jnp.concatenate([values[..., middle:], -values[..., :middle]], axis=-1)


def norm_back(grad_normed, inputs, scale):
    return scale * grad_normed - inputs * (scale * scale * scale) * jnp.mean(
        grad_normed * inputs, axis=-1, keepdims=True
    )


def matmul(left, right):
    return jnp.dot(left, right, preferred_element_type=jnp.float32)


def contract_last(left, right):
    return lax.dot_general(
        left, right, (((1,), (1,)), ((), ())), preferred_element_type=jnp.float32
    )


def contract_first(left, right):
    return lax.dot_general(
        left, right, (((0,), (0,)), ((), ())), preferred_element_type=jnp.float32
    )


def gather_tokens(rows):
    return lax.all_gather(rows, TP, axis=0, tiled=True)


def scatter_tokens(partial):
    return lax.psum_scatter(
        partial.astype(jnp.bfloat16), TP, scatter_dimension=0, tiled=True
    ).astype(jnp.float32)


SWAP = [(0, 1), (1, 0)]


def swap(pieces, axis):
    first = lax.axis_index(axis) == 0
    came = lax.ppermute(jnp.where(first, pieces[1], pieces[0]), axis, SWAP)
    own = jnp.where(first, pieces[0], pieces[1])
    return jnp.stack([jnp.where(first, own, came), jnp.where(first, came, own)])


def exchange(piece, axis):
    first = lax.axis_index(axis) == 0
    came = lax.ppermute(piece, axis, SWAP)
    return jnp.stack([jnp.where(first, piece, came), jnp.where(first, came, piece)])


def gather_holders(piece):
    if lax.axis_size("zh") == PAIR and lax.axis_size("x") == PAIR:
        both = exchange(exchange(piece, "zh"), "x")
        return jnp.moveaxis(both, 0, 1).reshape((PAIR * PAIR,) + piece.shape)
    return lax.all_gather(piece, HOLDERS, axis=0)


def add(left, right):
    return (left.astype(jnp.float32) + right.astype(jnp.float32)).astype(jnp.bfloat16)


def halve(pieces, axis):
    first = lax.axis_index(axis) == 0
    came = lax.ppermute(jnp.where(first, pieces[1], pieces[0]), axis, SWAP)
    return add(jnp.where(first, pieces[0], pieces[1]), came)


def scatter_holders(partial):
    if lax.axis_size("zh") == PAIR and lax.axis_size("x") == PAIR:
        pieces = jnp.moveaxis(partial.reshape((PAIR, PAIR) + partial.shape[1:]), 1, 0)
        return halve(halve(pieces, "x"), "zh")
    return lax.psum_scatter(partial, HOLDERS, scatter_dimension=0, tiled=False)


def neighbours():
    r, zl = lax.axis_index("rep"), lax.axis_index("zl")
    partner, across = r + 1 - 2 * lax.rem(r, 2), lax.rem(r + 2, 4)
    return {
        "core": {"rep": partner},
        "low": {"zl": 1 - zl},
        "y": {"rep": across},
        "both": {"rep": across, "zl": 1 - zl},
        "x": {"x": 1 - lax.axis_index("x")},
        "high": {"zh": 1 - lax.axis_index("zh")},
    }


def meet(near, names):
    barrier = pltpu.get_barrier_semaphore()
    for name in names:
        pl.semaphore_signal(barrier, 1, device_id=near[name], device_id_type=MESH)
    pl.semaphore_wait(barrier, len(names))


class Wires:
    def __init__(self, near, send, recv, local):
        self.near, self.sems, self.local_sems = near, (send, recv), local
        self.used, self.used_local, self.sent, self.kept = 0, 0, [], []

    def describe(self, source, target, name):
        at = self.used
        self.used += 1
        return pltpu.make_async_remote_copy(
            src_ref=source,
            dst_ref=target,
            send_sem=self.sems[0].at[at],
            recv_sem=self.sems[1].at[at],
            device_id=self.near[name],
            device_id_type=MESH,
        )

    def push(self, source, target, name):
        copy = self.describe(source, target, name)
        copy.start()
        self.sent.append(copy)
        return copy

    def keep(self, source, target):
        copy = pltpu.make_async_copy(source, target, self.local_sems.at[self.used_local])
        self.used_local += 1
        copy.start()
        self.kept.append(copy)
        return copy

    def finish(self):
        for copy in self.sent:
            copy.wait_send()
        for copy in self.kept:
            copy.wait()


class Spread:
    def __init__(self, wires, own, whole):
        self.wires, self.own, self.whole = wires, own, whole
        self.length = own.shape[0]
        r, zl = lax.axis_index("rep"), lax.axis_index("zl")
        self.slots = {
            "own": r * PAIR + zl,
            "low": r * PAIR + 1 - zl,
            "y": lax.rem(r + 2, 4) * PAIR + zl,
            "both": lax.rem(r + 2, 4) * PAIR + 1 - zl,
        }

    def part(self, kind, half=None):
        if half is None:
            return self.whole.at[pl.ds(self.slots[kind] * self.length, self.length)]
        size = self.length // 2
        return self.whole.at[pl.ds(self.slots[kind] * self.length + half * size, size)]

    def start(self, keep=True):
        push, size = self.wires.push, self.length // 2
        halves = [self.own.at[pl.ds(half * size, size)] for half in range(2)]
        self.low = [push(halves[h], self.part("own", h), "low") for h in (0, 1)]
        self.y = [push(halves[h], self.part("own", h), "y") for h in (1, 0)][::-1]
        self.core = push(self.own, self.part("own"), "core")
        if keep:
            self.wires.keep(self.own, self.part("own"))

    def pass_on(self):
        push = self.wires.push
        self.low[0].wait_recv()
        self.first = push(self.part("low", 0), self.part("low", 0), "y")
        self.y[1].wait_recv()
        self.second = push(self.part("y", 1), self.part("y", 1), "low")
        self.low[1].wait_recv()
        self.core_low = push(self.part("low"), self.part("low"), "core")
        self.y[0].wait_recv()
        self.core_y = push(self.part("y"), self.part("y"), "core")

    def last(self):
        self.first.wait_recv()
        self.second.wait_recv()
        self.core_both = self.wires.push(self.part("both"), self.part("both"), "core")

    def end(self):
        for copy in (self.core, self.core_low, self.core_y, self.core_both):
            copy.wait_recv()


SPREAD_COPIES = 10
SQUARE = ("core", "low", "y", "both")


class Gather:
    def __init__(self, near, scratch):
        self.near = near
        self.mine, self.out_core, self.in_core, self.out_far, self.in_far, self.sems = scratch

    def core_copy(self, kind):
        return pltpu.make_async_remote_copy(
            src_ref=self.out_core.at[kind],
            dst_ref=self.in_core.at[kind],
            send_sem=self.sems.at[0, kind],
            recv_sem=self.sems.at[1, kind],
            device_id=self.near["core"],
            device_id_type=MESH,
        )

    def far_copy(self, kind):
        r, zl = lax.axis_index("rep"), lax.axis_index("zl")
        target = {"rep": lax.rem(r + 2 * (kind // 2), 4), "zl": lax.rem(zl + lax.rem(kind, 2), 2)}
        return pltpu.make_async_remote_copy(
            src_ref=self.out_far.at[kind],
            dst_ref=self.in_far.at[kind],
            send_sem=self.sems.at[2, kind],
            recv_sem=self.sems.at[3, kind],
            device_id=target,
            device_id_type=MESH,
        )

    def slot(self, step):
        r, zl = lax.axis_index("rep"), lax.axis_index("zl")
        kind = step // 2
        rep = lax.rem(r + 2 * (kind // 2), 4)
        other = rep + 1 - 2 * lax.rem(rep, 2)
        rep = jnp.where(lax.rem(step, 2) == 0, other, rep)
        return rep * PAIR + lax.rem(zl + lax.rem(kind, 2), 2)

    def put(self, step, partial):
        kind = step // 2
        width = self.mine.shape[1]
        chunk = min(width, 512)

        @pl.when(lax.rem(step, 2) == 0)
        def _():
            for at in range(0, width, chunk):
                columns = slice(at, at + chunk)
                self.out_core[kind, :, columns] = partial(columns).astype(jnp.bfloat16)
            self.core_copy(kind).start()

        @pl.when(lax.rem(step, 2) == 1)
        def _():
            for at in range(0, width, chunk):
                columns = slice(at, at + chunk)
                self.mine[:, columns] = partial(columns)
            self.core_copy(kind).wait_recv()
            total = self.mine[...] + self.in_core[kind].astype(jnp.float32)

            @pl.when(kind == 0)
            def _():
                self.mine_total(total)

            @pl.when(kind > 0)
            def _():
                self.out_far[kind] = total.astype(jnp.bfloat16)
                self.far_copy(kind).start()

    def mine_total(self, total):
        self.out_far[0] = total.astype(jnp.bfloat16)

    def total(self):
        result = self.out_far[0].astype(jnp.float32)
        for kind in range(1, 4):
            self.far_copy(kind).wait_recv()
            result = result + self.in_far[kind].astype(jnp.float32)
        return result

    def finish(self):
        for kind in range(4):
            self.core_copy(kind).wait_send()
        for kind in range(1, 4):
            self.far_copy(kind).wait_send()


def gather_scratch(length, width):
    return [
        pltpu.VMEM((length, width), jnp.float32),
        pltpu.VMEM((4, length, width), jnp.bfloat16),
        pltpu.VMEM((4, length, width), jnp.bfloat16),
        pltpu.VMEM((4, length, width), jnp.bfloat16),
        pltpu.VMEM((4, length, width), jnp.bfloat16),
        pltpu.SemaphoreType.DMA((4, 4)),
    ]


def turn(values, cos_table, sin_table):
    wide = values.shape[1]
    lane = lax.broadcasted_iota(jnp.int32, values.shape, 1)
    other = jnp.where(
        lax.rem(lane, HD) < HD // 2,
        pltpu.roll(values, wide - HD // 2, 1),
        pltpu.roll(values, HD // 2, 1),
    )
    return values * cos_table + other * sin_table


def softmax_rows(query, key, causal, scale):
    scores = contract_last(query, key) * scale
    log_total = jnp.log(jnp.sum(jnp.where(causal, jnp.exp(scores), 0.0), axis=-1, keepdims=True))
    return jnp.where(causal, jnp.exp(scores - log_total), 0.0)


def causal_mask(length):
    rows = lax.broadcasted_iota(jnp.int32, (length, length), 0)
    return rows >= lax.broadcasted_iota(jnp.int32, (length, length), 1)


def forward_kernel(
    x_ref, gain_ref, attn_pack, mlp_pack, down_piece, out_piece, cot_ref, cos_ref, sin_ref,
    attn_w, mlp_w, down_w, out_w, gains, hidden, cot_all, qkv, attended, mixed, hidden_two,
    gain_slots, own_hidden, own_two, send, recv, local, *scratch,
):
    near = neighbours()
    r, zl = lax.axis_index("rep"), lax.axis_index("zl")
    zh, x = lax.axis_index("zh"), lax.axis_index("x")
    length, width = x_ref.shape
    rows, wide = attn_pack.shape[1:]
    heads_wide = wide - 2 * HD
    heads = heads_wide // HD
    deep = down_piece.shape[0]
    wires = Wires(near, send, recv, local)

    def shard(high, low, side):
        return (high * PAIR + low) * PAIR + side

    def slot(ref, high, low, side):
        return ref.at[pl.ds(shard(high, low, side) * rows, rows)]

    def deep_slot(high, side):
        return down_w.at[pl.ds((high * PAIR + side) * deep, deep)]

    meet(near, SQUARE + ("x", "high"))

    gain_own = gain_slots.at[(x * PAIR + zh) * PAIR + zl]
    gain_low = wires.push(gain_ref, gain_own, "low")
    attn_low = wires.push(attn_pack.at[1 - zl], slot(attn_w, zh, zl, x), "low")
    attn_own_high = wires.push(attn_pack.at[zl], slot(attn_w, zh, zl, x), "high")
    attn_own_x = wires.push(attn_pack.at[zl], slot(attn_w, zh, zl, x), "x")
    gain_slots[(x * PAIR + zh) * PAIR + zl] = gain_ref[...]
    wires.keep(attn_pack.at[zl], slot(attn_w, zh, zl, x))
    origin_high, origin_x = r // PAIR, lax.rem(r, PAIR)
    on_side, on_high = x == origin_x, zh == origin_high
    out_high = wires.describe(out_piece, out_w, "high")
    out_x = wires.describe(out_piece, out_w, "x")
    out_x_later = pltpu.make_async_remote_copy(
        src_ref=out_w,
        dst_ref=out_w,
        send_sem=wires.sems[0].at[wires.used - 1],
        recv_sem=wires.sems[1].at[wires.used - 1],
        device_id=near["x"],
        device_id_type=MESH,
    )
    out_keep = pltpu.make_async_copy(out_piece, out_w, local.at[local.shape[0] - 1])

    @pl.when(on_side & on_high)
    def _():
        out_high.start()
        out_x.start()
        out_keep.start()

    x_float = x_ref[...].astype(jnp.float32)
    rms_one = lax.rsqrt(jnp.mean(x_float * x_float, axis=-1, keepdims=True) + epsilon)

    gain_low.wait_recv()
    pair = gain_slots.at[pl.ds((x * PAIR + zh) * PAIR, PAIR)]
    gain_high = wires.push(pair, pair, "high")
    attn_low.wait_recv()
    attn_low_high = wires.push(slot(attn_w, zh, 1 - zl, x), slot(attn_w, zh, 1 - zl, x), "high")
    attn_low_x = wires.push(slot(attn_w, zh, 1 - zl, x), slot(attn_w, zh, 1 - zl, x), "x")
    gain_high.wait_recv()
    quad = gain_slots.at[pl.ds(x * PAIR * PAIR, PAIR * PAIR)]
    gain_x = wires.push(quad, quad, "x")
    gain_x.wait_recv()
    for high in range(PAIR):
        for low in range(PAIR):
            for side in range(PAIR):
                at = shard(high, low, side) * rows
                gains[:, at : at + rows] = gain_slots[(side * PAIR + high) * PAIR + low]

    own_hidden[...] = (x_float * rms_one * gains[0:1, :]).astype(jnp.bfloat16)
    spread = Spread(wires, own_hidden, hidden)
    spread.start(keep=False)
    hidden[pl.ds(spread.slots["own"] * length, length), :] = own_hidden[...]

    attn_own_high.wait_recv()
    attn_high_x = wires.push(slot(attn_w, 1 - zh, zl, x), slot(attn_w, 1 - zh, zl, x), "x")
    attn_low_high.wait_recv()
    attn_both_x = wires.push(slot(attn_w, 1 - zh, 1 - zl, x), slot(attn_w, 1 - zh, 1 - zl, x), "x")

    @pl.when(on_side & jnp.logical_not(on_high))
    def _():
        out_high.wait_recv()
        out_x_later.start()

    for copy in (attn_own_x, attn_low_x, attn_high_x, attn_both_x):
        copy.wait_recv()

    @pl.when(jnp.logical_not(on_side))
    def _():
        out_x.wait_recv()

    @pl.when(on_side & on_high)
    def _():
        out_keep.wait()

    wires.kept.pop(0).wait()

    mlp_own_high = wires.push(mlp_pack.at[zl], slot(mlp_w, zh, zl, x), "high")
    mlp_own_x = wires.push(mlp_pack.at[zl], slot(mlp_w, zh, zl, x), "x")
    down_high = wires.push(down_piece, deep_slot(zh, x), "high")
    down_x = wires.push(down_piece, deep_slot(zh, x), "x")
    wires.keep(mlp_pack.at[zl], slot(mlp_w, zh, zl, x))
    wires.keep(down_piece, deep_slot(zh, x))
    mlp_low = wires.push(mlp_pack.at[1 - zl], slot(mlp_w, zh, zl, x), "low")

    gather = Gather(near, scratch)
    causal = causal_mask(length)
    scale = HD ** (-0.5)

    def sequence(step, _):
        at = pl.multiple_of(gather.slot(step) * length, length)
        raw = matmul(hidden[pl.ds(at, length), :], attn_w[...])
        turned = turn(raw, cos_ref[...], sin_ref[...]).astype(jnp.bfloat16)
        qkv[pl.ds(at, length), :] = turned
        key, value = turned[:, heads_wide : heads_wide + HD], turned[:, heads_wide + HD :]
        outs = []
        for head in range(heads):
            query = turned[:, head * HD : (head + 1) * HD]
            weights = softmax_rows(query, key, causal, scale)
            outs.append(matmul(weights.astype(jnp.bfloat16), value))
        block = jnp.concatenate(outs, axis=1).astype(jnp.bfloat16)
        attended[pl.ds(at, length), :] = block
        gather.put(step, lambda columns: matmul(block, out_w[:, columns]))
        return 0

    spread.core.wait_recv()
    lax.fori_loop(0, 2, sequence, 0)
    spread.pass_on()
    spread.core_low.wait_recv()
    lax.fori_loop(2, 4, sequence, 0)
    mlp_low.wait_recv()
    mlp_low_high = wires.push(slot(mlp_w, zh, 1 - zl, x), slot(mlp_w, zh, 1 - zl, x), "high")
    mlp_low_x = wires.push(slot(mlp_w, zh, 1 - zl, x), slot(mlp_w, zh, 1 - zl, x), "x")
    spread.last()
    spread.core_y.wait_recv()
    spread.core_both.wait_recv()
    cot_spread = Spread(wires, cot_ref, cot_all)
    cot_spread.start()
    lax.fori_loop(4, 8, sequence, 0)
    mixed[...] = x_ref[...].astype(jnp.float32) + gather.total()
    mixed_sum = mixed[...]
    rms_two = lax.rsqrt(jnp.mean(mixed_sum * mixed_sum, axis=-1, keepdims=True) + epsilon)
    own_two[...] = (mixed_sum * rms_two * gains[1:2, :]).astype(jnp.bfloat16)
    two_spread = Spread(wires, own_two, hidden_two)
    two_spread.start()
    cot_spread.pass_on()
    mlp_own_high.wait_recv()
    mlp_high_x = wires.push(slot(mlp_w, 1 - zh, zl, x), slot(mlp_w, 1 - zh, zl, x), "x")
    cot_spread.last()
    two_spread.pass_on()
    two_spread.last()
    down_high.wait_recv()
    down_both_x = wires.push(deep_slot(1 - zh, x), deep_slot(1 - zh, x), "x")
    mlp_low_high.wait_recv()
    mlp_both_x = wires.push(slot(mlp_w, 1 - zh, 1 - zl, x), slot(mlp_w, 1 - zh, 1 - zl, x), "x")
    for copy in (mlp_own_x, mlp_low_x, mlp_high_x, mlp_both_x, down_x, down_both_x):
        copy.wait_recv()
    cot_spread.end()
    two_spread.end()
    gather.finish()

    @pl.when(on_side)
    def _():
        out_x.wait_send()

    @pl.when(on_side & on_high)
    def _():
        out_high.wait_send()

    wires.finish()


FORWARD_COPIES = 60


def forward(x_rows, gain_rows, attn_pack, mlp_pack, down_piece, out_piece, cotangent, tables):
    length, width = x_rows.shape
    group = SQUARE_DEVICES
    rows, wide = attn_pack.shape[1:]
    heads_wide = wide - 2 * HD
    deep = down_piece.shape[0]
    bf16, f32 = jnp.bfloat16, jnp.float32
    shapes = [
        ((width, wide), bf16, True),
        ((width, mlp_pack.shape[2]), bf16, False),
        ((PAIR * PAIR * deep, width), bf16, False),
        ((heads_wide, width), bf16, True),
        ((8, width), f32, True),
        ((group * length, width), bf16, True),
        ((group * length, width), bf16, False),
        ((group * length, wide), bf16, True),
        ((group * length, heads_wide), bf16, True),
        ((length, width), f32, True),
        ((group * length, width), bf16, False),
    ]
    vmem = pl.BlockSpec(memory_space=pltpu.VMEM)
    far = pl.BlockSpec(memory_space=pl.ANY)
    return pl.pallas_call(
        forward_kernel,
        out_shape=[jax.ShapeDtypeStruct(shape, kind) for shape, kind, _ in shapes],
        in_specs=[vmem] * 9,
        out_specs=[vmem if near else far for _, _, near in shapes],
        scratch_shapes=[
            pltpu.VMEM((8, 8, rows), f32),
            pltpu.VMEM((length, width), bf16),
            pltpu.VMEM((length, width), bf16),
            pltpu.SemaphoreType.DMA((FORWARD_COPIES,)),
            pltpu.SemaphoreType.DMA((FORWARD_COPIES,)),
            pltpu.SemaphoreType.DMA((8,)),
        ]
        + gather_scratch(length, width),
        compiler_params=pltpu.CompilerParams(
            collective_id=0, has_side_effects=True, vmem_limit_bytes=60 * 2**20
        ),
        name="forward",
    )(x_rows, gain_rows, attn_pack, mlp_pack, down_piece, out_piece, cotangent, *tables)


def spread_kernel(own, whole, send, recv, local):
    near = neighbours()
    meet(near, SQUARE)
    wires = Wires(near, send, recv, local)
    spread = Spread(wires, own, whole)
    spread.start()
    spread.pass_on()
    spread.last()
    spread.end()
    wires.finish()


def spread_rows(rows, call):
    length, width = rows.shape
    return pl.pallas_call(
        spread_kernel,
        out_shape=jax.ShapeDtypeStruct((SQUARE_DEVICES * length, width), rows.dtype),
        in_specs=[pl.BlockSpec(memory_space=pltpu.VMEM)],
        out_specs=pl.BlockSpec(memory_space=pl.ANY),
        scratch_shapes=[
            pltpu.SemaphoreType.DMA((SPREAD_COPIES,)),
            pltpu.SemaphoreType.DMA((SPREAD_COPIES,)),
            pltpu.SemaphoreType.DMA((1,)),
        ],
        compiler_params=pltpu.CompilerParams(collective_id=call, has_side_effects=True),
        name="spread",
    )(rows)


def gather_kernel(partial, result, *scratch):
    near = neighbours()
    meet(near, SQUARE)
    gather = Gather(near, scratch)
    length = result.shape[0]

    def block(step, _):
        at = pl.multiple_of(gather.slot(step) * length, length)
        gather.put(step, lambda columns: partial[pl.ds(at, length), columns].astype(jnp.float32))
        return 0

    for first in (6, 2, 4, 0):
        lax.fori_loop(first, first + 2, block, 0)
    result[...] = gather.total()
    gather.finish()


def gather_rows(partial, call):
    length, width = partial.shape[0] // SQUARE_DEVICES, partial.shape[1]
    vmem = pl.BlockSpec(memory_space=pltpu.VMEM)
    return pl.pallas_call(
        gather_kernel,
        out_shape=jax.ShapeDtypeStruct((length, width), jnp.float32),
        in_specs=[vmem],
        out_specs=vmem,
        scratch_shapes=gather_scratch(length, width),
        compiler_params=pltpu.CompilerParams(
            collective_id=call, has_side_effects=True, vmem_limit_bytes=40 * 2**20
        ),
        name="gather",
    )(partial)


def per_device(
    block_input,
    cotangent,
    attn_gain,
    query_weight,
    key_weight,
    value_weight,
    out_weight,
    mlp_gain,
    gate_weight,
    up_weight,
    down_weight,
):
    length, width = block_input.shape
    reps, xs = lax.axis_size("rep"), lax.axis_size("x")
    high = lax.axis_size("zh")
    holders = high * xs
    group = reps * PAIR
    r, zl, x = lax.axis_index("rep"), lax.axis_index("zl"), lax.axis_index("x")
    shard = (lax.axis_index("zh") * PAIR + zl) * xs + x
    rows = query_weight.shape[0]
    heads_wide = query_weight.shape[1] // group
    per_rep = holders // reps
    hidden_piece = down_weight.shape[0] // reps
    hidden_wide = holders * hidden_piece
    heads = heads_wide // HD
    scale_factor = HD ** (-0.5)

    def own_rep(values, axis):
        return lax.dynamic_index_in_dim(values, r, axis, keepdims=False)

    def by_holder(values, axis):
        shape = values.shape
        cut = values.reshape(shape[:axis] + (high, PAIR, xs, -1) + shape[axis + 1 :])
        cut = jnp.moveaxis(cut, axis + 1, 0)
        return cut.reshape((PAIR,) + shape[:axis] + (holders, -1) + shape[axis + 1 :])

    def query_columns(weight):
        pieces = by_holder(weight, 1).reshape(PAIR, rows, reps, heads_wide)
        return own_rep(pieces, 2)

    def hidden_columns(weight):
        pieces = by_holder(weight, 1).reshape(PAIR, rows, holders, reps, hidden_piece)
        return own_rep(pieces, 3).reshape(PAIR, rows, hidden_wide)

    key_heads = [
        (((r * per_rep // xs) * PAIR + low) * xs * heads_wide // (per_rep * HD)) * KV
        // (query_weight.shape[1] // HD)
        for low in range(PAIR)
    ]

    def key_columns(weight):
        pieces = weight.reshape(rows, KV, HD)
        return jnp.stack(
            [lax.dynamic_index_in_dim(pieces, k, 1, keepdims=False) for k in key_heads]
        )

    attn_pack = jnp.concatenate(
        [query_columns(query_weight), key_columns(key_weight), key_columns(value_weight)], axis=2
    )
    mlp_pack = jnp.concatenate([hidden_columns(gate_weight), hidden_columns(up_weight)], axis=2)

    gains = lax.all_gather(
        jnp.stack([attn_gain, mlp_gain]), ("zh", "zl", "x"), axis=1, tiled=True
    )
    gains = gains.astype(jnp.float32)
    gain_one, gain_two = gains[0], gains[1]

    def all_rows(pack):
        whole = gather_holders(swap(pack, "zl"))
        whole = whole.reshape((high, xs, PAIR) + whole.shape[2:])
        return jnp.swapaxes(whole, 1, 2).reshape(width, -1)

    attn_w = all_rows(attn_pack)
    out_w = own_rep(gather_holders(out_weight).reshape(reps, per_rep * rows, width), 0)
    down_w = gather_holders(own_rep(down_weight.reshape(reps, hidden_piece, width), 0))
    down_w = down_w.reshape(hidden_wide, width)
    mlp_w = all_rows(mlp_pack)

    x_float = block_input.astype(jnp.float32)
    rms_one = lax.rsqrt(jnp.mean(x_float * x_float, axis=-1, keepdims=True) + epsilon)
    normed_one = x_float * rms_one
    hidden_one = gather_tokens((normed_one * gain_one[None, :]).astype(jnp.bfloat16))
    cot_all = gather_tokens(cotangent)
    raw = matmul(hidden_one, attn_w).reshape(group, length, -1)
    cos_table, sin_table = rotary_tables(length, HD)

    def rotary(values):
        return (
            values * cos_table[:, None, :] + rotate_half(values) * sin_table[:, None, :]
        ).astype(jnp.bfloat16)

    def rotary_back(grads):
        return (
            grads * cos_table[:, None, :] + rotate_back(grads * sin_table[:, None, :])
        ).astype(jnp.bfloat16)

    query_rot = rotary(raw[..., :heads_wide].reshape(group, length, heads, HD))
    key_rot = rotary(raw[..., None, heads_wide : heads_wide + HD])[:, :, 0]
    value_rows = raw[..., heads_wide + HD :].astype(jnp.bfloat16)
    causal = jnp.arange(length)[:, None] >= jnp.arange(length)[None, :]

    def product_of(spec, left, right):
        return jnp.einsum(spec, left, right, preferred_element_type=jnp.float32)

    scores = product_of("bigd,bjd->bgij", query_rot, key_rot) * scale_factor
    log_total = jnp.log(jnp.sum(jnp.where(causal, jnp.exp(scores), 0.0), axis=-1))
    weights = jnp.where(causal, jnp.exp(scores - log_total[..., None]), 0.0)
    weights_bf = weights.astype(jnp.bfloat16)
    attended = product_of("bgij,bjd->bigd", weights_bf, value_rows)
    attended = attended.astype(jnp.bfloat16).reshape(group * length, heads_wide)
    mixed_sum = x_float + scatter_tokens(matmul(attended, out_w))

    rms_two = lax.rsqrt(jnp.mean(mixed_sum * mixed_sum, axis=-1, keepdims=True) + epsilon)
    normed_two = mixed_sum * rms_two
    hidden_two = gather_tokens((normed_two * gain_two[None, :]).astype(jnp.bfloat16))
    gate_up = matmul(hidden_two, mlp_w)
    gate_raw, up_raw = gate_up[:, :hidden_wide], gate_up[:, hidden_wide:]
    sigmoid = jax.nn.sigmoid(gate_raw)
    activated = gate_raw * sigmoid
    product = (activated * up_raw).astype(jnp.bfloat16)
    grad_product = contract_last(cot_all, down_w)
    grad_gate = grad_product * up_raw * sigmoid * (1.0 + gate_raw * (1.0 - sigmoid))
    grad_up = grad_product * activated
    grad_both = jnp.concatenate([grad_gate, grad_up], axis=1).astype(jnp.bfloat16)
    grad_hidden_two = scatter_tokens(contract_last(grad_both, mlp_w))
    block_output = (mixed_sum + scatter_tokens(matmul(product, down_w))).astype(jnp.bfloat16)
    down_local = contract_first(product, cot_all).astype(jnp.bfloat16)
    mlp_local = contract_first(hidden_two, grad_both).astype(jnp.bfloat16)

    grad_mixed = cotangent.astype(jnp.float32) + norm_back(
        grad_hidden_two * gain_two[None, :], mixed_sum, rms_two
    )

    grad_mixed_bf = gather_tokens(grad_mixed.astype(jnp.bfloat16))
    grad_attended = contract_last(grad_mixed_bf, out_w).astype(jnp.bfloat16)
    out_local = contract_first(attended, grad_mixed_bf).astype(jnp.bfloat16)
    grad_attended = grad_attended.reshape(group, length, heads, HD)
    grad_weights = product_of("bigd,bjd->bgij", grad_attended, value_rows)
    row_total = jnp.sum(weights * grad_weights, axis=-1, keepdims=True)
    grad_scores = (weights * (grad_weights - row_total) * scale_factor).astype(jnp.bfloat16)
    grad_query = rotary_back(product_of("bgij,bjd->bigd", grad_scores, key_rot))
    grad_key = rotary_back(product_of("bgij,bigd->bjd", grad_scores, query_rot)[:, :, None])
    grad_value = product_of("bgij,bigd->bjd", weights_bf, grad_attended).astype(jnp.bfloat16)
    grad_attn = jnp.concatenate(
        [
            grad_query.reshape(group * length, heads_wide),
            grad_key.reshape(group * length, HD),
            grad_value.reshape(group * length, HD),
        ],
        axis=1,
    )
    grad_hidden_one = scatter_tokens(contract_last(grad_attn, attn_w))
    attn_local = contract_first(hidden_one, grad_attn).astype(jnp.bfloat16)
    input_grad = grad_mixed + norm_back(
        grad_hidden_one * gain_one[None, :], x_float, rms_one
    )

    def to_owner(partial):
        pieces = partial.reshape(high, PAIR, xs, rows, -1)
        pieces = jnp.swapaxes(pieces, 1, 2).reshape(holders, PAIR, rows, -1)
        pieces = swap(scatter_holders(pieces), "zl")
        return lax.all_gather(pieces, "rep", axis=0).astype(jnp.float32)

    def from_holder(values):
        cut = values.reshape(PAIR, rows, high, xs, -1)
        return cut.transpose(1, 2, 0, 3, 4).reshape(rows, -1)

    down_grad = scatter_holders(down_local.reshape(holders, hidden_piece, width))
    down_grad = lax.all_gather(down_grad, "rep", axis=0, tiled=True).astype(jnp.float32)
    mlp_grad = to_owner(mlp_local).reshape(reps, PAIR, rows, 2, holders, hidden_piece)
    mlp_grad = mlp_grad.transpose(3, 1, 2, 4, 0, 5)
    gate_grad, up_grad = from_holder(mlp_grad[0]), from_holder(mlp_grad[1])
    out_padded = jnp.where(
        (jnp.arange(reps) == r)[:, None, None],
        out_local.reshape(1, per_rep * rows, width),
        jnp.zeros((), jnp.bfloat16),
    )
    out_padded = scatter_holders(out_padded.reshape(holders, rows, width))
    out_grad = lax.psum(out_padded, "rep").astype(jnp.float32)
    attn_grad = to_owner(attn_local)
    query_grad = attn_grad[..., :heads_wide].transpose(1, 2, 0, 3)
    query_grad = from_holder(query_grad.reshape(PAIR, rows, holders, -1))
    key_value = attn_grad[..., heads_wide:]

    def key_back(values):
        total = jnp.zeros((KV, rows, HD), jnp.float32)
        for rep in range(reps):
            for low in range(PAIR):
                head = (rep * per_rep // xs) * PAIR + low
                head = head * xs * heads_wide // (per_rep * HD)
                head = head * KV // (query_weight.shape[1] // HD)
                total = total.at[head].add(values[rep, low])
        return total.transpose(1, 0, 2).reshape(rows, -1)

    key_grad, value_grad = key_back(key_value[..., :HD]), key_back(key_value[..., HD:])
    gain_grads = lax.psum(
        jnp.stack(
            [
                jnp.sum(grad_hidden_one * normed_one, axis=0),
                jnp.sum(grad_hidden_two * normed_two, axis=0),
            ]
        ),
        ("rep", "zh", "zl", "x"),
    )
    gain_grads = lax.dynamic_slice_in_dim(gain_grads, shard * rows, rows, axis=1)
    return (
        block_output,
        input_grad,
        query_grad,
        key_grad,
        value_grad,
        out_grad,
        gate_grad,
        up_grad,
        down_grad,
        gain_grads[0],
        gain_grads[1],
    )


def per_device_square(
    block_input,
    cotangent,
    attn_gain,
    query_weight,
    key_weight,
    value_weight,
    out_weight,
    mlp_gain,
    gate_weight,
    up_weight,
    down_weight,
):
    length, width = block_input.shape
    reps, xs = lax.axis_size("rep"), lax.axis_size("x")
    high = lax.axis_size("zh")
    holders = high * xs
    group = reps * PAIR
    r, zl, x = lax.axis_index("rep"), lax.axis_index("zl"), lax.axis_index("x")
    shard = (lax.axis_index("zh") * PAIR + zl) * xs + x
    rows = query_weight.shape[0]
    heads_wide = query_weight.shape[1] // group
    per_rep = holders // reps
    hidden_piece = down_weight.shape[0] // reps
    hidden_wide = holders * hidden_piece
    heads = heads_wide // HD
    scale_factor = HD ** (-0.5)

    def own_rep(values, axis):
        return lax.dynamic_index_in_dim(values, r, axis, keepdims=False)

    def by_holder(values, axis):
        shape = values.shape
        cut = values.reshape(shape[:axis] + (high, PAIR, xs, -1) + shape[axis + 1 :])
        cut = jnp.moveaxis(cut, axis + 1, 0)
        return cut.reshape((PAIR,) + shape[:axis] + (holders, -1) + shape[axis + 1 :])

    def query_columns(weight):
        pieces = by_holder(weight, 1).reshape(PAIR, rows, reps, heads_wide)
        return own_rep(pieces, 2)

    def hidden_columns(weight):
        pieces = by_holder(weight, 1).reshape(PAIR, rows, holders, reps, hidden_piece)
        return own_rep(pieces, 3).reshape(PAIR, rows, hidden_wide)

    key_heads = [
        (((r * per_rep // xs) * PAIR + low) * xs * heads_wide // (per_rep * HD)) * KV
        // (query_weight.shape[1] // HD)
        for low in range(PAIR)
    ]

    def key_columns(weight):
        pieces = weight.reshape(rows, KV, HD)
        return jnp.stack(
            [lax.dynamic_index_in_dim(pieces, k, 1, keepdims=False) for k in key_heads]
        )

    attn_pack = jnp.concatenate(
        [query_columns(query_weight), key_columns(key_weight), key_columns(value_weight)], axis=2
    )
    mlp_pack = jnp.concatenate([hidden_columns(gate_weight), hidden_columns(up_weight)], axis=2)

    cos_table, sin_table = rotary_tables(length, HD)
    sign = jnp.where(jnp.arange(HD) < HD // 2, -1.0, 1.0)
    turned = heads + 1
    cos_wide = jnp.concatenate([jnp.tile(cos_table, (1, turned)), jnp.ones_like(cos_table)], axis=1)
    sin_wide = jnp.concatenate(
        [jnp.tile(sin_table * sign, (1, turned)), jnp.zeros_like(cos_table)], axis=1
    )
    gain_rows = jnp.zeros((8, rows), jnp.float32)
    gain_rows = gain_rows.at[0].set(attn_gain.astype(jnp.float32))
    gain_rows = gain_rows.at[1].set(mlp_gain.astype(jnp.float32))
    (
        attn_w, mlp_w, down_w, out_w, gains, hidden_one, cot_all, qkv, attended, mixed_sum, hidden_two,
    ) = forward(
        block_input,
        gain_rows,
        attn_pack,
        mlp_pack,
        own_rep(down_weight.reshape(reps, hidden_piece, width), 0),
        out_weight,
        cotangent,
        (cos_wide, sin_wide),
    )
    gain_one, gain_two = gains[0], gains[1]

    x_float = block_input.astype(jnp.float32)
    rms_one = lax.rsqrt(jnp.mean(x_float * x_float, axis=-1, keepdims=True) + epsilon)
    normed_one = x_float * rms_one

    def rotary_back(grads):
        return (
            grads * cos_table[:, None, :] + rotate_back(grads * sin_table[:, None, :])
        ).astype(jnp.bfloat16)

    qkv = qkv.reshape(group, length, -1)
    query_rot = qkv[..., :heads_wide].reshape(group, length, heads, HD)
    key_rot = qkv[..., heads_wide : heads_wide + HD]
    value_rows = qkv[..., heads_wide + HD :]
    causal = jnp.arange(length)[:, None] >= jnp.arange(length)[None, :]

    def product_of(spec, left, right):
        return jnp.einsum(spec, left, right, preferred_element_type=jnp.float32)

    scores = product_of("bigd,bjd->bgij", query_rot, key_rot) * scale_factor
    log_total = jnp.log(jnp.sum(jnp.where(causal, jnp.exp(scores), 0.0), axis=-1))
    weights = jnp.where(causal, jnp.exp(scores - log_total[..., None]), 0.0)
    weights_bf = weights.astype(jnp.bfloat16)

    rms_two = lax.rsqrt(jnp.mean(mixed_sum * mixed_sum, axis=-1, keepdims=True) + epsilon)
    normed_two = mixed_sum * rms_two
    gate_up = matmul(hidden_two, mlp_w)
    gate_raw, up_raw = gate_up[:, :hidden_wide], gate_up[:, hidden_wide:]
    sigmoid = jax.nn.sigmoid(gate_raw)
    activated = gate_raw * sigmoid
    product = (activated * up_raw).astype(jnp.bfloat16)
    grad_product = contract_last(cot_all, down_w)
    grad_gate = grad_product * up_raw * sigmoid * (1.0 + gate_raw * (1.0 - sigmoid))
    grad_up = grad_product * activated
    grad_both = jnp.concatenate([grad_gate, grad_up], axis=1).astype(jnp.bfloat16)
    grad_hidden_two = gather_rows(contract_last(grad_both, mlp_w).astype(jnp.bfloat16), 1)
    block_output = (mixed_sum + gather_rows(matmul(product, down_w).astype(jnp.bfloat16), 2)).astype(jnp.bfloat16)
    down_local = contract_first(product, cot_all).astype(jnp.bfloat16)
    mlp_local = contract_first(hidden_two, grad_both).astype(jnp.bfloat16)

    grad_mixed = cotangent.astype(jnp.float32) + norm_back(
        grad_hidden_two * gain_two[None, :], mixed_sum, rms_two
    )

    grad_mixed_bf = spread_rows(grad_mixed.astype(jnp.bfloat16), 3)
    grad_attended = contract_last(grad_mixed_bf, out_w).astype(jnp.bfloat16)
    out_local = contract_first(attended, grad_mixed_bf).astype(jnp.bfloat16)
    grad_attended = grad_attended.reshape(group, length, heads, HD)
    grad_weights = product_of("bigd,bjd->bgij", grad_attended, value_rows)
    row_total = jnp.sum(weights * grad_weights, axis=-1, keepdims=True)
    grad_scores = (weights * (grad_weights - row_total) * scale_factor).astype(jnp.bfloat16)
    grad_query = rotary_back(product_of("bgij,bjd->bigd", grad_scores, key_rot))
    grad_key = rotary_back(product_of("bgij,bigd->bjd", grad_scores, query_rot)[:, :, None])
    grad_value = product_of("bgij,bigd->bjd", weights_bf, grad_attended).astype(jnp.bfloat16)
    grad_attn = jnp.concatenate(
        [
            grad_query.reshape(group * length, heads_wide),
            grad_key.reshape(group * length, HD),
            grad_value.reshape(group * length, HD),
        ],
        axis=1,
    )
    grad_hidden_one = gather_rows(contract_last(grad_attn, attn_w).astype(jnp.bfloat16), 4)
    attn_local = contract_first(hidden_one, grad_attn).astype(jnp.bfloat16)
    input_grad = grad_mixed + norm_back(
        grad_hidden_one * gain_one[None, :], x_float, rms_one
    )

    def to_owner(partial):
        pieces = partial.reshape(high, PAIR, xs, rows, -1)
        pieces = jnp.swapaxes(pieces, 1, 2).reshape(holders, PAIR, rows, -1)
        pieces = swap(scatter_holders(pieces), "zl")
        return lax.all_gather(pieces, "rep", axis=0).astype(jnp.float32)

    def from_holder(values):
        cut = values.reshape(PAIR, rows, high, xs, -1)
        return cut.transpose(1, 2, 0, 3, 4).reshape(rows, -1)

    down_grad = scatter_holders(down_local.reshape(holders, hidden_piece, width))
    down_grad = lax.all_gather(down_grad, "rep", axis=0, tiled=True).astype(jnp.float32)
    mlp_grad = to_owner(mlp_local).reshape(reps, PAIR, rows, 2, holders, hidden_piece)
    mlp_grad = mlp_grad.transpose(3, 1, 2, 4, 0, 5)
    gate_grad, up_grad = from_holder(mlp_grad[0]), from_holder(mlp_grad[1])
    out_padded = jnp.where(
        (jnp.arange(reps) == r)[:, None, None],
        out_local.reshape(1, per_rep * rows, width),
        jnp.zeros((), jnp.bfloat16),
    )
    out_padded = scatter_holders(out_padded.reshape(holders, rows, width))
    out_grad = lax.psum(out_padded, "rep").astype(jnp.float32)
    attn_grad = to_owner(attn_local)
    query_grad = attn_grad[..., :heads_wide].transpose(1, 2, 0, 3)
    query_grad = from_holder(query_grad.reshape(PAIR, rows, holders, -1))
    key_value = attn_grad[..., heads_wide:]

    def key_back(values):
        total = jnp.zeros((KV, rows, HD), jnp.float32)
        for rep in range(reps):
            for low in range(PAIR):
                head = (rep * per_rep // xs) * PAIR + low
                head = head * xs * heads_wide // (per_rep * HD)
                head = head * KV // (query_weight.shape[1] // HD)
                total = total.at[head].add(values[rep, low])
        return total.transpose(1, 0, 2).reshape(rows, -1)

    key_grad, value_grad = key_back(key_value[..., :HD]), key_back(key_value[..., HD:])
    gain_grads = lax.psum(
        jnp.stack(
            [
                jnp.sum(grad_hidden_one * normed_one, axis=0),
                jnp.sum(grad_hidden_two * normed_two, axis=0),
            ]
        ),
        ("rep", "zh", "zl", "x"),
    )
    gain_grads = lax.dynamic_slice_in_dim(gain_grads, shard * rows, rows, axis=1)
    return (
        block_output,
        input_grad,
        query_grad,
        key_grad,
        value_grad,
        out_grad,
        gate_grad,
        up_grad,
        down_grad,
        gain_grads[0],
        gain_grads[1],
    )


def solution(mesh):
    reps, shards = mesh.shape["rep"], mesh.shape["shard"]
    xs = 1
    while 2 * (2 * xs) ** 2 <= shards:
        xs *= 2
    names = ("rep", "zh", "zl", "x")
    cube = Mesh(mesh.devices.reshape(reps, shards // (PAIR * xs), PAIR, xs), names)
    tokens, matrix, vector = P(names, None), P(names[1:], None), P(names[1:])
    in_specs = (tokens, tokens, vector) + (matrix,) * 4 + (vector,) + (matrix,) * 3
    out_specs = (tokens, tokens) + (matrix,) * 7 + (vector,) * 2
    square = reps == 4 and shards // (PAIR * xs) == PAIR and xs == PAIR
    return jax.shard_map(
        per_device_square if square else per_device, mesh=cube, in_specs=in_specs, out_specs=out_specs, check_vma=False
    )
```

```python
import math

import jax
import jax.numpy as jnp
from jax import lax
from jax.experimental import pallas as pl
from jax.experimental.pallas import tpu as pltpu
from jax.sharding import Mesh, PartitionSpec as P

KV = 4
HD = 64
PAIR = 2
SQUARE_DEVICES = 8
MESH = pl.DeviceIdType.MESH
epsilon = 1e-05

TP = ("rep", "zl")
HOLDERS = ("zh", "x")


def rotary_tables(length, head_size):
    positions = jnp.arange(length, dtype=jnp.float32)[:, None]
    spacing = jnp.arange(head_size // 2, dtype=jnp.float32) * (-2.0 * math.log(10000.0) / head_size)
    angles = positions * jnp.exp(spacing)[None, :]
    cos_table = jnp.cos(angles)
    sin_table = jnp.sin(angles)
    return (
        jnp.concatenate([cos_table, cos_table], axis=-1),
        jnp.concatenate([sin_table, sin_table], axis=-1),
    )


def rotate_half(values):
    middle = values.shape[-1] // 2
    return jnp.concatenate([-values[..., middle:], values[..., :middle]], axis=-1)


def rotate_back(values):
    middle = values.shape[-1] // 2
    return jnp.concatenate([values[..., middle:], -values[..., :middle]], axis=-1)


def norm_back(grad_normed, inputs, scale):
    return scale * grad_normed - inputs * (scale * scale * scale) * jnp.mean(
        grad_normed * inputs, axis=-1, keepdims=True
    )


def matmul(left, right):
    return jnp.dot(left, right, preferred_element_type=jnp.float32)


def contract_last(left, right):
    return lax.dot_general(
        left, right, (((1,), (1,)), ((), ())), preferred_element_type=jnp.float32
    )


def contract_first(left, right):
    return lax.dot_general(
        left, right, (((0,), (0,)), ((), ())), preferred_element_type=jnp.float32
    )


def gather_tokens(rows):
    return lax.all_gather(rows, TP, axis=0, tiled=True)


def scatter_tokens(partial):
    return lax.psum_scatter(
        partial.astype(jnp.bfloat16), TP, scatter_dimension=0, tiled=True
    ).astype(jnp.float32)


SWAP = [(0, 1), (1, 0)]


def swap(pieces, axis):
    first = lax.axis_index(axis) == 0
    came = lax.ppermute(jnp.where(first, pieces[1], pieces[0]), axis, SWAP)
    own = jnp.where(first, pieces[0], pieces[1])
    return jnp.stack([jnp.where(first, own, came), jnp.where(first, came, own)])


def exchange(piece, axis):
    first = lax.axis_index(axis) == 0
    came = lax.ppermute(piece, axis, SWAP)
    return jnp.stack([jnp.where(first, piece, came), jnp.where(first, came, piece)])


def gather_holders(piece):
    if lax.axis_size("zh") == PAIR and lax.axis_size("x") == PAIR:
        both = exchange(exchange(piece, "zh"), "x")
        return jnp.moveaxis(both, 0, 1).reshape((PAIR * PAIR,) + piece.shape)
    return lax.all_gather(piece, HOLDERS, axis=0)


def add(left, right):
    return (left.astype(jnp.float32) + right.astype(jnp.float32)).astype(jnp.bfloat16)


def halve(pieces, axis):
    first = lax.axis_index(axis) == 0
    came = lax.ppermute(jnp.where(first, pieces[1], pieces[0]), axis, SWAP)
    return add(jnp.where(first, pieces[0], pieces[1]), came)


def scatter_holders(partial):
    if lax.axis_size("zh") == PAIR and lax.axis_size("x") == PAIR:
        pieces = jnp.moveaxis(partial.reshape((PAIR, PAIR) + partial.shape[1:]), 1, 0)
        return halve(halve(pieces, "x"), "zh")
    return lax.psum_scatter(partial, HOLDERS, scatter_dimension=0, tiled=False)


def neighbours():
    r, zl = lax.axis_index("rep"), lax.axis_index("zl")
    partner, across = r + 1 - 2 * lax.rem(r, 2), lax.rem(r + 2, 4)
    return {
        "core": {"rep": partner},
        "low": {"zl": 1 - zl},
        "y": {"rep": across},
        "both": {"rep": across, "zl": 1 - zl},
        "x": {"x": 1 - lax.axis_index("x")},
        "high": {"zh": 1 - lax.axis_index("zh")},
    }


def meet(near, names):
    barrier = pltpu.get_barrier_semaphore()
    for name in names:
        pl.semaphore_signal(barrier, 1, device_id=near[name], device_id_type=MESH)
    pl.semaphore_wait(barrier, len(names))


class Wires:
    def __init__(self, near, send, recv, local):
        self.near, self.sems, self.local_sems = near, (send, recv), local
        self.used, self.used_local, self.sent, self.kept = 0, 0, [], []

    def describe(self, source, target, name):
        at = self.used
        self.used += 1
        return pltpu.make_async_remote_copy(
            src_ref=source,
            dst_ref=target,
            send_sem=self.sems[0].at[at],
            recv_sem=self.sems[1].at[at],
            device_id=self.near[name],
            device_id_type=MESH,
        )

    def push(self, source, target, name):
        copy = self.describe(source, target, name)
        copy.start()
        self.sent.append(copy)
        return copy

    def keep(self, source, target):
        copy = pltpu.make_async_copy(source, target, self.local_sems.at[self.used_local])
        self.used_local += 1
        copy.start()
        self.kept.append(copy)
        return copy

    def finish(self):
        for copy in self.sent:
            copy.wait_send()
        for copy in self.kept:
            copy.wait()


class Spread:
    def __init__(self, wires, own, whole):
        self.wires, self.own, self.whole = wires, own, whole
        self.length = own.shape[0]
        r, zl = lax.axis_index("rep"), lax.axis_index("zl")
        self.slots = {
            "own": r * PAIR + zl,
            "low": r * PAIR + 1 - zl,
            "y": lax.rem(r + 2, 4) * PAIR + zl,
            "both": lax.rem(r + 2, 4) * PAIR + 1 - zl,
        }

    def part(self, kind, half=None):
        if half is None:
            return self.whole.at[pl.ds(self.slots[kind] * self.length, self.length)]
        size = self.length // 2
        return self.whole.at[pl.ds(self.slots[kind] * self.length + half * size, size)]

    def start(self, keep=True):
        push, size = self.wires.push, self.length // 2
        halves = [self.own.at[pl.ds(half * size, size)] for half in range(2)]
        self.low = [push(halves[h], self.part("own", h), "low") for h in (0, 1)]
        self.y = [push(halves[h], self.part("own", h), "y") for h in (1, 0)][::-1]
        self.core = push(self.own, self.part("own"), "core")
        if keep:
            self.wires.keep(self.own, self.part("own"))

    def pass_on(self):
        push = self.wires.push
        self.low[0].wait_recv()
        self.first = push(self.part("low", 0), self.part("low", 0), "y")
        self.y[1].wait_recv()
        self.second = push(self.part("y", 1), self.part("y", 1), "low")
        self.low[1].wait_recv()
        self.core_low = push(self.part("low"), self.part("low"), "core")
        self.y[0].wait_recv()
        self.core_y = push(self.part("y"), self.part("y"), "core")

    def last(self):
        self.first.wait_recv()
        self.second.wait_recv()
        self.core_both = self.wires.push(self.part("both"), self.part("both"), "core")

    def end(self):
        for copy in (self.core, self.core_low, self.core_y, self.core_both):
            copy.wait_recv()


SPREAD_COPIES = 10
SQUARE = ("core", "low", "y", "both")


class Gather:
    def __init__(self, near, scratch, source=None):
        self.near, self.source = near, source
        self.mine, self.out_core, self.in_core, self.out_far, self.in_far, self.sems = scratch

    def core_copy(self, kind):
        outgoing = self.out_core.at[kind]
        if self.source is not None:
            length = self.mine.shape[0]
            at = pl.multiple_of(self.slot(2 * kind) * length, length)
            outgoing = self.source.at[pl.ds(at, length)]
        return pltpu.make_async_remote_copy(
            src_ref=outgoing,
            dst_ref=self.in_core.at[kind],
            send_sem=self.sems.at[0, kind],
            recv_sem=self.sems.at[1, kind],
            device_id=self.near["core"],
            device_id_type=MESH,
        )

    def far_copy(self, kind):
        r, zl = lax.axis_index("rep"), lax.axis_index("zl")
        target = {"rep": lax.rem(r + 2 * (kind // 2), 4), "zl": lax.rem(zl + lax.rem(kind, 2), 2)}
        return pltpu.make_async_remote_copy(
            src_ref=self.out_far.at[kind],
            dst_ref=self.in_far.at[kind],
            send_sem=self.sems.at[2, kind],
            recv_sem=self.sems.at[3, kind],
            device_id=target,
            device_id_type=MESH,
        )

    def slot(self, step):
        r, zl = lax.axis_index("rep"), lax.axis_index("zl")
        kind = step // 2
        rep = lax.rem(r + 2 * (kind // 2), 4)
        other = rep + 1 - 2 * lax.rem(rep, 2)
        rep = jnp.where(lax.rem(step, 2) == 0, other, rep)
        return rep * PAIR + lax.rem(zl + lax.rem(kind, 2), 2)

    def put(self, step, partial):
        kind = step // 2
        width = self.mine.shape[1]
        chunk = min(width, 512)

        @pl.when(lax.rem(step, 2) == 0)
        def _():
            for at in range(0, width, chunk) if self.source is None else ():
                columns = slice(at, at + chunk)
                self.out_core[kind, :, columns] = partial(columns).astype(jnp.bfloat16)
            self.core_copy(kind).start()

        @pl.when(lax.rem(step, 2) == 1)
        def _():
            for at in range(0, width, chunk):
                columns = slice(at, at + chunk)
                self.mine[:, columns] = partial(columns)
            self.core_copy(kind).wait_recv()
            total = self.mine[...] + self.in_core[kind].astype(jnp.float32)

            @pl.when(kind == 0)
            def _():
                self.mine_total(total)

            @pl.when(kind > 0)
            def _():
                self.out_far[kind] = total.astype(jnp.bfloat16)
                self.far_copy(kind).start()

    def mine_total(self, total):
        self.out_far[0] = total.astype(jnp.bfloat16)

    def total(self):
        result = self.out_far[0].astype(jnp.float32)
        for kind in range(1, 4):
            self.far_copy(kind).wait_recv()
            result = result + self.in_far[kind].astype(jnp.float32)
        return result

    def finish(self):
        for kind in range(4):
            self.core_copy(kind).wait_send()
        for kind in range(1, 4):
            self.far_copy(kind).wait_send()


def gather_scratch(length, width):
    return [
        pltpu.VMEM((length, width), jnp.float32),
        pltpu.VMEM((4, length, width), jnp.bfloat16),
        pltpu.VMEM((4, length, width), jnp.bfloat16),
        pltpu.VMEM((4, length, width), jnp.bfloat16),
        pltpu.VMEM((4, length, width), jnp.bfloat16),
        pltpu.SemaphoreType.DMA((4, 4)),
    ]


def turn(values, cos_table, sin_table):
    wide = values.shape[1]
    lane = lax.broadcasted_iota(jnp.int32, values.shape, 1)
    other = jnp.where(
        lax.rem(lane, HD) < HD // 2,
        pltpu.roll(values, wide - HD // 2, 1),
        pltpu.roll(values, HD // 2, 1),
    )
    return values * cos_table + other * sin_table


def softmax_rows(query, key, causal, scale):
    scores = contract_last(query, key) * scale
    log_total = jnp.log(jnp.sum(jnp.where(causal, jnp.exp(scores), 0.0), axis=-1, keepdims=True))
    return jnp.where(causal, jnp.exp(scores - log_total), 0.0)


def causal_mask(length):
    rows = lax.broadcasted_iota(jnp.int32, (length, length), 0)
    return rows >= lax.broadcasted_iota(jnp.int32, (length, length), 1)


def forward_kernel(
    x_ref, gain_ref, attn_pack, mlp_pack, down_piece, out_piece, cot_ref, cos_ref, sin_ref,
    attn_w, mlp_w, down_w, out_w, gains, hidden, cot_all, qkv, attended, mixed, hidden_two,
    gain_slots, own_hidden, own_two, send, recv, local, *scratch,
):
    near = neighbours()
    r, zl = lax.axis_index("rep"), lax.axis_index("zl")
    zh, x = lax.axis_index("zh"), lax.axis_index("x")
    length, width = x_ref.shape
    rows, wide = attn_pack.shape[1:]
    heads_wide = wide - 2 * HD
    heads = heads_wide // HD
    deep = down_piece.shape[0]
    wires = Wires(near, send, recv, local)

    def shard(high, low, side):
        return (high * PAIR + low) * PAIR + side

    def slot(ref, high, low, side):
        return ref.at[pl.ds(shard(high, low, side) * rows, rows)]

    def deep_slot(high, side):
        return down_w.at[pl.ds((high * PAIR + side) * deep, deep)]

    meet(near, SQUARE + ("x", "high"))

    gain_own = gain_slots.at[(x * PAIR + zh) * PAIR + zl]
    gain_low = wires.push(gain_ref, gain_own, "low")
    attn_low = wires.push(attn_pack.at[1 - zl], slot(attn_w, zh, zl, x), "low")
    attn_own_high = wires.push(attn_pack.at[zl], slot(attn_w, zh, zl, x), "high")
    attn_own_x = wires.push(attn_pack.at[zl], slot(attn_w, zh, zl, x), "x")
    gain_slots[(x * PAIR + zh) * PAIR + zl] = gain_ref[...]
    wires.keep(attn_pack.at[zl], slot(attn_w, zh, zl, x))
    origin_high, origin_x = r // PAIR, lax.rem(r, PAIR)
    on_side, on_high = x == origin_x, zh == origin_high
    out_high = wires.describe(out_piece, out_w, "high")
    out_x = wires.describe(out_piece, out_w, "x")
    out_x_later = pltpu.make_async_remote_copy(
        src_ref=out_w,
        dst_ref=out_w,
        send_sem=wires.sems[0].at[wires.used - 1],
        recv_sem=wires.sems[1].at[wires.used - 1],
        device_id=near["x"],
        device_id_type=MESH,
    )
    out_keep = pltpu.make_async_copy(out_piece, out_w, local.at[local.shape[0] - 1])

    @pl.when(on_side & on_high)
    def _():
        out_high.start()
        out_x.start()
        out_keep.start()

    x_float = x_ref[...].astype(jnp.float32)
    rms_one = lax.rsqrt(jnp.mean(x_float * x_float, axis=-1, keepdims=True) + epsilon)

    gain_low.wait_recv()
    pair = gain_slots.at[pl.ds((x * PAIR + zh) * PAIR, PAIR)]
    gain_high = wires.push(pair, pair, "high")
    attn_low.wait_recv()
    attn_low_high = wires.push(slot(attn_w, zh, 1 - zl, x), slot(attn_w, zh, 1 - zl, x), "high")
    attn_low_x = wires.push(slot(attn_w, zh, 1 - zl, x), slot(attn_w, zh, 1 - zl, x), "x")
    gain_high.wait_recv()
    quad = gain_slots.at[pl.ds(x * PAIR * PAIR, PAIR * PAIR)]
    gain_x = wires.push(quad, quad, "x")
    gain_x.wait_recv()
    for high in range(PAIR):
        for low in range(PAIR):
            for side in range(PAIR):
                at = shard(high, low, side) * rows
                gains[:, at : at + rows] = gain_slots[(side * PAIR + high) * PAIR + low]

    own_hidden[...] = (x_float * rms_one * gains[0:1, :]).astype(jnp.bfloat16)
    spread = Spread(wires, own_hidden, hidden)
    spread.start(keep=False)
    hidden[pl.ds(spread.slots["own"] * length, length), :] = own_hidden[...]

    attn_own_high.wait_recv()
    attn_high_x = wires.push(slot(attn_w, 1 - zh, zl, x), slot(attn_w, 1 - zh, zl, x), "x")
    attn_low_high.wait_recv()
    attn_both_x = wires.push(slot(attn_w, 1 - zh, 1 - zl, x), slot(attn_w, 1 - zh, 1 - zl, x), "x")

    @pl.when(on_side & jnp.logical_not(on_high))
    def _():
        out_high.wait_recv()
        out_x_later.start()

    for copy in (attn_own_x, attn_low_x, attn_high_x, attn_both_x):
        copy.wait_recv()

    @pl.when(jnp.logical_not(on_side))
    def _():
        out_x.wait_recv()

    @pl.when(on_side & on_high)
    def _():
        out_keep.wait()

    wires.kept.pop(0).wait()

    mlp_own_high = wires.push(mlp_pack.at[zl], slot(mlp_w, zh, zl, x), "high")
    mlp_own_x = wires.push(mlp_pack.at[zl], slot(mlp_w, zh, zl, x), "x")
    down_high = wires.push(down_piece, deep_slot(zh, x), "high")
    down_x = wires.push(down_piece, deep_slot(zh, x), "x")
    wires.keep(mlp_pack.at[zl], slot(mlp_w, zh, zl, x))
    wires.keep(down_piece, deep_slot(zh, x))
    mlp_low = wires.push(mlp_pack.at[1 - zl], slot(mlp_w, zh, zl, x), "low")

    gather = Gather(near, scratch)
    causal = causal_mask(length)
    scale = HD ** (-0.5)

    def sequence(step, _):
        at = pl.multiple_of(gather.slot(step) * length, length)
        raw = matmul(hidden[pl.ds(at, length), :], attn_w[...])
        turned = turn(raw, cos_ref[...], sin_ref[...]).astype(jnp.bfloat16)
        qkv[pl.ds(at, length), :] = turned
        key, value = turned[:, heads_wide : heads_wide + HD], turned[:, heads_wide + HD :]
        outs = []
        for head in range(heads):
            query = turned[:, head * HD : (head + 1) * HD]
            weights = softmax_rows(query, key, causal, scale)
            outs.append(matmul(weights.astype(jnp.bfloat16), value))
        block = jnp.concatenate(outs, axis=1).astype(jnp.bfloat16)
        attended[pl.ds(at, length), :] = block
        gather.put(step, lambda columns: matmul(block, out_w[:, columns]))
        return 0

    spread.core.wait_recv()
    lax.fori_loop(0, 2, sequence, 0)
    spread.pass_on()
    spread.core_low.wait_recv()
    lax.fori_loop(2, 4, sequence, 0)
    mlp_low.wait_recv()
    mlp_low_high = wires.push(slot(mlp_w, zh, 1 - zl, x), slot(mlp_w, zh, 1 - zl, x), "high")
    mlp_low_x = wires.push(slot(mlp_w, zh, 1 - zl, x), slot(mlp_w, zh, 1 - zl, x), "x")
    spread.last()
    spread.core_y.wait_recv()
    spread.core_both.wait_recv()
    cot_spread = Spread(wires, cot_ref, cot_all)
    cot_spread.start()
    lax.fori_loop(4, 8, sequence, 0)
    mixed[...] = x_ref[...].astype(jnp.float32) + gather.total()
    mixed_sum = mixed[...]
    rms_two = lax.rsqrt(jnp.mean(mixed_sum * mixed_sum, axis=-1, keepdims=True) + epsilon)
    own_two[...] = (mixed_sum * rms_two * gains[1:2, :]).astype(jnp.bfloat16)
    two_spread = Spread(wires, own_two, hidden_two)
    two_spread.start()
    cot_spread.pass_on()
    mlp_own_high.wait_recv()
    mlp_high_x = wires.push(slot(mlp_w, 1 - zh, zl, x), slot(mlp_w, 1 - zh, zl, x), "x")
    cot_spread.last()
    two_spread.pass_on()
    two_spread.last()
    down_high.wait_recv()
    down_both_x = wires.push(deep_slot(1 - zh, x), deep_slot(1 - zh, x), "x")
    mlp_low_high.wait_recv()
    mlp_both_x = wires.push(slot(mlp_w, 1 - zh, 1 - zl, x), slot(mlp_w, 1 - zh, 1 - zl, x), "x")
    for copy in (mlp_own_x, mlp_low_x, mlp_high_x, mlp_both_x, down_x, down_both_x):
        copy.wait_recv()
    cot_spread.end()
    two_spread.end()
    gather.finish()

    @pl.when(on_side)
    def _():
        out_x.wait_send()

    @pl.when(on_side & on_high)
    def _():
        out_high.wait_send()

    wires.finish()


FORWARD_COPIES = 60


def forward(x_rows, gain_rows, attn_pack, mlp_pack, down_piece, out_piece, cotangent, tables):
    length, width = x_rows.shape
    group = SQUARE_DEVICES
    rows, wide = attn_pack.shape[1:]
    heads_wide = wide - 2 * HD
    deep = down_piece.shape[0]
    bf16, f32 = jnp.bfloat16, jnp.float32
    shapes = [
        ((width, wide), bf16, True),
        ((width, mlp_pack.shape[2]), bf16, False),
        ((PAIR * PAIR * deep, width), bf16, False),
        ((heads_wide, width), bf16, True),
        ((8, width), f32, True),
        ((group * length, width), bf16, True),
        ((group * length, width), bf16, False),
        ((group * length, wide), bf16, True),
        ((group * length, heads_wide), bf16, True),
        ((length, width), f32, True),
        ((group * length, width), bf16, False),
    ]
    vmem = pl.BlockSpec(memory_space=pltpu.VMEM)
    far = pl.BlockSpec(memory_space=pl.ANY)
    return pl.pallas_call(
        forward_kernel,
        out_shape=[jax.ShapeDtypeStruct(shape, kind) for shape, kind, _ in shapes],
        in_specs=[vmem] * 9,
        out_specs=[vmem if near else far for _, _, near in shapes],
        scratch_shapes=[
            pltpu.VMEM((8, 8, rows), f32),
            pltpu.VMEM((length, width), bf16),
            pltpu.VMEM((length, width), bf16),
            pltpu.SemaphoreType.DMA((FORWARD_COPIES,)),
            pltpu.SemaphoreType.DMA((FORWARD_COPIES,)),
            pltpu.SemaphoreType.DMA((8,)),
        ]
        + gather_scratch(length, width),
        compiler_params=pltpu.CompilerParams(
            collective_id=0, has_side_effects=True, vmem_limit_bytes=60 * 2**20
        ),
        name="forward",
    )(x_rows, gain_rows, attn_pack, mlp_pack, down_piece, out_piece, cotangent, *tables)


def spread_kernel(own, whole, send, recv, local):
    near = neighbours()
    meet(near, SQUARE)
    wires = Wires(near, send, recv, local)
    spread = Spread(wires, own, whole)
    spread.start()
    spread.pass_on()
    spread.last()
    spread.end()
    wires.finish()


def spread_rows(rows, call):
    length, width = rows.shape
    return pl.pallas_call(
        spread_kernel,
        out_shape=jax.ShapeDtypeStruct((SQUARE_DEVICES * length, width), rows.dtype),
        in_specs=[pl.BlockSpec(memory_space=pltpu.VMEM)],
        out_specs=pl.BlockSpec(memory_space=pl.ANY),
        scratch_shapes=[
            pltpu.SemaphoreType.DMA((SPREAD_COPIES,)),
            pltpu.SemaphoreType.DMA((SPREAD_COPIES,)),
            pltpu.SemaphoreType.DMA((1,)),
        ],
        compiler_params=pltpu.CompilerParams(collective_id=call, has_side_effects=True),
        name="spread",
    )(rows)


def gather_kernel(partial, result, *scratch):
    near = neighbours()
    meet(near, SQUARE)
    gather = Gather(near, scratch, partial)
    length = result.shape[0]

    def block(step, _):
        at = pl.multiple_of(gather.slot(step) * length, length)
        gather.put(step, lambda columns: partial[pl.ds(at, length), columns].astype(jnp.float32))
        return 0

    for first in (6, 2, 4, 0):
        lax.fori_loop(first, first + 2, block, 0)
    result[...] = gather.total()
    gather.finish()


def gather_rows(partial, call):
    length, width = partial.shape[0] // SQUARE_DEVICES, partial.shape[1]
    vmem = pl.BlockSpec(memory_space=pltpu.VMEM)
    return pl.pallas_call(
        gather_kernel,
        out_shape=jax.ShapeDtypeStruct((length, width), jnp.float32),
        in_specs=[vmem],
        out_specs=vmem,
        scratch_shapes=gather_scratch(length, width),
        compiler_params=pltpu.CompilerParams(
            collective_id=call, has_side_effects=True, vmem_limit_bytes=40 * 2**20
        ),
        name="gather",
    )(partial)


def backward_kernel(
    partial, mlp_local, down_local, hidden, attn_w, out_w, qkv, attended, mixed, cot_ref, x_ref,
    gains, cos_ref, sin_ref,
    mlp_out, down_out, attn_out, out_out, input_grad, gain_grads,
    mlp_x, down_x, attn_x, out_x, mlp_high, down_high, attn_high, out_high, gain_in,
    own_mixed, grad_mixed, grad_attn, attn_local, out_local, send, recv, local,
    mine, out_core, in_core, out_far, in_far, sems_two, sems_one,
):
    near = neighbours()
    r, zl = lax.axis_index("rep"), lax.axis_index("zl")
    zh, x = lax.axis_index("zh"), lax.axis_index("x")
    length, width = x_ref.shape
    wide = attn_w.shape[1]
    rows = mlp_x.shape[1]
    heads_wide = wide - 2 * HD
    heads = heads_wide // HD
    deep = down_x.shape[1]
    wires = Wires(near, send, recv, local)
    push = wires.push
    float32, bf16 = jnp.float32, jnp.bfloat16

    def slot(ref, high, low, side):
        return ref.at[pl.ds(pl.multiple_of(((high * PAIR + low) * PAIR + side) * rows, 16), rows)]

    def deep_slot(high, side):
        return down_local.at[pl.ds(pl.multiple_of((high * PAIR + side) * deep, 16), deep)]

    def add_into(target, *others):
        total = target[...].astype(float32)
        for other in others:
            total = total + other[...].astype(float32)
        target[...] = total.astype(bf16)

    meet(near, SQUARE + ("x", "high"))

    mlp_x_copies, down_x_copies = {}, {}
    for at, high in ((0, 1 - zh), (1, zh)):
        for lower, low in ((0, 1 - zl), (1, zl)):
            mlp_x_copies[at, lower] = push(
                slot(mlp_local, high, low, 1 - x), mlp_x.at[2 * at + lower], "x"
            )
        down_x_copies[at] = push(deep_slot(high, 1 - x), down_x.at[at], "x")

    def to_high(lower, low):
        mlp_x_copies[0, lower].wait_recv()
        add_into(mlp_x.at[lower], slot(mlp_local, 1 - zh, low, x))
        return push(mlp_x.at[lower], mlp_high.at[lower], "high")

    gather = Gather(near, (mine, out_core, in_core, out_far, in_far, sems_two), partial)

    def block(step, _):
        at = pl.multiple_of(gather.slot(step) * length, length)
        gather.put(step, lambda columns: partial[pl.ds(at, length), columns].astype(float32))
        return 0

    for first in (6, 2, 4, 0):
        lax.fori_loop(first, first + 2, block, 0)
    grad_hidden = gather.total()
    mixed_sum = mixed[...]
    rms_two = lax.rsqrt(jnp.mean(mixed_sum * mixed_sum, axis=-1, keepdims=True) + epsilon)
    gain_grads[1:2, :] = jnp.sum(grad_hidden * (mixed_sum * rms_two), axis=0, keepdims=True)
    grad = cot_ref[...].astype(float32) + norm_back(
        grad_hidden * gains[1:2, :], mixed_sum, rms_two
    )
    input_grad[...] = grad
    own_mixed[...] = grad.astype(bf16)
    spread = Spread(wires, own_mixed, grad_mixed)
    spread.start(keep=False)
    grad_mixed[pl.ds(pl.multiple_of(spread.slots["own"] * length, length), length), :] = own_mixed[...]
    gather.finish()
    mlp_high_copies = [to_high(0, 1 - zl)]

    gather = Gather(near, (mine, out_core, in_core, out_far, in_far, sems_one))
    causal = causal_mask(length)
    scale = HD ** (-0.5)

    def sequence(step, _):
        at = pl.multiple_of(gather.slot(step) * length, length)
        here = pl.ds(at, length)
        grad_out = contract_last(grad_mixed[here, :], out_w[...]).astype(bf16)
        turned = qkv[here, :]
        key, value = turned[:, heads_wide : heads_wide + HD], turned[:, heads_wide + HD :]
        grads = []
        grad_key = jnp.zeros((length, HD), float32)
        grad_value = jnp.zeros((length, HD), float32)
        for head in range(heads):
            own = slice(head * HD, (head + 1) * HD)
            query, upper = turned[:, own], grad_out[:, own]
            weights = softmax_rows(query, key, causal, scale)
            grad_weights = contract_last(upper, value)
            row_total = jnp.sum(weights * grad_weights, axis=-1, keepdims=True)
            grad_scores = (weights * (grad_weights - row_total) * scale).astype(bf16)
            grads.append(matmul(grad_scores, key))
            grad_key = grad_key + contract_first(grad_scores, query)
            grad_value = grad_value + contract_first(weights.astype(bf16), upper)
        grads = jnp.concatenate(grads + [grad_key, grad_value], axis=1)
        grads = turn(grads, cos_ref[...], -sin_ref[...]).astype(bf16)
        grad_attn[here, :] = grads
        gather.put(step, lambda columns: contract_last(grads, attn_w[columns, :]))
        return 0

    spread.core.wait_recv()
    lax.fori_loop(0, 2, sequence, 0)
    spread.pass_on()
    mlp_high_copies.append(to_high(1, zl))
    spread.core_low.wait_recv()
    lax.fori_loop(2, 4, sequence, 0)
    spread.last()
    down_x_copies[0].wait_recv()
    add_into(down_x.at[0], deep_slot(1 - zh, x))
    down_high_copy = push(down_x.at[0], down_high, "high")
    spread.core_y.wait_recv()
    spread.core_both.wait_recv()
    lax.fori_loop(4, 8, sequence, 0)

    def own_columns(at, _):
        here = pl.ds(pl.multiple_of(at * rows, rows), rows)
        attn_local[here, :] = contract_first(hidden[:, here], grad_attn[...]).astype(bf16)
        return 0

    lax.fori_loop(0, width // rows, own_columns, 0)
    attn_x_copies = {}
    for at, high in ((0, 1 - zh), (1, zh)):
        for lower, low in ((0, 1 - zl), (1, zl)):
            attn_x_copies[at, lower] = push(
                slot(attn_local, high, low, 1 - x), attn_x.at[2 * at + lower], "x"
            )

    def out_columns(at, _):
        here = pl.ds(pl.multiple_of(at * 512, 512), 512)
        out_local[:, here] = contract_first(attended[...], grad_mixed[:, here]).astype(bf16)
        return 0

    lax.fori_loop(0, width // 512, out_columns, 0)
    on_side, on_high = x == lax.rem(r, PAIR), zh == r // PAIR
    out_x_copy = wires.describe(out_local, out_x, "x")
    out_high_copy = wires.describe(out_local, out_high, "high")

    @pl.when(jnp.logical_not(on_side))
    def _():
        out_x_copy.start()

    def to_group(out, piece_rows, column, forward):
        here = out.at[pl.ds(pl.multiple_of(column * piece_rows, 16), piece_rows)]
        return push(here, here, "y"), push(here, here, "core")

    column_own, column_low = r * PAIR + zl, r * PAIR + 1 - zl
    across = lax.rem(r + 2, 4)

    def entry(out, column, size):
        return out.at[pl.ds(pl.multiple_of(column * size, 16), size)]

    def finish_first(x_copy, in_x, part, high_copy, in_high, out):
        x_copy.wait_recv()
        high_copy.wait_recv()
        add_into(in_x, part, in_high)
        return push(in_x, entry(out, column_own, rows), "low")

    def finish_second(x_copy, in_x, part, high_copy, in_high, out, column, size):
        x_copy.wait_recv()
        high_copy.wait_recv()
        add_into(in_x, part, in_high)
        target = entry(out, column, size)
        wires.keep(in_x, target)
        return push(in_x, target, "y"), push(in_x, target, "core")

    mlp_low = finish_first(
        mlp_x_copies[1, 0], mlp_x.at[2], slot(mlp_local, zh, 1 - zl, x),
        mlp_high_copies[0], mlp_high.at[0], mlp_out,
    )

    grad_hidden = gather.total()
    x_float = x_ref[...].astype(float32)
    rms_one = lax.rsqrt(jnp.mean(x_float * x_float, axis=-1, keepdims=True) + epsilon)
    gain_grads[0:1, :] = jnp.sum(grad_hidden * (x_float * rms_one), axis=0, keepdims=True)
    input_grad[...] = input_grad[...] + norm_back(grad_hidden * gains[0:1, :], x_float, rms_one)
    gain_grads[2:8, :] = jnp.zeros((6, width), float32)

    attn_high_copies = []
    for lower, low in ((0, 1 - zl), (1, zl)):
        attn_x_copies[0, lower].wait_recv()
        add_into(attn_x.at[lower], slot(attn_local, 1 - zh, low, x))
        attn_high_copies.append(push(attn_x.at[lower], attn_high.at[lower], "high"))

    @pl.when(on_side)
    def _():
        out_x_copy.wait_recv()
        add_into(out_local, out_x)

        @pl.when(jnp.logical_not(on_high))
        def _():
            out_high_copy.start()

    mlp_second = finish_second(
        mlp_x_copies[1, 1], mlp_x.at[3], slot(mlp_local, zh, zl, x),
        mlp_high_copies[1], mlp_high.at[1], mlp_out, column_own, rows,
    )
    for at, name in enumerate(("x", "high", "low", "y", "core")):
        copy = push(gain_grads, gain_in.at[at], name)
        copy.wait()
        wires.sent.pop()
        gain_grads[...] = gain_grads[...] + gain_in[at]
    mlp_low.wait_recv()
    mlp_third = to_group(mlp_out, rows, column_low, None)
    down_second = finish_second(
        down_x_copies[1], down_x.at[1], deep_slot(zh, x),
        down_high_copy, down_high, down_out, r, deep,
    )
    mlp_second[0].wait_recv()
    here = entry(mlp_out, across * PAIR + zl, rows)
    last = [push(here, here, "core")]
    mlp_third[0].wait_recv()
    here = entry(mlp_out, across * PAIR + 1 - zl, rows)
    last.append(push(here, here, "core"))
    attn_low = finish_first(
        attn_x_copies[1, 0], attn_x.at[2], slot(attn_local, zh, 1 - zl, x),
        attn_high_copies[0], attn_high.at[0], attn_out,
    )
    attn_second = finish_second(
        attn_x_copies[1, 1], attn_x.at[3], slot(attn_local, zh, zl, x),
        attn_high_copies[1], attn_high.at[1], attn_out, column_own, rows,
    )

    holder = zh * PAIR + x
    role = lax.rem(r - holder + 4, 4)
    is_core = r == holder + 1 - 2 * lax.rem(holder, 2)
    is_y = role == 2
    out_core_copy = wires.describe(out_local, out_out, "core")
    out_y_copy = wires.describe(out_local, out_out, "y")
    out_y_later = pltpu.make_async_remote_copy(
        src_ref=out_out,
        dst_ref=out_out,
        send_sem=send.at[wires.used - 1],
        recv_sem=recv.at[wires.used - 1],
        device_id=near["y"],
        device_id_type=MESH,
    )
    out_keep = pltpu.make_async_copy(out_local, out_out, local.at[local.shape[0] - 1])

    @pl.when(role == 0)
    def _():
        out_high_copy.wait_recv()
        add_into(out_local, out_high)
        out_core_copy.start()
        out_y_copy.start()
        out_keep.start()

    attn_low.wait_recv()
    attn_third = to_group(attn_out, rows, column_low, None)
    down_second[0].wait_recv()
    here = entry(down_out, across, deep)
    last.append(push(here, here, "core"))
    attn_second[0].wait_recv()
    here = entry(attn_out, across * PAIR + zl, rows)
    last.append(push(here, here, "core"))

    @pl.when(is_core)
    def _():
        out_core_copy.wait_recv()
        out_y_later.start()

    attn_third[0].wait_recv()
    here = entry(attn_out, across * PAIR + 1 - zl, rows)
    last.append(push(here, here, "core"))

    @pl.when((role != 0) & jnp.logical_not(is_core))
    def _():
        out_y_copy.wait_recv()

    for copy in (mlp_second[1], mlp_third[1], down_second[1], attn_second[1], attn_third[1], *last):
        copy.wait_recv()

    @pl.when(role == 0)
    def _():
        out_core_copy.wait_send()
        out_y_copy.wait_send()
        out_keep.wait()

    @pl.when(is_core)
    def _():
        out_y_later.wait_send()

    @pl.when(jnp.logical_not(on_side))
    def _():
        out_x_copy.wait_send()

    @pl.when(on_side & jnp.logical_not(on_high))
    def _():
        out_high_copy.wait_send()

    gather.finish()
    wires.finish()


BACKWARD_COPIES = 64


def backward(partial, mlp_local, down_local, saved, x_rows, cotangent, tables):
    hidden, attn_w, out_w, qkv, attended, mixed, gains = saved
    length, width = x_rows.shape
    rows = width // SQUARE_DEVICES
    wide, mlp_wide = attn_w.shape[1], mlp_local.shape[1]
    heads_wide = wide - 2 * HD
    deep = down_local.shape[0] // (PAIR * PAIR)
    bf16, f32 = jnp.bfloat16, jnp.float32
    shapes = [
        ((width, mlp_wide), bf16, False),
        ((PAIR * PAIR * deep, width), bf16, False),
        ((width, wide), bf16, False),
        ((heads_wide, width), bf16, False),
        ((length, width), f32, True),
        ((8, width), f32, True),
    ]
    vmem = pl.BlockSpec(memory_space=pltpu.VMEM)
    far = pl.BlockSpec(memory_space=pl.ANY)
    return pl.pallas_call(
        backward_kernel,
        out_shape=[jax.ShapeDtypeStruct(shape, kind) for shape, kind, _ in shapes],
        in_specs=[vmem] * 14,
        out_specs=[vmem if near else far for _, _, near in shapes],
        scratch_shapes=[
            pltpu.VMEM((4, rows, mlp_wide), bf16),
            pltpu.VMEM((2, deep, width), bf16),
            pltpu.VMEM((4, rows, wide), bf16),
            pltpu.VMEM((heads_wide, width), bf16),
            pltpu.VMEM((2, rows, mlp_wide), bf16),
            pltpu.VMEM((deep, width), bf16),
            pltpu.VMEM((2, rows, wide), bf16),
            pltpu.VMEM((heads_wide, width), bf16),
            pltpu.VMEM((5, 8, width), f32),
            pltpu.VMEM((length, width), bf16),
            pltpu.VMEM((SQUARE_DEVICES * length, width), bf16),
            pltpu.VMEM((SQUARE_DEVICES * length, wide), bf16),
            pltpu.VMEM((width, wide), bf16),
            pltpu.VMEM((heads_wide, width), bf16),
            pltpu.SemaphoreType.DMA((BACKWARD_COPIES,)),
            pltpu.SemaphoreType.DMA((BACKWARD_COPIES,)),
            pltpu.SemaphoreType.DMA((8,)),
        ]
        + gather_scratch(length, width)
        + [pltpu.SemaphoreType.DMA((4, 4))],
        compiler_params=pltpu.CompilerParams(
            collective_id=5, has_side_effects=True, vmem_limit_bytes=63 * 2**20
        ),
        name="backward",
    )(
        partial, mlp_local, down_local, hidden, attn_w, out_w, qkv, attended, mixed, cotangent,
        x_rows, gains, *tables,
    )


def per_device(
    block_input,
    cotangent,
    attn_gain,
    query_weight,
    key_weight,
    value_weight,
    out_weight,
    mlp_gain,
    gate_weight,
    up_weight,
    down_weight,
):
    length, width = block_input.shape
    reps, xs = lax.axis_size("rep"), lax.axis_size("x")
    high = lax.axis_size("zh")
    holders = high * xs
    group = reps * PAIR
    r, zl, x = lax.axis_index("rep"), lax.axis_index("zl"), lax.axis_index("x")
    shard = (lax.axis_index("zh") * PAIR + zl) * xs + x
    rows = query_weight.shape[0]
    heads_wide = query_weight.shape[1] // group
    per_rep = holders // reps
    hidden_piece = down_weight.shape[0] // reps
    hidden_wide = holders * hidden_piece
    heads = heads_wide // HD
    scale_factor = HD ** (-0.5)

    def own_rep(values, axis):
        return lax.dynamic_index_in_dim(values, r, axis, keepdims=False)

    def by_holder(values, axis):
        shape = values.shape
        cut = values.reshape(shape[:axis] + (high, PAIR, xs, -1) + shape[axis + 1 :])
        cut = jnp.moveaxis(cut, axis + 1, 0)
        return cut.reshape((PAIR,) + shape[:axis] + (holders, -1) + shape[axis + 1 :])

    def query_columns(weight):
        pieces = by_holder(weight, 1).reshape(PAIR, rows, reps, heads_wide)
        return own_rep(pieces, 2)

    def hidden_columns(weight):
        pieces = by_holder(weight, 1).reshape(PAIR, rows, holders, reps, hidden_piece)
        return own_rep(pieces, 3).reshape(PAIR, rows, hidden_wide)

    key_heads = [
        (((r * per_rep // xs) * PAIR + low) * xs * heads_wide // (per_rep * HD)) * KV
        // (query_weight.shape[1] // HD)
        for low in range(PAIR)
    ]

    def key_columns(weight):
        pieces = weight.reshape(rows, KV, HD)
        return jnp.stack(
            [lax.dynamic_index_in_dim(pieces, k, 1, keepdims=False) for k in key_heads]
        )

    attn_pack = jnp.concatenate(
        [query_columns(query_weight), key_columns(key_weight), key_columns(value_weight)], axis=2
    )
    mlp_pack = jnp.concatenate([hidden_columns(gate_weight), hidden_columns(up_weight)], axis=2)

    gains = lax.all_gather(
        jnp.stack([attn_gain, mlp_gain]), ("zh", "zl", "x"), axis=1, tiled=True
    )
    gains = gains.astype(jnp.float32)
    gain_one, gain_two = gains[0], gains[1]

    def all_rows(pack):
        whole = gather_holders(swap(pack, "zl"))
        whole = whole.reshape((high, xs, PAIR) + whole.shape[2:])
        return jnp.swapaxes(whole, 1, 2).reshape(width, -1)

    attn_w = all_rows(attn_pack)
    out_w = own_rep(gather_holders(out_weight).reshape(reps, per_rep * rows, width), 0)
    down_w = gather_holders(own_rep(down_weight.reshape(reps, hidden_piece, width), 0))
    down_w = down_w.reshape(hidden_wide, width)
    mlp_w = all_rows(mlp_pack)

    x_float = block_input.astype(jnp.float32)
    rms_one = lax.rsqrt(jnp.mean(x_float * x_float, axis=-1, keepdims=True) + epsilon)
    normed_one = x_float * rms_one
    hidden_one = gather_tokens((normed_one * gain_one[None, :]).astype(jnp.bfloat16))
    cot_all = gather_tokens(cotangent)
    raw = matmul(hidden_one, attn_w).reshape(group, length, -1)
    cos_table, sin_table = rotary_tables(length, HD)

    def rotary(values):
        return (
            values * cos_table[:, None, :] + rotate_half(values) * sin_table[:, None, :]
        ).astype(jnp.bfloat16)

    def rotary_back(grads):
        return (
            grads * cos_table[:, None, :] + rotate_back(grads * sin_table[:, None, :])
        ).astype(jnp.bfloat16)

    query_rot = rotary(raw[..., :heads_wide].reshape(group, length, heads, HD))
    key_rot = rotary(raw[..., None, heads_wide : heads_wide + HD])[:, :, 0]
    value_rows = raw[..., heads_wide + HD :].astype(jnp.bfloat16)
    causal = jnp.arange(length)[:, None] >= jnp.arange(length)[None, :]

    def product_of(spec, left, right):
        return jnp.einsum(spec, left, right, preferred_element_type=jnp.float32)

    scores = product_of("bigd,bjd->bgij", query_rot, key_rot) * scale_factor
    log_total = jnp.log(jnp.sum(jnp.where(causal, jnp.exp(scores), 0.0), axis=-1))
    weights = jnp.where(causal, jnp.exp(scores - log_total[..., None]), 0.0)
    weights_bf = weights.astype(jnp.bfloat16)
    attended = product_of("bgij,bjd->bigd", weights_bf, value_rows)
    attended = attended.astype(jnp.bfloat16).reshape(group * length, heads_wide)
    mixed_sum = x_float + scatter_tokens(matmul(attended, out_w))

    rms_two = lax.rsqrt(jnp.mean(mixed_sum * mixed_sum, axis=-1, keepdims=True) + epsilon)
    normed_two = mixed_sum * rms_two
    hidden_two = gather_tokens((normed_two * gain_two[None, :]).astype(jnp.bfloat16))
    gate_up = matmul(hidden_two, mlp_w)
    gate_raw, up_raw = gate_up[:, :hidden_wide], gate_up[:, hidden_wide:]
    sigmoid = jax.nn.sigmoid(gate_raw)
    activated = gate_raw * sigmoid
    product = (activated * up_raw).astype(jnp.bfloat16)
    grad_product = contract_last(cot_all, down_w)
    grad_gate = grad_product * up_raw * sigmoid * (1.0 + gate_raw * (1.0 - sigmoid))
    grad_up = grad_product * activated
    grad_both = jnp.concatenate([grad_gate, grad_up], axis=1).astype(jnp.bfloat16)
    grad_hidden_two = scatter_tokens(contract_last(grad_both, mlp_w))
    block_output = (mixed_sum + scatter_tokens(matmul(product, down_w))).astype(jnp.bfloat16)
    down_local = contract_first(product, cot_all).astype(jnp.bfloat16)
    mlp_local = contract_first(hidden_two, grad_both).astype(jnp.bfloat16)

    grad_mixed = cotangent.astype(jnp.float32) + norm_back(
        grad_hidden_two * gain_two[None, :], mixed_sum, rms_two
    )

    grad_mixed_bf = gather_tokens(grad_mixed.astype(jnp.bfloat16))
    grad_attended = contract_last(grad_mixed_bf, out_w).astype(jnp.bfloat16)
    out_local = contract_first(attended, grad_mixed_bf).astype(jnp.bfloat16)
    grad_attended = grad_attended.reshape(group, length, heads, HD)
    grad_weights = product_of("bigd,bjd->bgij", grad_attended, value_rows)
    row_total = jnp.sum(weights * grad_weights, axis=-1, keepdims=True)
    grad_scores = (weights * (grad_weights - row_total) * scale_factor).astype(jnp.bfloat16)
    grad_query = rotary_back(product_of("bgij,bjd->bigd", grad_scores, key_rot))
    grad_key = rotary_back(product_of("bgij,bigd->bjd", grad_scores, query_rot)[:, :, None])
    grad_value = product_of("bgij,bigd->bjd", weights_bf, grad_attended).astype(jnp.bfloat16)
    grad_attn = jnp.concatenate(
        [
            grad_query.reshape(group * length, heads_wide),
            grad_key.reshape(group * length, HD),
            grad_value.reshape(group * length, HD),
        ],
        axis=1,
    )
    grad_hidden_one = scatter_tokens(contract_last(grad_attn, attn_w))
    attn_local = contract_first(hidden_one, grad_attn).astype(jnp.bfloat16)
    input_grad = grad_mixed + norm_back(
        grad_hidden_one * gain_one[None, :], x_float, rms_one
    )

    def to_owner(partial):
        pieces = partial.reshape(high, PAIR, xs, rows, -1)
        pieces = jnp.swapaxes(pieces, 1, 2).reshape(holders, PAIR, rows, -1)
        pieces = swap(scatter_holders(pieces), "zl")
        return lax.all_gather(pieces, "rep", axis=0).astype(jnp.float32)

    def from_holder(values):
        cut = values.reshape(PAIR, rows, high, xs, -1)
        return cut.transpose(1, 2, 0, 3, 4).reshape(rows, -1)

    down_grad = scatter_holders(down_local.reshape(holders, hidden_piece, width))
    down_grad = lax.all_gather(down_grad, "rep", axis=0, tiled=True).astype(jnp.float32)
    mlp_grad = to_owner(mlp_local).reshape(reps, PAIR, rows, 2, holders, hidden_piece)
    mlp_grad = mlp_grad.transpose(3, 1, 2, 4, 0, 5)
    gate_grad, up_grad = from_holder(mlp_grad[0]), from_holder(mlp_grad[1])
    out_padded = jnp.where(
        (jnp.arange(reps) == r)[:, None, None],
        out_local.reshape(1, per_rep * rows, width),
        jnp.zeros((), jnp.bfloat16),
    )
    out_padded = scatter_holders(out_padded.reshape(holders, rows, width))
    out_grad = lax.psum(out_padded, "rep").astype(jnp.float32)
    attn_grad = to_owner(attn_local)
    query_grad = attn_grad[..., :heads_wide].transpose(1, 2, 0, 3)
    query_grad = from_holder(query_grad.reshape(PAIR, rows, holders, -1))
    key_value = attn_grad[..., heads_wide:]

    def key_back(values):
        total = jnp.zeros((KV, rows, HD), jnp.float32)
        for rep in range(reps):
            for low in range(PAIR):
                head = (rep * per_rep // xs) * PAIR + low
                head = head * xs * heads_wide // (per_rep * HD)
                head = head * KV // (query_weight.shape[1] // HD)
                total = total.at[head].add(values[rep, low])
        return total.transpose(1, 0, 2).reshape(rows, -1)

    key_grad, value_grad = key_back(key_value[..., :HD]), key_back(key_value[..., HD:])
    gain_grads = lax.psum(
        jnp.stack(
            [
                jnp.sum(grad_hidden_one * normed_one, axis=0),
                jnp.sum(grad_hidden_two * normed_two, axis=0),
            ]
        ),
        ("rep", "zh", "zl", "x"),
    )
    gain_grads = lax.dynamic_slice_in_dim(gain_grads, shard * rows, rows, axis=1)
    return (
        block_output,
        input_grad,
        query_grad,
        key_grad,
        value_grad,
        out_grad,
        gate_grad,
        up_grad,
        down_grad,
        gain_grads[0],
        gain_grads[1],
    )


def per_device_square(
    block_input,
    cotangent,
    attn_gain,
    query_weight,
    key_weight,
    value_weight,
    out_weight,
    mlp_gain,
    gate_weight,
    up_weight,
    down_weight,
):
    length, width = block_input.shape
    reps, xs = lax.axis_size("rep"), lax.axis_size("x")
    high = lax.axis_size("zh")
    holders = high * xs
    group = reps * PAIR
    r, zl, x = lax.axis_index("rep"), lax.axis_index("zl"), lax.axis_index("x")
    shard = (lax.axis_index("zh") * PAIR + zl) * xs + x
    rows = query_weight.shape[0]
    heads_wide = query_weight.shape[1] // group
    per_rep = holders // reps
    hidden_piece = down_weight.shape[0] // reps
    hidden_wide = holders * hidden_piece
    heads = heads_wide // HD
    scale_factor = HD ** (-0.5)

    def own_rep(values, axis):
        return lax.dynamic_index_in_dim(values, r, axis, keepdims=False)

    def by_holder(values, axis):
        shape = values.shape
        cut = values.reshape(shape[:axis] + (high, PAIR, xs, -1) + shape[axis + 1 :])
        cut = jnp.moveaxis(cut, axis + 1, 0)
        return cut.reshape((PAIR,) + shape[:axis] + (holders, -1) + shape[axis + 1 :])

    def query_columns(weight):
        pieces = by_holder(weight, 1).reshape(PAIR, rows, reps, heads_wide)
        return own_rep(pieces, 2)

    def hidden_columns(weight):
        pieces = by_holder(weight, 1).reshape(PAIR, rows, holders, reps, hidden_piece)
        return own_rep(pieces, 3).reshape(PAIR, rows, hidden_wide)

    key_heads = [
        (((r * per_rep // xs) * PAIR + low) * xs * heads_wide // (per_rep * HD)) * KV
        // (query_weight.shape[1] // HD)
        for low in range(PAIR)
    ]

    def key_columns(weight):
        pieces = weight.reshape(rows, KV, HD)
        return jnp.stack(
            [lax.dynamic_index_in_dim(pieces, k, 1, keepdims=False) for k in key_heads]
        )

    attn_pack = jnp.concatenate(
        [query_columns(query_weight), key_columns(key_weight), key_columns(value_weight)], axis=2
    )
    mlp_pack = jnp.concatenate([hidden_columns(gate_weight), hidden_columns(up_weight)], axis=2)

    cos_table, sin_table = rotary_tables(length, HD)
    sign = jnp.where(jnp.arange(HD) < HD // 2, -1.0, 1.0)
    turned = heads + 1
    cos_wide = jnp.concatenate([jnp.tile(cos_table, (1, turned)), jnp.ones_like(cos_table)], axis=1)
    sin_wide = jnp.concatenate(
        [jnp.tile(sin_table * sign, (1, turned)), jnp.zeros_like(cos_table)], axis=1
    )
    gain_rows = jnp.zeros((8, rows), jnp.float32)
    gain_rows = gain_rows.at[0].set(attn_gain.astype(jnp.float32))
    gain_rows = gain_rows.at[1].set(mlp_gain.astype(jnp.float32))
    (
        attn_w, mlp_w, down_w, out_w, gains, hidden_one, cot_all, qkv, attended, mixed_sum, hidden_two,
    ) = forward(
        block_input,
        gain_rows,
        attn_pack,
        mlp_pack,
        own_rep(down_weight.reshape(reps, hidden_piece, width), 0),
        out_weight,
        cotangent,
        (cos_wide, sin_wide),
    )
    gate_up = matmul(hidden_two, mlp_w)
    gate_raw, up_raw = gate_up[:, :hidden_wide], gate_up[:, hidden_wide:]
    sigmoid = jax.nn.sigmoid(gate_raw)
    activated = gate_raw * sigmoid
    product = (activated * up_raw).astype(jnp.bfloat16)
    grad_product = contract_last(cot_all, down_w)
    grad_gate = grad_product * up_raw * sigmoid * (1.0 + gate_raw * (1.0 - sigmoid))
    grad_up = grad_product * activated
    grad_both = jnp.concatenate([grad_gate, grad_up], axis=1).astype(jnp.bfloat16)
    hidden_partial = contract_last(grad_both, mlp_w).astype(jnp.bfloat16)
    block_output = (mixed_sum + gather_rows(matmul(product, down_w).astype(jnp.bfloat16), 2)).astype(jnp.bfloat16)
    down_local = contract_first(product, cot_all).astype(jnp.bfloat16)
    mlp_local = contract_first(hidden_two, grad_both).astype(jnp.bfloat16)

    mlp_grad, down_grad, attn_grad, out_grad, input_grad, gain_grads = backward(
        hidden_partial,
        mlp_local,
        down_local,
        (hidden_one, attn_w, out_w, qkv, attended, mixed_sum, gains),
        block_input,
        cotangent,
        (cos_wide, sin_wide),
    )

    def from_holder(values):
        cut = values.reshape(PAIR, rows, high, xs, -1)
        return cut.transpose(1, 2, 0, 3, 4).reshape(rows, -1)

    down_grad = down_grad.astype(jnp.float32)
    out_grad = out_grad.astype(jnp.float32)
    mlp_grad = mlp_grad.astype(jnp.float32).reshape(reps, PAIR, rows, 2, holders, hidden_piece)
    mlp_grad = mlp_grad.transpose(3, 1, 2, 4, 0, 5)
    gate_grad, up_grad = from_holder(mlp_grad[0]), from_holder(mlp_grad[1])
    attn_grad = attn_grad.astype(jnp.float32).reshape(reps, PAIR, rows, -1)
    query_grad = attn_grad[..., :heads_wide].transpose(1, 2, 0, 3)
    query_grad = from_holder(query_grad.reshape(PAIR, rows, holders, -1))
    key_value = attn_grad[..., heads_wide:]

    def key_back(values):
        total = jnp.zeros((KV, rows, HD), jnp.float32)
        for rep in range(reps):
            for low in range(PAIR):
                head = (rep * per_rep // xs) * PAIR + low
                head = head * xs * heads_wide // (per_rep * HD)
                head = head * KV // (query_weight.shape[1] // HD)
                total = total.at[head].add(values[rep, low])
        return total.transpose(1, 0, 2).reshape(rows, -1)

    key_grad, value_grad = key_back(key_value[..., :HD]), key_back(key_value[..., HD:])
    gain_grads = lax.dynamic_slice_in_dim(gain_grads, shard * rows, rows, axis=1)
    return (
        block_output,
        input_grad,
        query_grad,
        key_grad,
        value_grad,
        out_grad,
        gate_grad,
        up_grad,
        down_grad,
        gain_grads[0],
        gain_grads[1],
    )


def solution(mesh):
    reps, shards = mesh.shape["rep"], mesh.shape["shard"]
    xs = 1
    while 2 * (2 * xs) ** 2 <= shards:
        xs *= 2
    names = ("rep", "zh", "zl", "x")
    cube = Mesh(mesh.devices.reshape(reps, shards // (PAIR * xs), PAIR, xs), names)
    tokens, matrix, vector = P(names, None), P(names[1:], None), P(names[1:])
    in_specs = (tokens, tokens, vector) + (matrix,) * 4 + (vector,) + (matrix,) * 3
    out_specs = (tokens, tokens) + (matrix,) * 7 + (vector,) * 2
    square = reps == 4 and shards // (PAIR * xs) == PAIR and xs == PAIR
    return jax.shard_map(
        per_device_square if square else per_device, mesh=cube, in_specs=in_specs, out_specs=out_specs, check_vma=False
    )
```

```python
import math

import jax
import jax.numpy as jnp
import numpy as np
from jax import lax
from jax.experimental import pallas as pl
from jax.experimental.pallas import tpu as pltpu
from jax.sharding import Mesh, PartitionSpec as P

KV = 4
HD = 64
PAIR = 2
SQUARE_DEVICES = 8
MESH = pl.DeviceIdType.MESH
epsilon = 1e-05

TP = ("rep", "zl")
HOLDERS = ("zh", "x")


def rotary_tables(length, head_size):
    positions = jnp.arange(length, dtype=jnp.float32)[:, None]
    spacing = jnp.arange(head_size // 2, dtype=jnp.float32) * (-2.0 * math.log(10000.0) / head_size)
    angles = positions * jnp.exp(spacing)[None, :]
    cos_table = jnp.cos(angles)
    sin_table = jnp.sin(angles)
    return (
        jnp.concatenate([cos_table, cos_table], axis=-1),
        jnp.concatenate([sin_table, sin_table], axis=-1),
    )


def rotate_half(values):
    middle = values.shape[-1] // 2
    return jnp.concatenate([-values[..., middle:], values[..., :middle]], axis=-1)


def rotate_back(values):
    middle = values.shape[-1] // 2
    return jnp.concatenate([values[..., middle:], -values[..., :middle]], axis=-1)


def norm_back(grad_normed, inputs, scale):
    return scale * grad_normed - inputs * (scale * scale * scale) * jnp.mean(
        grad_normed * inputs, axis=-1, keepdims=True
    )


def matmul(left, right):
    return jnp.dot(left, right, preferred_element_type=jnp.float32)


def contract_last(left, right):
    return lax.dot_general(
        left, right, (((1,), (1,)), ((), ())), preferred_element_type=jnp.float32
    )


def contract_first(left, right):
    return lax.dot_general(
        left, right, (((0,), (0,)), ((), ())), preferred_element_type=jnp.float32
    )


def gather_tokens(rows):
    return lax.all_gather(rows, TP, axis=0, tiled=True)


def scatter_tokens(partial):
    return lax.psum_scatter(
        partial.astype(jnp.bfloat16), TP, scatter_dimension=0, tiled=True
    ).astype(jnp.float32)


SWAP = [(0, 1), (1, 0)]


def swap(pieces, axis):
    first = lax.axis_index(axis) == 0
    came = lax.ppermute(jnp.where(first, pieces[1], pieces[0]), axis, SWAP)
    own = jnp.where(first, pieces[0], pieces[1])
    return jnp.stack([jnp.where(first, own, came), jnp.where(first, came, own)])


def exchange(piece, axis):
    first = lax.axis_index(axis) == 0
    came = lax.ppermute(piece, axis, SWAP)
    return jnp.stack([jnp.where(first, piece, came), jnp.where(first, came, piece)])


def gather_holders(piece):
    if lax.axis_size("zh") == PAIR and lax.axis_size("x") == PAIR:
        both = exchange(exchange(piece, "zh"), "x")
        return jnp.moveaxis(both, 0, 1).reshape((PAIR * PAIR,) + piece.shape)
    return lax.all_gather(piece, HOLDERS, axis=0)


def add(left, right):
    return (left.astype(jnp.float32) + right.astype(jnp.float32)).astype(jnp.bfloat16)


def halve(pieces, axis):
    first = lax.axis_index(axis) == 0
    came = lax.ppermute(jnp.where(first, pieces[1], pieces[0]), axis, SWAP)
    return add(jnp.where(first, pieces[0], pieces[1]), came)


def scatter_holders(partial):
    if lax.axis_size("zh") == PAIR and lax.axis_size("x") == PAIR:
        pieces = jnp.moveaxis(partial.reshape((PAIR, PAIR) + partial.shape[1:]), 1, 0)
        return halve(halve(pieces, "x"), "zh")
    return lax.psum_scatter(partial, HOLDERS, scatter_dimension=0, tiled=False)


def neighbours():
    r, zl = lax.axis_index("rep"), lax.axis_index("zl")
    zh, x = lax.axis_index("zh"), lax.axis_index("x")
    partner, across = r + 1 - 2 * lax.rem(r, 2), lax.rem(r + 2, 4)
    near = {
        "core": {"rep": partner},
        "low": {"zl": 1 - zl},
        "y": {"rep": across},
        "x": {"x": 1 - x},
        "high": {"zh": 1 - zh},
    }
    for at, (high, low, side) in enumerate(((0, 1, 1), (1, 0, 1), (1, 1, 0), (1, 1, 1))):
        flip = {}
        if high:
            flip["zh"] = 1 - zh
        if low:
            flip["zl"] = 1 - zl
        if side:
            flip["x"] = 1 - x
        near[f"peer{at}"] = flip
    return near


PEERS = ("low", "x", "high", "peer0", "peer1", "peer2", "peer3")
SQUARE = ("core", "low", "y")


def meet(near, names):
    barrier = pltpu.get_barrier_semaphore()
    for name in names:
        pl.semaphore_signal(barrier, 1, device_id=near[name], device_id_type=MESH)
    pl.semaphore_wait(barrier, len(names))


class Wires:
    def __init__(self, near, send, recv, local):
        self.near, self.sems, self.local_sems = near, (send, recv), local
        self.used, self.used_local, self.sent, self.kept = 0, 0, [], []

    def done(self, *copies):
        for copy in copies:
            copy.wait()
        self.kept = [kept for kept in self.kept if all(kept is not copy for copy in copies)]

    def describe(self, source, target, name):
        at = self.used
        self.used += 1
        return pltpu.make_async_remote_copy(
            src_ref=source,
            dst_ref=target,
            send_sem=self.sems[0].at[at],
            recv_sem=self.sems[1].at[at],
            device_id=self.near[name],
            device_id_type=MESH,
        )

    def push(self, source, target, name):
        copy = self.describe(source, target, name)
        copy.start()
        self.sent.append(copy)
        return copy

    def keep(self, source, target):
        copy = pltpu.make_async_copy(source, target, self.local_sems.at[self.used_local])
        self.used_local += 1
        copy.start()
        self.kept.append(copy)
        return copy

    def finish(self):
        for copy in self.sent:
            copy.wait_send()
        for copy in self.kept:
            copy.wait()


class Spread:
    def __init__(self, wires, own, whole):
        self.wires, self.own, self.whole = wires, own, whole
        self.length = own.shape[0]
        r, zl = lax.axis_index("rep"), lax.axis_index("zl")
        across = lax.rem(r + 2, 4)
        self.slots = {
            "own": r * PAIR + zl,
            "low": r * PAIR + 1 - zl,
            "y": across * PAIR + zl,
            "both": across * PAIR + 1 - zl,
        }

    def part(self, kind):
        start = pl.multiple_of(self.slots[kind] * self.length, 16)
        return self.whole.at[pl.ds(start, self.length)]

    def start(self, keep=True):
        push = self.wires.push
        self.low = push(self.own, self.part("own"), "low")
        self.y = push(self.own, self.part("own"), "y")
        self.core = push(self.own, self.part("own"), "core")
        if keep:
            self.wires.keep(self.own, self.part("own"))

    def pass_low(self):
        push = self.wires.push
        self.low.wait_recv()
        self.both = push(self.part("low"), self.part("low"), "y")
        self.core_low = push(self.part("low"), self.part("low"), "core")

    def pass_y(self):
        self.y.wait_recv()
        self.core_y = self.wires.push(self.part("y"), self.part("y"), "core")

    def pass_both(self):
        self.both.wait_recv()
        self.core_both = self.wires.push(self.part("both"), self.part("both"), "core")

    def end(self):
        for copy in (self.core, self.core_low, self.core_y, self.core_both):
            copy.wait_recv()


SPREAD_COPIES = 7
BOTH, ACROSS, OWN, LOW = 3, 2, 0, 1


class Gather:
    def __init__(self, near, scratch, source=None):
        self.near, self.source = near, source
        self.mine, self.out_core, self.in_core, self.out_far, self.in_far, self.sems = scratch

    def core_copy(self, kind):
        outgoing = self.out_core.at[kind]
        if self.source is not None:
            outgoing = self.source.at[pl.ds(self.start_of(kind, True), self.mine.shape[0])]
        return pltpu.make_async_remote_copy(
            src_ref=outgoing,
            dst_ref=self.in_core.at[kind],
            send_sem=self.sems.at[0, kind],
            recv_sem=self.sems.at[1, kind],
            device_id=self.near["core"],
            device_id_type=MESH,
        )

    def far_copy(self, kind):
        return pltpu.make_async_remote_copy(
            src_ref=self.out_far.at[kind],
            dst_ref=self.in_far.at[kind],
            send_sem=self.sems.at[2, kind],
            recv_sem=self.sems.at[3, kind],
            device_id=self.near["low" if kind == LOW else "y"],
            device_id_type=MESH,
        )

    def start_of(self, kind, other):
        r, zl = lax.axis_index("rep"), lax.axis_index("zl")
        rep = lax.rem(r + 2 * (kind // 2), 4)
        if other:
            rep = rep + 1 - 2 * lax.rem(rep, 2)
        slot = rep * PAIR + lax.rem(zl + kind % 2, 2)
        return pl.multiple_of(slot * self.mine.shape[0], 16)

    def run(self, partial):
        length, width = self.mine.shape
        chunk = min(width, 512)
        order = (BOTH, ACROSS, OWN, LOW)

        def send_core(kind):
            if self.source is None:
                start = self.start_of(kind, True)
                for at in range(0, width, chunk):
                    columns = slice(at, at + chunk)
                    self.out_core[kind, :, columns] = partial(start, columns).astype(jnp.bfloat16)
            self.core_copy(kind).start()

        def send_far(kind):
            start = self.start_of(kind, False)
            self.core_copy(kind).wait_recv()
            if kind == LOW:
                self.far_copy(BOTH).wait_recv()
            for at in range(0, width, chunk):
                columns = slice(at, at + chunk)
                total = partial(start, columns) + self.in_core[kind, :, columns].astype(jnp.float32)
                if kind == LOW:
                    total = total + self.in_far[BOTH, :, columns].astype(jnp.float32)
                if kind == OWN:
                    self.mine[:, columns] = total
                else:
                    self.out_far[kind, :, columns] = total.astype(jnp.bfloat16)
            if kind != OWN:
                self.far_copy(kind).start()

        send_core(order[0])
        for before, kind in zip(order, order[1:]):
            send_core(kind)
            send_far(before)
        send_far(order[-1])

    def total(self):
        self.far_copy(ACROSS).wait_recv()
        self.far_copy(LOW).wait_recv()
        result = self.mine[...] + self.in_far[ACROSS].astype(jnp.float32)
        return result + self.in_far[LOW].astype(jnp.float32)

    def finish(self):
        for kind in range(4):
            self.core_copy(kind).wait_send()
        for kind in range(1, 4):
            self.far_copy(kind).wait_send()


def gather_scratch(length, width):
    return [
        pltpu.VMEM((length, width), jnp.float32),
        pltpu.VMEM((4, length, width), jnp.bfloat16),
        pltpu.VMEM((4, length, width), jnp.bfloat16),
        pltpu.VMEM((4, length, width), jnp.bfloat16),
        pltpu.VMEM((4, length, width), jnp.bfloat16),
        pltpu.SemaphoreType.DMA((4, 4)),
    ]


def turn(values, cos_table, sin_table):
    wide = values.shape[1]
    lane = lax.broadcasted_iota(jnp.int32, values.shape, 1)
    other = jnp.where(
        lax.rem(lane, HD) < HD // 2,
        pltpu.roll(values, wide - HD // 2, 1),
        pltpu.roll(values, HD // 2, 1),
    )
    return values * cos_table + other * sin_table


def softmax_rows(query, key, causal, scale):
    scores = contract_last(query, key) * scale
    log_total = jnp.log(jnp.sum(jnp.where(causal, jnp.exp(scores), 0.0), axis=-1, keepdims=True))
    return jnp.where(causal, jnp.exp(scores - log_total), 0.0)


def causal_mask(length):
    rows = lax.broadcasted_iota(jnp.int32, (length, length), 0)
    return rows >= lax.broadcasted_iota(jnp.int32, (length, length), 1)


def sequence_order(step):
    r, zl = lax.axis_index("rep"), lax.axis_index("zl")
    kind = step // 2
    rep = lax.rem(r + 2 * (kind // 2), 4)
    other = rep + 1 - 2 * lax.rem(rep, 2)
    rep = jnp.where(lax.rem(step, 2) == 0, rep, other)
    return rep * PAIR + lax.rem(zl + lax.rem(kind, 2), 2)


def shard_of(high, low, side):
    return (high * PAIR + low) * PAIR + side


def forward_kernel(
    x_ref, gain_ref, query_w, key_w, value_w, cos_ref, sin_ref,
    gate_far, up_far, down_far, out_piece, cot_far,
    attn_w, mlp_w, down_w, out_w, gains, hidden, cot_all, qkv, attended, mixed, hidden_two,
    gain_slots, own_hidden, own_two, attn_pack, mlp_pack, gate_near, up_near,
    send, recv, local, *scratch,
):
    near = neighbours()
    r, zl = lax.axis_index("rep"), lax.axis_index("zl")
    zh, x = lax.axis_index("zh"), lax.axis_index("x")
    length, width = x_ref.shape
    rows, wide = attn_pack.shape[1:]
    heads_wide = wide - 2 * HD
    heads = heads_wide // HD
    reps = lax.axis_size("rep")
    hidden_piece = down_far.shape[0] // reps
    deep = hidden_piece
    wires = Wires(near, send, recv, local)
    push = wires.push

    def slot(ref, high, low, side):
        return ref.at[pl.ds(pl.multiple_of(shard_of(high, low, side) * rows, 16), rows)]

    def deep_slot(high, side):
        return down_w.at[pl.ds(pl.multiple_of((high * PAIR + side) * deep, 16), deep)]

    gate_in = wires.keep(gate_far, gate_near)
    up_in = wires.keep(up_far, up_near)
    cot_spread = Spread(wires, cot_far, cot_all)
    wires.keep(cot_far, cot_spread.part("own"))
    down_piece = down_far.at[pl.ds(pl.multiple_of(r * deep, 16), deep)]
    wires.keep(down_piece, deep_slot(zh, x))
    for low in range(PAIR):
        at = pl.multiple_of(shard_of(r // PAIR, low, lax.rem(r, PAIR)) * heads_wide, 128)
        attn_pack[low, :, :heads_wide] = query_w[:, pl.ds(at, heads_wide)]
        pair = pl.ds(pl.multiple_of((r // PAIR) * (PAIR * HD), 128), PAIR * HD)
        own = slice(low * HD, (low + 1) * HD)
        attn_pack[low, :, heads_wide : heads_wide + HD] = key_w[:, pair][:, own]
        attn_pack[low, :, heads_wide + HD :] = value_w[:, pair][:, own]
    meet(near, ("core", "y") + PEERS)

    own_shard = shard_of(zh, zl, x)
    gain_copies = [push(gain_ref, gain_slots.at[own_shard], name) for name in PEERS]
    gain_slots[own_shard] = gain_ref[...]
    attn_low = push(attn_pack.at[1 - zl], slot(attn_w, zh, zl, x), "low")
    attn_own_high = push(attn_pack.at[zl], slot(attn_w, zh, zl, x), "high")
    attn_own_x = push(attn_pack.at[zl], slot(attn_w, zh, zl, x), "x")
    attn_keep = wires.keep(attn_pack.at[zl], slot(attn_w, zh, zl, x))

    x_float = x_ref[...].astype(jnp.float32)
    rms_one = lax.rsqrt(jnp.mean(x_float * x_float, axis=-1, keepdims=True) + epsilon)
    for copy in gain_copies:
        copy.wait_recv()
    for at in range(SQUARE_DEVICES):
        gains[:, at * rows : (at + 1) * rows] = gain_slots[at]
    own_hidden[...] = (x_float * rms_one * gains[0:1, :]).astype(jnp.bfloat16)
    spread = Spread(wires, own_hidden, hidden)
    spread.start(keep=False)
    hidden[pl.ds(pl.multiple_of(spread.slots["own"] * length, 16), length), :] = own_hidden[...]

    attn_low.wait_recv()
    attn_low_high = push(slot(attn_w, zh, 1 - zl, x), slot(attn_w, zh, 1 - zl, x), "high")
    attn_low_x = push(slot(attn_w, zh, 1 - zl, x), slot(attn_w, zh, 1 - zl, x), "x")

    on_side, on_high = x == lax.rem(r, PAIR), zh == r // PAIR
    out_high = wires.describe(out_piece, out_w, "high")
    out_x = wires.describe(out_piece, out_w, "x")
    out_x_later = pltpu.make_async_remote_copy(
        src_ref=out_w,
        dst_ref=out_w,
        send_sem=send.at[wires.used - 1],
        recv_sem=recv.at[wires.used - 1],
        device_id=near["x"],
        device_id_type=MESH,
    )
    out_keep = pltpu.make_async_copy(out_piece, out_w, local.at[local.shape[0] - 1])

    @pl.when(on_side & on_high)
    def _():
        out_high.start()
        out_x.start()
        out_keep.start()

    attn_own_high.wait_recv()
    attn_high_x = push(slot(attn_w, 1 - zh, zl, x), slot(attn_w, 1 - zh, zl, x), "x")

    wires.done(gate_in, up_in)
    hidden_wide = mlp_pack.shape[2] // 2
    for rep in range(reps):

        @pl.when(r == rep)
        def _(rep=rep):
            def pack(step, _):
                here = pl.ds(pl.multiple_of(step * 32, 32), 32)
                for low in range(PAIR):
                    for base, source in ((0, gate_near), (hidden_wide, up_near)):
                        parts = []
                        for high in range(PAIR):
                            for side in range(PAIR):
                                at = (shard_of(high, low, side) * reps + rep) * hidden_piece
                                parts.append(source[here, at : at + hidden_piece])
                        mlp_pack[low, here, base : base + hidden_wide] = jnp.concatenate(
                            parts, axis=1
                        )
                return 0

            lax.fori_loop(0, rows // 32, pack, 0)

    attn_low_high.wait_recv()
    attn_both_x = push(slot(attn_w, 1 - zh, 1 - zl, x), slot(attn_w, 1 - zh, 1 - zl, x), "x")

    mlp_own_high = push(mlp_pack.at[zl], slot(mlp_w, zh, zl, x), "high")
    mlp_low = push(mlp_pack.at[1 - zl], slot(mlp_w, zh, zl, x), "low")
    for copy in (attn_own_x, attn_low_x, attn_high_x, attn_both_x):
        copy.wait_recv()
    mlp_own_x = push(mlp_pack.at[zl], slot(mlp_w, zh, zl, x), "x")
    down_x = push(down_piece, deep_slot(zh, x), "x")
    wires.keep(mlp_pack.at[zl], slot(mlp_w, zh, zl, x))
    wires.done(attn_keep)

    gather = Gather(near, scratch)
    causal = causal_mask(length)
    scale = HD ** (-0.5)

    def sequence(step, _):
        at = pl.multiple_of(sequence_order(step) * length, length)
        raw = matmul(hidden[pl.ds(at, length), :], attn_w[...])
        turned = turn(raw, cos_ref[...], sin_ref[...]).astype(jnp.bfloat16)
        qkv[pl.ds(at, length), :] = turned
        key, value = turned[:, heads_wide : heads_wide + HD], turned[:, heads_wide + HD :]
        outs = []
        for head in range(heads):
            query = turned[:, head * HD : (head + 1) * HD]
            weights = softmax_rows(query, key, causal, scale)
            outs.append(matmul(weights.astype(jnp.bfloat16), value))
        attended[pl.ds(at, length), :] = jnp.concatenate(outs, axis=1).astype(jnp.bfloat16)
        return 0

    spread.pass_low()
    spread.pass_y()
    spread.core.wait_recv()
    lax.fori_loop(0, 2, sequence, 0)
    spread.core_low.wait_recv()
    lax.fori_loop(2, 4, sequence, 0)
    down_high = push(down_piece, deep_slot(zh, x), "high")
    spread.pass_both()
    spread.core_y.wait_recv()
    lax.fori_loop(4, 6, sequence, 0)

    @pl.when(on_side & jnp.logical_not(on_high))
    def _():
        out_high.wait_recv()
        out_x_later.start()

    spread.core_both.wait_recv()
    lax.fori_loop(6, 8, sequence, 0)

    @pl.when(jnp.logical_not(on_side))
    def _():
        out_x.wait_recv()

    @pl.when(on_side & on_high)
    def _():
        out_keep.wait()

    gather.run(
        lambda start, columns: matmul(attended[pl.ds(start, length), :], out_w[:, columns])
    )
    mlp_own_high.wait_recv()
    mlp_high_x = push(slot(mlp_w, 1 - zh, zl, x), slot(mlp_w, 1 - zh, zl, x), "x")
    mlp_low.wait_recv()
    mlp_low_high = push(slot(mlp_w, zh, 1 - zl, x), slot(mlp_w, zh, 1 - zl, x), "high")
    mlp_low_x = push(slot(mlp_w, zh, 1 - zl, x), slot(mlp_w, zh, 1 - zl, x), "x")

    mixed[...] = x_ref[...].astype(jnp.float32) + gather.total()
    mixed_sum = mixed[...]
    rms_two = lax.rsqrt(jnp.mean(mixed_sum * mixed_sum, axis=-1, keepdims=True) + epsilon)
    own_two[...] = (mixed_sum * rms_two * gains[1:2, :]).astype(jnp.bfloat16)
    two_spread = Spread(wires, own_two, hidden_two)
    two_spread.start()
    cot_spread.start(keep=False)
    down_high.wait_recv()
    down_both_x = push(deep_slot(1 - zh, x), deep_slot(1 - zh, x), "x")
    two_spread.pass_low()
    two_spread.pass_y()
    two_spread.pass_both()
    cot_spread.pass_low()
    cot_spread.pass_y()
    cot_spread.pass_both()
    mlp_low_high.wait_recv()
    mlp_both_x = push(slot(mlp_w, 1 - zh, 1 - zl, x), slot(mlp_w, 1 - zh, 1 - zl, x), "x")
    two_spread.end()
    cot_spread.end()
    for copy in (mlp_own_x, mlp_low_x, mlp_high_x, down_x, down_both_x, mlp_both_x):
        copy.wait_recv()
    gather.finish()

    @pl.when(on_side)
    def _():
        out_x.wait_send()

    @pl.when(on_side & on_high)
    def _():
        out_high.wait_send()

    wires.finish()


FORWARD_COPIES = 64


def forward(x_rows, gain_rows, attention, mlp, out_piece, cotangent, tables):
    length, width = x_rows.shape
    group = SQUARE_DEVICES
    rows = attention[0].shape[0]
    heads_wide = width // group
    wide = heads_wide + 2 * HD
    deep = mlp[2].shape[0] // 4
    mlp_wide = 2 * PAIR * PAIR * deep
    bf16, f32 = jnp.bfloat16, jnp.float32
    shapes = [
        ((width, wide), bf16, True),
        ((width, mlp_wide), bf16, False),
        ((PAIR * PAIR * deep, width), bf16, False),
        ((heads_wide, width), bf16, True),
        ((8, width), f32, True),
        ((group * length, width), bf16, True),
        ((group * length, width), bf16, False),
        ((group * length, wide), bf16, True),
        ((group * length, heads_wide), bf16, True),
        ((length, width), f32, True),
        ((group * length, width), bf16, False),
    ]
    vmem = pl.BlockSpec(memory_space=pltpu.VMEM)
    far = pl.BlockSpec(memory_space=pl.ANY)
    return pl.pallas_call(
        forward_kernel,
        out_shape=[jax.ShapeDtypeStruct(shape, kind) for shape, kind, _ in shapes],
        in_specs=[vmem] * 7 + [far] * 5,
        out_specs=[vmem if near else far for _, _, near in shapes],
        scratch_shapes=[
            pltpu.VMEM((group, 8, rows), f32),
            pltpu.VMEM((length, width), bf16),
            pltpu.VMEM((length, width), bf16),
            pltpu.VMEM((PAIR, rows, wide), bf16),
            pltpu.VMEM((PAIR, rows, mlp_wide), bf16),
            pltpu.VMEM(mlp[0].shape, bf16),
            pltpu.VMEM(mlp[1].shape, bf16),
            pltpu.SemaphoreType.DMA((FORWARD_COPIES,)),
            pltpu.SemaphoreType.DMA((FORWARD_COPIES,)),
            pltpu.SemaphoreType.DMA((10,)),
        ]
        + gather_scratch(length, width),
        compiler_params=pltpu.CompilerParams(
            collective_id=0, has_side_effects=True, vmem_limit_bytes=60 * 2**20
        ),
        name="forward",
    )(x_rows, gain_rows, *attention, *tables, *mlp, out_piece, cotangent)


def gather_kernel(partial, result, *scratch):
    near = neighbours()
    meet(near, SQUARE)
    gather = Gather(near, scratch, partial)
    length = result.shape[0]
    gather.run(lambda start, columns: partial[pl.ds(start, length), columns].astype(jnp.float32))
    result[...] = gather.total()
    gather.finish()


def gather_rows(partial, call):
    length, width = partial.shape[0] // SQUARE_DEVICES, partial.shape[1]
    vmem = pl.BlockSpec(memory_space=pltpu.VMEM)
    return pl.pallas_call(
        gather_kernel,
        out_shape=jax.ShapeDtypeStruct((length, width), jnp.float32),
        in_specs=[vmem],
        out_specs=vmem,
        scratch_shapes=gather_scratch(length, width),
        compiler_params=pltpu.CompilerParams(
            collective_id=call, has_side_effects=True, vmem_limit_bytes=40 * 2**20
        ),
        name="gather",
    )(partial)


def backward_kernel(
    partial, mlp_local, down_local, hidden, attn_w, out_w, qkv, attended, mixed, cot_ref, x_ref,
    gains, cos_ref, sin_ref,
    mlp_out, down_out, attn_out, out_out, input_grad, gain_grads,
    mlp_x, down_x, attn_x, out_x, mlp_high, down_high, attn_high, out_high, gain_in,
    own_mixed, grad_mixed, grad_attn, attn_local, out_local, send, recv, local,
    mine, out_core, in_core, out_far, in_far, sems_two, sems_one,
):
    near = neighbours()
    r, zl = lax.axis_index("rep"), lax.axis_index("zl")
    zh, x = lax.axis_index("zh"), lax.axis_index("x")
    length, width = x_ref.shape
    wide = attn_w.shape[1]
    rows = mlp_x.shape[1]
    heads_wide = wide - 2 * HD
    heads = heads_wide // HD
    deep = down_x.shape[1]
    wires = Wires(near, send, recv, local)
    push = wires.push
    float32, bf16 = jnp.float32, jnp.bfloat16

    def slot(ref, high, low, side):
        return ref.at[pl.ds(pl.multiple_of(((high * PAIR + low) * PAIR + side) * rows, 16), rows)]

    def deep_slot(high, side):
        return down_local.at[pl.ds(pl.multiple_of((high * PAIR + side) * deep, 16), deep)]

    def add_into(target, *others):
        total = target[...].astype(float32)
        for other in others:
            total = total + other[...].astype(float32)
        target[...] = total.astype(bf16)

    meet(near, SQUARE + ("x", "high"))

    mlp_x_copies, down_x_copies = {}, {}
    for at, high in ((0, 1 - zh), (1, zh)):
        for lower, low in ((0, 1 - zl), (1, zl)):
            mlp_x_copies[at, lower] = push(
                slot(mlp_local, high, low, 1 - x), mlp_x.at[2 * at + lower], "x"
            )
        down_x_copies[at] = push(deep_slot(high, 1 - x), down_x.at[at], "x")

    def to_high(lower, low):
        mlp_x_copies[0, lower].wait_recv()
        add_into(mlp_x.at[lower], slot(mlp_local, 1 - zh, low, x))
        return push(mlp_x.at[lower], mlp_high.at[lower], "high")

    gather = Gather(near, (mine, out_core, in_core, out_far, in_far, sems_two), partial)

    gather.run(lambda start, columns: partial[pl.ds(start, length), columns].astype(float32))
    grad_hidden = gather.total()
    mixed_sum = mixed[...]
    rms_two = lax.rsqrt(jnp.mean(mixed_sum * mixed_sum, axis=-1, keepdims=True) + epsilon)
    gain_grads[1:2, :] = jnp.sum(grad_hidden * (mixed_sum * rms_two), axis=0, keepdims=True)
    grad = cot_ref[...].astype(float32) + norm_back(
        grad_hidden * gains[1:2, :], mixed_sum, rms_two
    )
    input_grad[...] = grad
    own_mixed[...] = grad.astype(bf16)
    spread = Spread(wires, own_mixed, grad_mixed)
    spread.start(keep=False)
    grad_mixed[pl.ds(pl.multiple_of(spread.slots["own"] * length, length), length), :] = own_mixed[...]
    gather.finish()
    mlp_high_copies = [to_high(0, 1 - zl)]

    gather = Gather(near, (mine, out_core, in_core, out_far, in_far, sems_one))
    causal = causal_mask(length)
    scale = HD ** (-0.5)

    def sequence(step, _):
        at = pl.multiple_of(sequence_order(step) * length, length)
        here = pl.ds(at, length)
        grad_out = contract_last(grad_mixed[here, :], out_w[...]).astype(bf16)
        turned = qkv[here, :]
        key, value = turned[:, heads_wide : heads_wide + HD], turned[:, heads_wide + HD :]
        grads = []
        grad_key = jnp.zeros((length, HD), float32)
        grad_value = jnp.zeros((length, HD), float32)
        for head in range(heads):
            own = slice(head * HD, (head + 1) * HD)
            query, upper = turned[:, own], grad_out[:, own]
            weights = softmax_rows(query, key, causal, scale)
            grad_weights = contract_last(upper, value)
            row_total = jnp.sum(weights * grad_weights, axis=-1, keepdims=True)
            grad_scores = (weights * (grad_weights - row_total) * scale).astype(bf16)
            grads.append(matmul(grad_scores, key))
            grad_key = grad_key + contract_first(grad_scores, query)
            grad_value = grad_value + contract_first(weights.astype(bf16), upper)
        grads = jnp.concatenate(grads + [grad_key, grad_value], axis=1)
        grads = turn(grads, cos_ref[...], -sin_ref[...]).astype(bf16)
        grad_attn[here, :] = grads
        return 0

    spread.pass_low()
    spread.pass_y()
    spread.core.wait_recv()
    lax.fori_loop(0, 2, sequence, 0)
    mlp_high_copies.append(to_high(1, zl))
    spread.core_low.wait_recv()
    lax.fori_loop(2, 4, sequence, 0)
    spread.pass_both()
    spread.core_y.wait_recv()
    lax.fori_loop(4, 6, sequence, 0)
    down_x_copies[0].wait_recv()
    add_into(down_x.at[0], deep_slot(1 - zh, x))
    down_high_copy = push(down_x.at[0], down_high, "high")
    spread.core_both.wait_recv()
    lax.fori_loop(6, 8, sequence, 0)
    gather.run(
        lambda start, columns: contract_last(
            grad_attn[pl.ds(start, length), :], attn_w[columns, :]
        )
    )

    def own_columns(at, _):
        here = pl.ds(pl.multiple_of(at * rows, rows), rows)
        attn_local[here, :] = contract_first(hidden[:, here], grad_attn[...]).astype(bf16)
        return 0

    lax.fori_loop(0, width // rows, own_columns, 0)
    attn_x_copies = {}
    for at, high in ((0, 1 - zh), (1, zh)):
        for lower, low in ((0, 1 - zl), (1, zl)):
            attn_x_copies[at, lower] = push(
                slot(attn_local, high, low, 1 - x), attn_x.at[2 * at + lower], "x"
            )

    def out_columns(at, _):
        here = pl.ds(pl.multiple_of(at * 512, 512), 512)
        out_local[:, here] = contract_first(attended[...], grad_mixed[:, here]).astype(bf16)
        return 0

    lax.fori_loop(0, width // 512, out_columns, 0)
    on_side, on_high = x == lax.rem(r, PAIR), zh == r // PAIR
    out_x_copy = wires.describe(out_local, out_x, "x")
    out_high_copy = wires.describe(out_local, out_high, "high")

    @pl.when(jnp.logical_not(on_side))
    def _():
        out_x_copy.start()

    def to_group(out, piece_rows, column, forward):
        here = out.at[pl.ds(pl.multiple_of(column * piece_rows, 16), piece_rows)]
        return push(here, here, "y"), push(here, here, "core")

    column_own, column_low = r * PAIR + zl, r * PAIR + 1 - zl
    across = lax.rem(r + 2, 4)

    def entry(out, column, size):
        return out.at[pl.ds(pl.multiple_of(column * size, 16), size)]

    def finish_first(x_copy, in_x, part, high_copy, in_high, out):
        x_copy.wait_recv()
        high_copy.wait_recv()
        add_into(in_x, part, in_high)
        return push(in_x, entry(out, column_own, rows), "low")

    def finish_second(x_copy, in_x, part, high_copy, in_high, out, column, size):
        x_copy.wait_recv()
        high_copy.wait_recv()
        add_into(in_x, part, in_high)
        target = entry(out, column, size)
        wires.keep(in_x, target)
        return push(in_x, target, "y"), push(in_x, target, "core")

    mlp_low = finish_first(
        mlp_x_copies[1, 0], mlp_x.at[2], slot(mlp_local, zh, 1 - zl, x),
        mlp_high_copies[0], mlp_high.at[0], mlp_out,
    )

    grad_hidden = gather.total()
    x_float = x_ref[...].astype(float32)
    rms_one = lax.rsqrt(jnp.mean(x_float * x_float, axis=-1, keepdims=True) + epsilon)
    gain_grads[0:1, :] = jnp.sum(grad_hidden * (x_float * rms_one), axis=0, keepdims=True)
    input_grad[...] = input_grad[...] + norm_back(grad_hidden * gains[0:1, :], x_float, rms_one)
    gain_grads[2:8, :] = jnp.zeros((6, width), float32)

    directions = ("core", "y", "low", "x", "high")
    steps = []

    def total_step(at):
        if steps:
            steps[-1].wait()
            wires.sent = [copy for copy in wires.sent if copy is not steps[-1]]
            gain_grads[...] = gain_grads[...] + gain_in[at - 1]
        if at < len(directions):
            steps.append(push(gain_grads, gain_in.at[at], directions[at]))

    total_step(0)

    attn_high_copies = []
    for lower, low in ((0, 1 - zl), (1, zl)):
        attn_x_copies[0, lower].wait_recv()
        add_into(attn_x.at[lower], slot(attn_local, 1 - zh, low, x))
        attn_high_copies.append(push(attn_x.at[lower], attn_high.at[lower], "high"))

    @pl.when(on_side)
    def _():
        out_x_copy.wait_recv()
        add_into(out_local, out_x)

        @pl.when(jnp.logical_not(on_high))
        def _():
            out_high_copy.start()

    mlp_second = finish_second(
        mlp_x_copies[1, 1], mlp_x.at[3], slot(mlp_local, zh, zl, x),
        mlp_high_copies[1], mlp_high.at[1], mlp_out, column_own, rows,
    )
    total_step(1)
    mlp_low.wait_recv()
    mlp_third = to_group(mlp_out, rows, column_low, None)
    total_step(2)
    down_second = finish_second(
        down_x_copies[1], down_x.at[1], deep_slot(zh, x),
        down_high_copy, down_high, down_out, r, deep,
    )
    total_step(3)
    mlp_second[0].wait_recv()
    here = entry(mlp_out, across * PAIR + zl, rows)
    last = [push(here, here, "core")]
    total_step(4)
    mlp_third[0].wait_recv()
    here = entry(mlp_out, across * PAIR + 1 - zl, rows)
    last.append(push(here, here, "core"))
    attn_low = finish_first(
        attn_x_copies[1, 0], attn_x.at[2], slot(attn_local, zh, 1 - zl, x),
        attn_high_copies[0], attn_high.at[0], attn_out,
    )
    attn_second = finish_second(
        attn_x_copies[1, 1], attn_x.at[3], slot(attn_local, zh, zl, x),
        attn_high_copies[1], attn_high.at[1], attn_out, column_own, rows,
    )

    holder = zh * PAIR + x
    role = lax.rem(r - holder + 4, 4)
    is_core = r == holder + 1 - 2 * lax.rem(holder, 2)
    is_y = role == 2
    out_core_copy = wires.describe(out_local, out_out, "core")
    out_y_copy = wires.describe(out_local, out_out, "y")
    out_y_later = pltpu.make_async_remote_copy(
        src_ref=out_out,
        dst_ref=out_out,
        send_sem=send.at[wires.used - 1],
        recv_sem=recv.at[wires.used - 1],
        device_id=near["y"],
        device_id_type=MESH,
    )
    out_keep = pltpu.make_async_copy(out_local, out_out, local.at[local.shape[0] - 1])

    @pl.when(role == 0)
    def _():
        out_high_copy.wait_recv()
        add_into(out_local, out_high)
        out_core_copy.start()
        out_y_copy.start()
        out_keep.start()

    total_step(5)
    attn_low.wait_recv()
    attn_third = to_group(attn_out, rows, column_low, None)
    down_second[0].wait_recv()
    here = entry(down_out, across, deep)
    last.append(push(here, here, "core"))
    attn_second[0].wait_recv()
    here = entry(attn_out, across * PAIR + zl, rows)
    last.append(push(here, here, "core"))

    @pl.when(is_core)
    def _():
        out_core_copy.wait_recv()
        out_y_later.start()

    attn_third[0].wait_recv()
    here = entry(attn_out, across * PAIR + 1 - zl, rows)
    last.append(push(here, here, "core"))

    @pl.when((role != 0) & jnp.logical_not(is_core))
    def _():
        out_y_copy.wait_recv()

    for copy in (mlp_second[1], mlp_third[1], down_second[1], attn_second[1], attn_third[1], *last):
        copy.wait_recv()

    @pl.when(role == 0)
    def _():
        out_core_copy.wait_send()
        out_y_copy.wait_send()
        out_keep.wait()

    @pl.when(is_core)
    def _():
        out_y_later.wait_send()

    @pl.when(jnp.logical_not(on_side))
    def _():
        out_x_copy.wait_send()

    @pl.when(on_side & jnp.logical_not(on_high))
    def _():
        out_high_copy.wait_send()

    gather.finish()
    wires.finish()


BACKWARD_COPIES = 64


def backward(partial, mlp_local, down_local, saved, x_rows, cotangent, tables):
    hidden, attn_w, out_w, qkv, attended, mixed, gains = saved
    length, width = x_rows.shape
    rows = width // SQUARE_DEVICES
    wide, mlp_wide = attn_w.shape[1], mlp_local.shape[1]
    heads_wide = wide - 2 * HD
    deep = down_local.shape[0] // (PAIR * PAIR)
    bf16, f32 = jnp.bfloat16, jnp.float32
    shapes = [
        ((width, mlp_wide), bf16, False),
        ((PAIR * PAIR * deep, width), bf16, False),
        ((width, wide), bf16, False),
        ((heads_wide, width), bf16, False),
        ((length, width), f32, True),
        ((8, width), f32, True),
    ]
    vmem = pl.BlockSpec(memory_space=pltpu.VMEM)
    far = pl.BlockSpec(memory_space=pl.ANY)
    return pl.pallas_call(
        backward_kernel,
        out_shape=[jax.ShapeDtypeStruct(shape, kind) for shape, kind, _ in shapes],
        in_specs=[vmem] * 14,
        out_specs=[vmem if near else far for _, _, near in shapes],
        scratch_shapes=[
            pltpu.VMEM((4, rows, mlp_wide), bf16),
            pltpu.VMEM((2, deep, width), bf16),
            pltpu.VMEM((4, rows, wide), bf16),
            pltpu.VMEM((heads_wide, width), bf16),
            pltpu.VMEM((2, rows, mlp_wide), bf16),
            pltpu.VMEM((deep, width), bf16),
            pltpu.VMEM((2, rows, wide), bf16),
            pltpu.VMEM((heads_wide, width), bf16),
            pltpu.VMEM((5, 8, width), f32),
            pltpu.VMEM((length, width), bf16),
            pltpu.VMEM((SQUARE_DEVICES * length, width), bf16),
            pltpu.VMEM((SQUARE_DEVICES * length, wide), bf16),
            pltpu.VMEM((width, wide), bf16),
            pltpu.VMEM((heads_wide, width), bf16),
            pltpu.SemaphoreType.DMA((BACKWARD_COPIES,)),
            pltpu.SemaphoreType.DMA((BACKWARD_COPIES,)),
            pltpu.SemaphoreType.DMA((8,)),
        ]
        + gather_scratch(length, width)
        + [pltpu.SemaphoreType.DMA((4, 4))],
        compiler_params=pltpu.CompilerParams(
            collective_id=5, has_side_effects=True, vmem_limit_bytes=63 * 2**20
        ),
        name="backward",
    )(
        partial, mlp_local, down_local, hidden, attn_w, out_w, qkv, attended, mixed, cotangent,
        x_rows, gains, *tables,
    )


def arrange_kernel(mlp, attn, down, out, gate_grad, up_grad, query_grad, key_grad, value_grad, down_grad, out_grad):
    float32 = jnp.float32
    down_grad[...] = down[...].astype(float32)
    out_grad[...] = out[...].astype(float32)
    columns, _, mlp_wide = mlp.shape
    reps = columns // PAIR
    heads_wide = attn.shape[2] - 2 * HD
    piece = mlp_wide // (2 * PAIR * PAIR)
    for high in range(PAIR):
        for low in range(PAIR):
            for side in range(PAIR):
                shard, holder = shard_of(high, low, side), high * PAIR + side
                for base, target in ((0, gate_grad), (mlp_wide // 2, up_grad)):
                    at = base + holder * piece
                    parts = [mlp[rep * PAIR + low, :, at : at + piece] for rep in range(reps)]
                    joined = jnp.concatenate(parts, axis=1).astype(float32)
                    target[:, shard * reps * piece : (shard + 1) * reps * piece] = joined
                query_grad[:, shard * heads_wide : (shard + 1) * heads_wide] = attn[
                    holder * PAIR + low, :, :heads_wide
                ].astype(float32)
    for at, target in ((heads_wide, key_grad), (heads_wide + HD, value_grad)):
        heads = []
        for high in range(PAIR):
            for low in range(PAIR):
                first, second = high * PAIR * PAIR + low, (high * PAIR + 1) * PAIR + low
                heads.append(
                    attn[first, :, at : at + HD].astype(float32)
                    + attn[second, :, at : at + HD].astype(float32)
                )
        target[...] = jnp.concatenate(heads, axis=1)


def arrange(mlp, attn, down, out):
    columns, rows, _ = mlp.shape
    steps = 8
    block = rows // steps
    width = out.shape[1]
    reps = columns // PAIR
    f32 = jnp.float32

    def split(rows_in, wide):
        return pl.BlockSpec((rows_in // steps, wide), lambda i: (i, 0))

    def deep(values):
        return pl.BlockSpec((columns, block, values.shape[2]), lambda i: (0, i, 0))

    mlp_columns = mlp.shape[2] // 2 * columns
    shapes = [
        (rows, mlp_columns), (rows, mlp_columns), (rows, width), (rows, KV * HD), (rows, KV * HD),
        (down.shape[0], width), (out.shape[0], width),
    ]
    return pl.pallas_call(
        arrange_kernel,
        grid=(steps,),
        out_shape=[jax.ShapeDtypeStruct(shape, f32) for shape in shapes],
        in_specs=[deep(mlp), deep(attn), split(down.shape[0], width), split(out.shape[0], width)],
        out_specs=[split(*shape) for shape in shapes],
        compiler_params=pltpu.CompilerParams(vmem_limit_bytes=40 * 2**20),
        name="arrange",
    )(mlp, attn, down, out)


def rotary_numbers(length, wide):
    positions = np.arange(length, dtype=np.float32)[:, None]
    spacing = np.arange(HD // 2, dtype=np.float32) * np.float32(-2.0 * math.log(10000.0) / HD)
    angles = positions * np.exp(spacing)[None, :]
    cos_half, sin_half = np.cos(angles), np.sin(angles)
    turned = wide // HD - 1
    cos_one = np.concatenate([cos_half, cos_half], axis=1)
    sin_one = np.concatenate([-sin_half, sin_half], axis=1)
    cos_wide = np.concatenate([cos_one] * turned + [np.ones_like(cos_one)], axis=1)
    sin_wide = np.concatenate([sin_one] * turned + [np.zeros_like(sin_one)], axis=1)
    return jnp.asarray(cos_wide, jnp.float32), jnp.asarray(sin_wide, jnp.float32)


def per_device(
    block_input,
    cotangent,
    attn_gain,
    query_weight,
    key_weight,
    value_weight,
    out_weight,
    mlp_gain,
    gate_weight,
    up_weight,
    down_weight,
):
    length, width = block_input.shape
    reps, xs = lax.axis_size("rep"), lax.axis_size("x")
    high = lax.axis_size("zh")
    holders = high * xs
    group = reps * PAIR
    r, zl, x = lax.axis_index("rep"), lax.axis_index("zl"), lax.axis_index("x")
    shard = (lax.axis_index("zh") * PAIR + zl) * xs + x
    rows = query_weight.shape[0]
    heads_wide = query_weight.shape[1] // group
    per_rep = holders // reps
    hidden_piece = down_weight.shape[0] // reps
    hidden_wide = holders * hidden_piece
    heads = heads_wide // HD
    scale_factor = HD ** (-0.5)

    def own_rep(values, axis):
        return lax.dynamic_index_in_dim(values, r, axis, keepdims=False)

    def by_holder(values, axis):
        shape = values.shape
        cut = values.reshape(shape[:axis] + (high, PAIR, xs, -1) + shape[axis + 1 :])
        cut = jnp.moveaxis(cut, axis + 1, 0)
        return cut.reshape((PAIR,) + shape[:axis] + (holders, -1) + shape[axis + 1 :])

    def query_columns(weight):
        pieces = by_holder(weight, 1).reshape(PAIR, rows, reps, heads_wide)
        return own_rep(pieces, 2)

    def hidden_columns(weight):
        pieces = by_holder(weight, 1).reshape(PAIR, rows, holders, reps, hidden_piece)
        return own_rep(pieces, 3).reshape(PAIR, rows, hidden_wide)

    key_heads = [
        (((r * per_rep // xs) * PAIR + low) * xs * heads_wide // (per_rep * HD)) * KV
        // (query_weight.shape[1] // HD)
        for low in range(PAIR)
    ]

    def key_columns(weight):
        pieces = weight.reshape(rows, KV, HD)
        return jnp.stack(
            [lax.dynamic_index_in_dim(pieces, k, 1, keepdims=False) for k in key_heads]
        )

    attn_pack = jnp.concatenate(
        [query_columns(query_weight), key_columns(key_weight), key_columns(value_weight)], axis=2
    )
    mlp_pack = jnp.concatenate([hidden_columns(gate_weight), hidden_columns(up_weight)], axis=2)

    gains = lax.all_gather(
        jnp.stack([attn_gain, mlp_gain]), ("zh", "zl", "x"), axis=1, tiled=True
    )
    gains = gains.astype(jnp.float32)
    gain_one, gain_two = gains[0], gains[1]

    def all_rows(pack):
        whole = gather_holders(swap(pack, "zl"))
        whole = whole.reshape((high, xs, PAIR) + whole.shape[2:])
        return jnp.swapaxes(whole, 1, 2).reshape(width, -1)

    attn_w = all_rows(attn_pack)
    out_w = own_rep(gather_holders(out_weight).reshape(reps, per_rep * rows, width), 0)
    down_w = gather_holders(own_rep(down_weight.reshape(reps, hidden_piece, width), 0))
    down_w = down_w.reshape(hidden_wide, width)
    mlp_w = all_rows(mlp_pack)

    x_float = block_input.astype(jnp.float32)
    rms_one = lax.rsqrt(jnp.mean(x_float * x_float, axis=-1, keepdims=True) + epsilon)
    normed_one = x_float * rms_one
    hidden_one = gather_tokens((normed_one * gain_one[None, :]).astype(jnp.bfloat16))
    cot_all = gather_tokens(cotangent)
    raw = matmul(hidden_one, attn_w).reshape(group, length, -1)
    cos_table, sin_table = rotary_tables(length, HD)

    def rotary(values):
        return (
            values * cos_table[:, None, :] + rotate_half(values) * sin_table[:, None, :]
        ).astype(jnp.bfloat16)

    def rotary_back(grads):
        return (
            grads * cos_table[:, None, :] + rotate_back(grads * sin_table[:, None, :])
        ).astype(jnp.bfloat16)

    query_rot = rotary(raw[..., :heads_wide].reshape(group, length, heads, HD))
    key_rot = rotary(raw[..., None, heads_wide : heads_wide + HD])[:, :, 0]
    value_rows = raw[..., heads_wide + HD :].astype(jnp.bfloat16)
    causal = jnp.arange(length)[:, None] >= jnp.arange(length)[None, :]

    def product_of(spec, left, right):
        return jnp.einsum(spec, left, right, preferred_element_type=jnp.float32)

    scores = product_of("bigd,bjd->bgij", query_rot, key_rot) * scale_factor
    log_total = jnp.log(jnp.sum(jnp.where(causal, jnp.exp(scores), 0.0), axis=-1))
    weights = jnp.where(causal, jnp.exp(scores - log_total[..., None]), 0.0)
    weights_bf = weights.astype(jnp.bfloat16)
    attended = product_of("bgij,bjd->bigd", weights_bf, value_rows)
    attended = attended.astype(jnp.bfloat16).reshape(group * length, heads_wide)
    mixed_sum = x_float + scatter_tokens(matmul(attended, out_w))

    rms_two = lax.rsqrt(jnp.mean(mixed_sum * mixed_sum, axis=-1, keepdims=True) + epsilon)
    normed_two = mixed_sum * rms_two
    hidden_two = gather_tokens((normed_two * gain_two[None, :]).astype(jnp.bfloat16))
    gate_up = matmul(hidden_two, mlp_w)
    gate_raw, up_raw = gate_up[:, :hidden_wide], gate_up[:, hidden_wide:]
    sigmoid = jax.nn.sigmoid(gate_raw)
    activated = gate_raw * sigmoid
    product = (activated * up_raw).astype(jnp.bfloat16)
    grad_product = contract_last(cot_all, down_w)
    grad_gate = grad_product * up_raw * sigmoid * (1.0 + gate_raw * (1.0 - sigmoid))
    grad_up = grad_product * activated
    grad_both = jnp.concatenate([grad_gate, grad_up], axis=1).astype(jnp.bfloat16)
    grad_hidden_two = scatter_tokens(contract_last(grad_both, mlp_w))
    block_output = (mixed_sum + scatter_tokens(matmul(product, down_w))).astype(jnp.bfloat16)
    down_local = contract_first(product, cot_all).astype(jnp.bfloat16)
    mlp_local = contract_first(hidden_two, grad_both).astype(jnp.bfloat16)

    grad_mixed = cotangent.astype(jnp.float32) + norm_back(
        grad_hidden_two * gain_two[None, :], mixed_sum, rms_two
    )

    grad_mixed_bf = gather_tokens(grad_mixed.astype(jnp.bfloat16))
    grad_attended = contract_last(grad_mixed_bf, out_w).astype(jnp.bfloat16)
    out_local = contract_first(attended, grad_mixed_bf).astype(jnp.bfloat16)
    grad_attended = grad_attended.reshape(group, length, heads, HD)
    grad_weights = product_of("bigd,bjd->bgij", grad_attended, value_rows)
    row_total = jnp.sum(weights * grad_weights, axis=-1, keepdims=True)
    grad_scores = (weights * (grad_weights - row_total) * scale_factor).astype(jnp.bfloat16)
    grad_query = rotary_back(product_of("bgij,bjd->bigd", grad_scores, key_rot))
    grad_key = rotary_back(product_of("bgij,bigd->bjd", grad_scores, query_rot)[:, :, None])
    grad_value = product_of("bgij,bigd->bjd", weights_bf, grad_attended).astype(jnp.bfloat16)
    grad_attn = jnp.concatenate(
        [
            grad_query.reshape(group * length, heads_wide),
            grad_key.reshape(group * length, HD),
            grad_value.reshape(group * length, HD),
        ],
        axis=1,
    )
    grad_hidden_one = scatter_tokens(contract_last(grad_attn, attn_w))
    attn_local = contract_first(hidden_one, grad_attn).astype(jnp.bfloat16)
    input_grad = grad_mixed + norm_back(
        grad_hidden_one * gain_one[None, :], x_float, rms_one
    )

    def to_owner(partial):
        pieces = partial.reshape(high, PAIR, xs, rows, -1)
        pieces = jnp.swapaxes(pieces, 1, 2).reshape(holders, PAIR, rows, -1)
        pieces = swap(scatter_holders(pieces), "zl")
        return lax.all_gather(pieces, "rep", axis=0).astype(jnp.float32)

    def from_holder(values):
        cut = values.reshape(PAIR, rows, high, xs, -1)
        return cut.transpose(1, 2, 0, 3, 4).reshape(rows, -1)

    down_grad = scatter_holders(down_local.reshape(holders, hidden_piece, width))
    down_grad = lax.all_gather(down_grad, "rep", axis=0, tiled=True).astype(jnp.float32)
    mlp_grad = to_owner(mlp_local).reshape(reps, PAIR, rows, 2, holders, hidden_piece)
    mlp_grad = mlp_grad.transpose(3, 1, 2, 4, 0, 5)
    gate_grad, up_grad = from_holder(mlp_grad[0]), from_holder(mlp_grad[1])
    out_padded = jnp.where(
        (jnp.arange(reps) == r)[:, None, None],
        out_local.reshape(1, per_rep * rows, width),
        jnp.zeros((), jnp.bfloat16),
    )
    out_padded = scatter_holders(out_padded.reshape(holders, rows, width))
    out_grad = lax.psum(out_padded, "rep").astype(jnp.float32)
    attn_grad = to_owner(attn_local)
    query_grad = attn_grad[..., :heads_wide].transpose(1, 2, 0, 3)
    query_grad = from_holder(query_grad.reshape(PAIR, rows, holders, -1))
    key_value = attn_grad[..., heads_wide:]

    def key_back(values):
        total = jnp.zeros((KV, rows, HD), jnp.float32)
        for rep in range(reps):
            for low in range(PAIR):
                head = (rep * per_rep // xs) * PAIR + low
                head = head * xs * heads_wide // (per_rep * HD)
                head = head * KV // (query_weight.shape[1] // HD)
                total = total.at[head].add(values[rep, low])
        return total.transpose(1, 0, 2).reshape(rows, -1)

    key_grad, value_grad = key_back(key_value[..., :HD]), key_back(key_value[..., HD:])
    gain_grads = lax.psum(
        jnp.stack(
            [
                jnp.sum(grad_hidden_one * normed_one, axis=0),
                jnp.sum(grad_hidden_two * normed_two, axis=0),
            ]
        ),
        ("rep", "zh", "zl", "x"),
    )
    gain_grads = lax.dynamic_slice_in_dim(gain_grads, shard * rows, rows, axis=1)
    return (
        block_output,
        input_grad,
        query_grad,
        key_grad,
        value_grad,
        out_grad,
        gate_grad,
        up_grad,
        down_grad,
        gain_grads[0],
        gain_grads[1],
    )


def per_device_square(
    block_input,
    cotangent,
    attn_gain,
    query_weight,
    key_weight,
    value_weight,
    out_weight,
    mlp_gain,
    gate_weight,
    up_weight,
    down_weight,
):
    length, width = block_input.shape
    rows = query_weight.shape[0]
    zl, x = lax.axis_index("zl"), lax.axis_index("x")
    shard = shard_of(lax.axis_index("zh"), zl, x)
    tables = rotary_numbers(length, width // SQUARE_DEVICES + 2 * HD)
    gain_rows = jnp.concatenate(
        [jnp.stack([attn_gain, mlp_gain]).astype(jnp.float32), jnp.zeros((6, rows), jnp.float32)]
    )
    (
        attn_w, mlp_w, down_w, out_w, gains, hidden_one, cot_all, qkv, attended, mixed_sum, hidden_two,
    ) = forward(
        block_input,
        gain_rows,
        (query_weight, key_weight, value_weight),
        (gate_weight, up_weight, down_weight),
        out_weight,
        cotangent,
        tables,
    )

    hidden_wide = down_w.shape[0]
    gate_up = matmul(hidden_two, mlp_w)
    gate_raw, up_raw = gate_up[:, :hidden_wide], gate_up[:, hidden_wide:]
    sigmoid = jax.nn.sigmoid(gate_raw)
    activated = gate_raw * sigmoid
    product = (activated * up_raw).astype(jnp.bfloat16)
    grad_product = contract_last(cot_all, down_w)
    grad_gate = grad_product * up_raw * sigmoid * (1.0 + gate_raw * (1.0 - sigmoid))
    grad_up = grad_product * activated
    grad_both = jnp.concatenate([grad_gate, grad_up], axis=1).astype(jnp.bfloat16)
    hidden_partial = contract_last(grad_both, mlp_w).astype(jnp.bfloat16)
    down_sum = gather_rows(matmul(product, down_w).astype(jnp.bfloat16), 2)
    block_output = (mixed_sum + down_sum).astype(jnp.bfloat16)
    down_local = contract_first(product, cot_all).astype(jnp.bfloat16)
    mlp_local = contract_first(hidden_two, grad_both).astype(jnp.bfloat16)

    mlp_grad, down_grad, attn_grad, out_grad, input_grad, gain_grads = backward(
        hidden_partial,
        mlp_local,
        down_local,
        (hidden_one, attn_w, out_w, qkv, attended, mixed_sum, gains),
        block_input,
        cotangent,
        tables,
    )
    gate_grad, up_grad, query_grad, key_grad, value_grad, down_grad, out_grad = arrange(
        mlp_grad.reshape(SQUARE_DEVICES, rows, -1),
        attn_grad.reshape(SQUARE_DEVICES, rows, -1),
        down_grad,
        out_grad,
    )
    gain_grads = lax.dynamic_slice_in_dim(gain_grads, shard * rows, rows, axis=1)
    return (
        block_output,
        input_grad,
        query_grad,
        key_grad,
        value_grad,
        out_grad,
        gate_grad,
        up_grad,
        down_grad,
        gain_grads[0],
        gain_grads[1],
    )


def solution(mesh):
    reps, shards = mesh.shape["rep"], mesh.shape["shard"]
    xs = 1
    while 2 * (2 * xs) ** 2 <= shards:
        xs *= 2
    names = ("rep", "zh", "zl", "x")
    cube = Mesh(mesh.devices.reshape(reps, shards // (PAIR * xs), PAIR, xs), names)
    tokens, matrix, vector = P(names, None), P(names[1:], None), P(names[1:])
    in_specs = (tokens, tokens, vector) + (matrix,) * 4 + (vector,) + (matrix,) * 3
    out_specs = (tokens, tokens) + (matrix,) * 7 + (vector,) * 2
    square = reps == 4 and shards // (PAIR * xs) == PAIR and xs == PAIR
    return jax.shard_map(
        per_device_square if square else per_device, mesh=cube, in_specs=in_specs, out_specs=out_specs, check_vma=False
    )
```
